128 devices in a mesh: req: 32 (over x, y, core), head: 4 (over z).
Axes of the slice: x: 4, y: 4, z: 4, core: 2. Of those that a mesh axis runs over, the one named last changes fastest.
Arguments:
- queries: bfloat16 [512, 64, 128], P('req', 'head'), may hold values from -6 to 6
- k_codes: bfloat16 [32768, 16, 8, 128], P('req', None, 'head'), may hold values from -6 to 6
- value_quantized_codes: bfloat16 [32768, 16, 8, 128], P('req', None, 'head'), may hold values from -6 to 6
- key_page_scale: float32 [32768, 8], P('req', 'head'), may hold values from 0.5 to 2
- value_page_scale: float32 [32768, 8], P('req', 'head'), may hold values from 4 to 16
- lengths: int32 [512], P('req'), may hold values from 1 to 2032
- page_table: int32 [512, 128], P('req'), may hold values from -1 to 32767, as said below
- out_weight: bfloat16 [8192, 8192], P('head', 'req'), may hold values from -0.0625 to 0.0625
Outputs:
- attn_out: bfloat16 [512, 8192], P(None, ('req', 'head'))
The draws below stay inside these ranges and needn't reach their ends.
Inputs may be any that keep to these rules, and one draw needn't show every extreme that they name: `page_table`: entries j below ceil(lengths[r] / 16) name pool pages; all such entries of all requests together name every pool page exactly once. Entries beyond are -1.
All inputs are finite; a program needn't handle non-finite values.
Results may differ from the reference program's by a relative error of at most 0.02.
Values may be sent and summed in bfloat16 or wider, within the bound.
A program may use at most 128 MiB of HBM per device.

```python
import math
import jax
import jax.numpy as jnp
from jax import lax

QUERY_HEADS = 64
KEY_VALUE_HEADS = 8
HEAD_DIMENSION = 128
DMODEL = 8192
PAGE_TOKENS = 16
MAXP = 128
R_DEV = 16
REQS = 512
POOL_PAGES = 32768
N_REQ = 32


def page_layout(key):
    half_count = REQS // 2
    middle = MAXP // 2
    sign_dev = 2 * jax.random.randint(jax.random.fold_in(key, 1), (N_REQ // 2,), 0, 2) - 1
    shift = jax.random.randint(jax.random.fold_in(key, 2), (half_count,), 0, middle)
    selected_pages = jax.random.randint(jax.random.fold_in(key, 3), (), 0, half_count)
    shift = shift.at[selected_pages].set(middle - 1)
    owner_dev = jnp.arange(half_count, dtype=jnp.int32) // R_DEV
    turned = sign_dev[owner_dev] * shift
    page_count = jnp.concatenate([middle + turned, middle - turned]).astype(jnp.int32)
    remainder = jax.random.randint(jax.random.fold_in(key, 4), (REQS,), 1, PAGE_TOKENS + 1)
    longest = jnp.where(sign_dev[selected_pages // R_DEV] > 0, selected_pages, selected_pages + half_count)
    remainder = remainder.at[longest].set(PAGE_TOKENS)
    lengths = ((page_count - 1) * PAGE_TOKENS + remainder).astype(jnp.int32)
    shuffled = jax.random.permutation(jax.random.fold_in(key, 5), POOL_PAGES).astype(jnp.int32)
    starts = jnp.cumsum(page_count) - page_count
    entry = jnp.arange(MAXP, dtype=jnp.int32)[None, :]
    slot = jnp.clip(starts[:, None] + entry, 0, POOL_PAGES - 1)
    table = jnp.where(entry < page_count[:, None], shuffled[slot], -1).astype(jnp.int32)
    return (lengths, table)


def draw_lengths(key, part):
    return page_layout(jax.random.fold_in(key, 11))[0]


def draw_page_table(key, part):
    return page_layout(jax.random.fold_in(key, 11))[1]


def draw_queries(key, part):
    value_rows = jnp.clip(jax.random.normal(jax.random.fold_in(key, 21), (REQS, QUERY_HEADS, HEAD_DIMENSION), jnp.float32), -6.0, 6.0)
    return value_rows.astype(jnp.bfloat16)


def draw_k_codes(key, part):
    value_rows = jnp.clip(jax.random.normal(jax.random.fold_in(key, 31), (POOL_PAGES, PAGE_TOKENS, KEY_VALUE_HEADS, HEAD_DIMENSION), jnp.float32), -6.0, 6.0)
    return value_rows.astype(jnp.bfloat16)


def steps_of(rng, extent, split, smallest, high):
    level = 1.0
    for dim, parts in split:
        draws = jax.random.uniform(jax.random.fold_in(jax.random.fold_in(rng, 6), dim), (parts,), jnp.float32, smallest / len(split), high / len(split))
        level = level * jnp.repeat(jnp.exp(draws), extent[dim] // parts).reshape((-1,) + (1,) * (len(extent) - 1 - dim))
    return level


def normal_values(key, extent, width, reach, shards=(), held_as=jnp.bfloat16):
    level = steps_of(key, extent, shards, -0.22, 0.18) if shards else 1.0
    array = jax.random.normal(key, extent, jnp.float32) * width * level
    return jnp.minimum(jnp.maximum(array, -reach), reach).astype(held_as)


def setup_inputs(seed: int = 0) -> dict:
    arg_keys = jax.random.split(jax.random.key(seed), 9)
    queries = draw_queries(jax.random.fold_in(arg_keys[8], 71), 0)
    k_codes = draw_k_codes(jax.random.fold_in(arg_keys[8], 71), 0)
    value_quantized_codes = normal_values(arg_keys[2], (POOL_PAGES, PAGE_TOKENS, KEY_VALUE_HEADS, HEAD_DIMENSION), 1.0, 6.0, ((0, 32), (2, 4)))
    key_page_scale = jnp.clip(jnp.exp(math.log(2.0) - 1.3862944 * jax.random.uniform(arg_keys[3], (POOL_PAGES, KEY_VALUE_HEADS), jnp.float32) ** steps_of(arg_keys[3], (POOL_PAGES, KEY_VALUE_HEADS), ((0, 32), (1, 4)), -0.2, 0.2)), 0.5, 2.0)
    value_page_scale = jnp.clip(jnp.exp(math.log(16.0) - 1.3862944 * jax.random.uniform(arg_keys[4], (POOL_PAGES, KEY_VALUE_HEADS), jnp.float32) ** steps_of(arg_keys[4], (POOL_PAGES, KEY_VALUE_HEADS), ((0, 32), (1, 4)), -0.2, 0.2)), 4.0, 16.0)
    lengths = draw_lengths(jax.random.fold_in(arg_keys[8], 71), 0)
    page_table = draw_page_table(jax.random.fold_in(arg_keys[8], 71), 0)
    out_weight = normal_values(arg_keys[7], (QUERY_HEADS * HEAD_DIMENSION, DMODEL), (QUERY_HEADS * HEAD_DIMENSION) ** -0.5, 0.0625, ((0, 4), (1, 32)))
    return {"queries": queries, "k_codes": k_codes, "value_quantized_codes": value_quantized_codes, "key_page_scale": key_page_scale, "value_page_scale": value_page_scale, "lengths": lengths, "page_table": page_table, "out_weight": out_weight}


floor_score = -1e+30

def reference(queries, k_codes, value_quantized_codes, key_page_scale, value_page_scale, lengths, page_table, out_weight):
    query_group_count = QUERY_HEADS // KEY_VALUE_HEADS

    def per_request(inputs_row):
        query_vector, length_row, table_row = inputs_row
        page_ids = jnp.maximum(table_row, 0).astype(jnp.int32)
        keys = k_codes[page_ids].astype(jnp.float32)
        value_rows = value_quantized_codes[page_ids].astype(jnp.float32)
        query_float = query_vector.astype(jnp.float32).reshape(KEY_VALUE_HEADS, query_group_count, HEAD_DIMENSION)
        scores = jnp.einsum('kgd,ptkd->pkgt', query_float, keys)
        scores = scores * (key_page_scale[page_ids][:, :, None, None] / math.sqrt(HEAD_DIMENSION))
        position = jnp.arange(MAXP, dtype=jnp.int32)[:, None] * PAGE_TOKENS + jnp.arange(PAGE_TOKENS, dtype=jnp.int32)[None, :]
        is_live = (position < length_row)[:, None, None, :]
        page_max = lax.optimization_barrier(jnp.max(jnp.where(is_live, scores, floor_score), axis=-1))
        weights = jnp.where(is_live, jnp.exp(scores - page_max[..., None]), 0.0)
        weights = lax.optimization_barrier(weights.astype(jnp.bfloat16)).astype(jnp.float32)
        page_sum = lax.optimization_barrier(jnp.sum(weights, axis=-1))
        page_out = jnp.einsum('pkgt,ptkd->pkgd', weights, value_rows) * value_page_scale[page_ids][:, :, None, None]
        peak = lax.optimization_barrier(jnp.max(page_max, axis=0))
        factor = jnp.exp(page_max - peak)
        numerator = lax.optimization_barrier(jnp.sum(page_out * factor[..., None], axis=0))
        denominator = lax.optimization_barrier(jnp.sum(page_sum * factor, axis=0))
        return (numerator / denominator[..., None]).reshape(QUERY_HEADS * HEAD_DIMENSION)
    attention = lax.map(per_request, (queries, lengths, page_table))
    return jnp.dot(attention.astype(jnp.bfloat16), out_weight, preferred_element_type=jnp.float32).astype(jnp.bfloat16)
```

```python
import math

import jax
import jax.numpy as jnp
from jax import lax
from jax.sharding import PartitionSpec as P

floor_score = -1e30


def in_one_piece(arrays, axis, dim, along):
    widths = [math.prod(a.shape[along:]) for a in arrays]
    both = jnp.concatenate(
        [a.reshape(*a.shape[:along], w) for a, w in zip(arrays, widths)], axis=along
    )
    out = lax.all_gather(both, axis, axis=dim, tiled=True)
    blocks = jnp.split(out, [sum(widths[:k]) for k in range(1, len(widths))], axis=along)
    return tuple((b.reshape(*out.shape[:along], *a.shape[along:]) for a, b in zip(arrays, blocks)))


def joined_along(blocks, dim):
    lengths = list(blocks.shape[1:])
    lengths[dim] *= blocks.shape[0]
    return jnp.moveaxis(blocks, 0, dim).reshape(lengths)


def from_everyone(shard, axis):
    copies = jnp.broadcast_to(shard, (lax.axis_size(axis), *shard.shape))
    return lax.all_to_all(copies, axis, split_axis=0, concat_axis=0, tiled=True)


def collect(shard, axis, dim):
    return joined_along(from_everyone(shard, axis), dim)


def split_up(shard, dim, peers):
    before, after = (shard.shape[:dim], shard.shape[dim + 1 :])
    return jnp.moveaxis(shard.reshape(*before, peers, -1, *after), dim, 0)


def summed_on_arrival(shard, axis, dim):
    blocks = split_up(shard, dim, lax.axis_size(axis))
    arrived = lax.all_to_all(blocks, axis, split_axis=0, concat_axis=0, tiled=True)
    return arrived.astype(jnp.float32).sum(axis=0)


def split_product(member_b, data):
    high_part = data.astype(jnp.bfloat16)
    low_part = (data - high_part.astype(jnp.float32)).astype(jnp.bfloat16)
    first = jnp.dot(member_b, high_part, preferred_element_type=jnp.float32)
    return first + jnp.dot(member_b, low_part, preferred_element_type=jnp.float32)


def locate_pages(page_table, lengths, pages_here):
    rows_here, table_width = page_table.shape
    peers = lax.axis_size("req")
    entry = jnp.arange(table_width, dtype=jnp.int32)[None, :]
    live = jnp.clip(lengths[:, None] - 16 * entry, 0, 16)
    row = jnp.arange(rows_here, dtype=jnp.int32)[:, None]
    code = jnp.where(live > 0, row * 16 + live, 0).reshape(-1)
    ids = page_table.reshape(-1)
    highs = peers * pages_here // 128
    in_high = (ids[None, :] >> 7) == jnp.arange(highs, dtype=jnp.int32)[:, None]
    in_low = (ids[:, None] & 127) == jnp.arange(128, dtype=jnp.int32)[None, :]
    coded = jnp.where(in_low, code[:, None], 0).astype(jnp.bfloat16)
    blocks = jnp.dot(in_high.astype(jnp.bfloat16), coded, preferred_element_type=jnp.float32)
    blocks = blocks.reshape(peers, pages_here // 128, 128)
    found = lax.all_to_all(blocks, "req", split_axis=0, concat_axis=0, tiled=True).astype(jnp.int32)
    source = jnp.arange(peers, dtype=jnp.int32)[:, None, None]
    value = jnp.sum(jnp.where(found > 0, source * 256 + found - 1, 0), axis=0).reshape(pages_here)
    return value // 16, value % 16 + 1


def on_device(
    queries,
    k_codes,
    value_quantized_codes,
    key_page_scale,
    value_page_scale,
    lengths,
    page_table,
    out_weight,
):
    pages_here, page_size, kv_local, head_size = k_codes.shape
    rows_here = queries.shape[0]
    heads_local = queries.shape[1]
    query_group_count = heads_local // kv_local
    every_query = lax.all_gather(queries, "req", axis=0, tiled=True)
    request_count = every_query.shape[0]
    owners, live_count = locate_pages(page_table, lengths, pages_here)
    is_live = jnp.arange(page_size, dtype=jnp.int32)[None, :] < live_count[:, None]
    is_live = is_live[:, None, None, :]
    member = owners[:, None] == jnp.arange(request_count, dtype=jnp.int32)[None, :]
    pick = member.astype(jnp.bfloat16)
    page_query = jnp.dot(
        pick, every_query.reshape(request_count, -1), preferred_element_type=jnp.float32
    ).astype(jnp.bfloat16)
    page_query = page_query.reshape(pages_here, kv_local, query_group_count, head_size)
    scores = jnp.einsum("pkgd,ptkd->pkgt", page_query, k_codes, preferred_element_type=jnp.float32)
    scores = scores * (key_page_scale[:, :, None, None] / math.sqrt(head_size))
    page_max = jnp.max(jnp.where(is_live, scores, floor_score), axis=-1)
    weights = jnp.where(is_live, jnp.exp(scores - page_max[..., None]), 0.0).astype(jnp.bfloat16)
    page_sum = jnp.sum(weights.astype(jnp.float32), axis=-1).reshape(pages_here, heads_local)
    page_out = jnp.einsum(
        "pkgt,ptkd->pkgd", weights, value_quantized_codes, preferred_element_type=jnp.float32
    )
    page_out = (page_out * value_page_scale[:, :, None, None]).reshape(
        pages_here, heads_local, head_size
    )
    page_max = page_max.reshape(pages_here, heads_local)
    local_peak = jnp.max(jnp.where(member[:, :, None], page_max[:, None, :], floor_score), axis=0)
    member_b = member.astype(jnp.bfloat16).T
    factor = jnp.exp(page_max - local_peak[owners])
    weighted = (page_out * factor[:, :, None]).reshape(pages_here, heads_local * head_size)
    numerator = jnp.dot(
        member_b, weighted.astype(jnp.bfloat16), preferred_element_type=jnp.float32
    ).astype(jnp.bfloat16)
    denominator = split_product(member_b, page_sum * factor)
    sources = lax.axis_size("req")
    numer_in = lax.all_to_all(
        numerator.reshape(sources, rows_here, heads_local * head_size),
        "req",
        split_axis=0,
        concat_axis=0,
        tiled=True,
    )
    denom_in = lax.all_to_all(
        denominator.reshape(sources, rows_here, heads_local),
        "req",
        split_axis=0,
        concat_axis=0,
        tiled=True,
    )
    peak_in = lax.all_to_all(
        local_peak.reshape(sources, rows_here, heads_local),
        "req",
        split_axis=0,
        concat_axis=0,
        tiled=True,
    )
    row_count = numer_in.shape[1]
    overall = jnp.max(peak_in, axis=0)
    factor = jnp.exp(peak_in - overall[None])
    numer_sum = jnp.sum(
        numer_in.astype(jnp.float32).reshape(sources, row_count, heads_local, head_size) * factor[..., None], axis=0
    )
    denom_sum = jnp.sum(denom_in * factor, axis=0)
    attention = (numer_sum / denom_sum[..., None]).reshape(row_count, heads_local * head_size)
    attention = attention.astype(jnp.bfloat16)
    terms = jnp.dot(collect(attention, "req", 0), out_weight, preferred_element_type=jnp.float32)
    return summed_on_arrival(terms.astype(jnp.bfloat16), "head", 1).astype(jnp.bfloat16)


def solution(mesh):
    in_specs = (
        P("req", "head", None),
        P("req", None, "head", None),
        P("req", None, "head", None),
        P("req", "head"),
        P("req", "head"),
        P("req"),
        P("req", None),
        P("head", "req"),
    )
    out_specs = P(None, ("req", "head"))
    return jax.shard_map(
        on_device, mesh=mesh, in_specs=in_specs, out_specs=out_specs, check_vma=False
    )
```

```python
import functools
import math

import jax
import jax.numpy as jnp
from jax import lax
from jax.experimental import pallas as pl
from jax.experimental.pallas import tpu as pltpu
from jax.sharding import PartitionSpec as P

LOG2E = 1.4426950408889634


def local_kernel(
    steps, code_ref, ks_ref, vs_ref, q_ref, k_ref, v_ref,
    att_ref, lse_ref,
    rows_ref, live_ref, ks0_ref, ks1_ref, vs0_ref, vs1_ref,
    pick_ref, pickt_ref, qs_ref, po_ref, pm_ref, ps_ref,
):
    step = pl.program_id(0)
    f32, bf16 = jnp.float32, jnp.bfloat16
    requests = q_ref.shape[0]
    pages = k_ref.shape[0] // 32
    heads = q_ref.shape[1] // 128
    half = heads // 2
    blocks = pages // 128
    scale = LOG2E / math.sqrt(128.0)
    for b in range(blocks):
        at = step * blocks + b
        code = code_ref[pl.ds(at, 1), :]
        lanes = pl.ds(pl.multiple_of(at * 128, 128), 128)
        owner_row = jnp.floor(code * (1.0 / 16.0))
        rows_ref[0:1, :] = owner_row
        rows_ref[1:2, :] = code - 16.0 * owner_row + 1.0
        rows_ref[2:4, :] = ks_ref[:, lanes] * scale
        rows_ref[4:6, :] = vs_ref[:, lanes]
        cols = rows_ref[...].T
        here = pl.ds(b * 128, 128)
        wide = lambda i: jnp.broadcast_to(cols[:, i : i + 1], (128, 128))
        live_ref[here, :] = wide(1)
        ks0_ref[here, :] = wide(2)
        ks1_ref[here, :] = wide(3)
        vs0_ref[here, :] = wide(4)
        vs1_ref[here, :] = wide(5)
        owner = wide(0)
        where_to = pl.ds(pl.multiple_of(step * pages + b * 128, 128), 128)
        lane = lax.broadcasted_iota(jnp.int32, (128, 128), 1).astype(f32)
        for c in range(requests // 128):
            pick_ref[where_to, c * 128 : (c + 1) * 128] = jnp.where(
                owner == lane + float(c * 128), 1.0, 0.0
            ).astype(bf16)
        row = lax.broadcasted_iota(jnp.int32, (requests, 128), 0).astype(f32)
        pickt_ref[:, lanes] = jnp.where(row == owner_row, 1.0, 0.0).astype(bf16)
    mine = pl.ds(pl.multiple_of(step * pages, pages), pages)
    pick = pick_ref[mine, :]
    for n in range(heads // 2):
        got = jnp.dot(pick, q_ref[:, n * 256 : (n + 1) * 256], preferred_element_type=f32)
        for j in range(2):
            h = 2 * n + j
            qs_ref[:, h * 8 : (h + 1) * 8, :] = got[:, j * 128 : (j + 1) * 128].reshape(
                pages // 8, 8, 128
            )
    lane = lax.broadcasted_iota(jnp.int32, (8, 256), 1)
    sub = lax.broadcasted_iota(jnp.int32, (8, 256), 0)
    own = (lane >> 5) == sub
    token = ((lane & 31) >> 1).astype(f32)
    far = jnp.float32(1e9)
    token0 = jnp.where(own & ((lane & 1) == 0), token, far)
    token1 = jnp.where(own & ((lane & 1) == 1), token, far)
    lane8 = lax.broadcasted_iota(jnp.int32, (8, 128), 1)
    ones = jnp.ones((256, 128), bf16)

    def tile(g):
        p8 = pl.ds(pl.multiple_of(g * 8, 8), 8)
        kv_rows = pl.ds(pl.multiple_of(g * 256, 256), 256)
        q = qs_ref[g].astype(bf16)
        s = lax.dot_general(
            q, k_ref[kv_rows, :], (((1,), (1,)), ((), ())), preferred_element_type=f32
        )
        live = live_ref[p8, :]
        live = jnp.concatenate([live, live], axis=1)
        parts = []
        peaks = []
        for half_id, (token_id, ks) in enumerate(((token0, ks0_ref), (token1, ks1_ref))):
            keep = (token_id < live)[None]
            k8 = ks[p8, :]
            k8 = jnp.concatenate([k8, k8], axis=1)[None]
            part = s[half_id * 64 : (half_id + 1) * 64].reshape(8, 8, 256)
            part = jnp.where(keep, part * k8, -1e30)
            top = jnp.max(part, axis=2, keepdims=True)
            parts.append(jnp.exp2(part - top).reshape(64, 256).astype(bf16))
            peaks.append(top)
        weights = jnp.concatenate(parts, axis=0)
        both = jnp.concatenate([v_ref[kv_rows, :], ones], axis=1)
        out = jnp.dot(weights, both, preferred_element_type=f32)
        pm = jnp.zeros((8, 128), f32)
        ps = jnp.zeros((8, 128), f32)
        rows = pl.ds(pl.multiple_of(step * pages + g * 8, 8), 8)
        for h in range(heads):
            vs = (vs0_ref if h < half else vs1_ref)[p8, :]
            po_ref[rows, h * 128 : (h + 1) * 128] = out[h * 8 : (h + 1) * 8, 0:128] * vs
            ps = jnp.where(lane8 == h, out[h * 8 : (h + 1) * 8, 128:256], ps)
            pm = jnp.where(lane8 == h, peaks[h // half][h % half], pm)
        pm_ref[rows, :] = pm
        ps_ref[rows, :] = ps

    group = 4

    def body(i, carry):
        for u in range(group):
            tile(i * group + u)
        return carry

    lax.fori_loop(0, pages // 8 // group, body, 0)

    @pl.when(step == steps - 1)
    def _():
        pm = pm_ref[...]
        first = jnp.dot(
            pickt_ref[...], jnp.exp2(pm * (1.0 / 16.0)).astype(bf16), preferred_element_type=f32
        )
        some = first > 0.0
        coarse = jnp.where(some, 16.0 * jnp.log2(jnp.where(some, first, 1.0)), 0.0).astype(bf16)
        back = jnp.dot(pick_ref[...], coarse, preferred_element_type=f32)
        second = jnp.dot(
            pickt_ref[...], jnp.exp2((pm - back) * 0.5).astype(bf16), preferred_element_type=f32
        )
        fine = coarse.astype(f32) + 2.0 * jnp.log2(jnp.where(some, second, 1.0))
        shift = fine.astype(bf16)
        factor = jnp.exp2(pm - jnp.dot(pick_ref[...], shift, preferred_element_type=f32))
        sums = ps_ref[...] * factor
        high = sums.astype(bf16)
        low = (sums - high.astype(f32)).astype(bf16)
        den = jnp.dot(pickt_ref[...], high, preferred_element_type=f32)
        den = den + jnp.dot(pickt_ref[...], low, preferred_element_type=f32)
        safe = jnp.where(some, den, 1.0)
        lse_ref[...] = jnp.where(some, shift.astype(f32) + jnp.log2(safe), -1e30)
        ps_ref[...] = factor
        inverse = 1.0 / safe
        for n in range(heads // 2):
            cols = []
            for j in range(2):
                h = 2 * n + j
                cols.append(
                    (po_ref[:, h * 128 : (h + 1) * 128] * ps_ref[:, h : h + 1]).astype(bf16)
                )
            total = jnp.dot(
                pickt_ref[...], jnp.concatenate(cols, axis=1), preferred_element_type=f32
            )
            for j in range(2):
                h = 2 * n + j
                att_ref[:, h * 128 : (h + 1) * 128] = (
                    total[:, j * 128 : (j + 1) * 128] * inverse[:, h : h + 1]
                ).astype(bf16)


def local_attention(code, ks, vs, every_query, keys, values):
    total_pages = keys.shape[0] // 32
    steps = 4
    pages = total_pages // steps
    requests, width = every_query.shape
    vmem = pl.BlockSpec(memory_space=pltpu.VMEM)
    f32, bf16 = jnp.float32, jnp.bfloat16
    return pl.pallas_call(
        functools.partial(local_kernel, steps),
        grid=(steps,),
        out_shape=(
            jax.ShapeDtypeStruct((requests, width), bf16),
            jax.ShapeDtypeStruct((requests, 128), f32),
        ),
        in_specs=[vmem, vmem, vmem, vmem]
        + [pl.BlockSpec((pages * 32, 128), lambda t: (t, 0))] * 2,
        out_specs=(vmem, vmem),
        scratch_shapes=[pltpu.VMEM((8, 128), f32)]
        + [pltpu.VMEM((pages, 128), f32)] * 5
        + [
            pltpu.VMEM((total_pages, requests), bf16),
            pltpu.VMEM((requests, total_pages), bf16),
            pltpu.VMEM((pages // 8, 128, 128), f32),
            pltpu.VMEM((total_pages, width), f32),
            pltpu.VMEM((total_pages, 128), f32),
            pltpu.VMEM((total_pages, 128), f32),
        ],
        compiler_params=pltpu.CompilerParams(vmem_limit_bytes=60 * 1024 * 1024),
        name="local_attention",
    )(code, ks, vs, every_query, keys, values)


def joined_along(blocks, dim):
    lengths = list(blocks.shape[1:])
    lengths[dim] *= blocks.shape[0]
    return jnp.moveaxis(blocks, 0, dim).reshape(lengths)


def from_everyone(shard, axis):
    copies = jnp.broadcast_to(shard, (lax.axis_size(axis), *shard.shape))
    return lax.all_to_all(copies, axis, split_axis=0, concat_axis=0, tiled=True)


def collect(shard, axis, dim):
    return joined_along(from_everyone(shard, axis), dim)


def split_up(shard, dim, peers):
    before, after = (shard.shape[:dim], shard.shape[dim + 1 :])
    return jnp.moveaxis(shard.reshape(*before, peers, -1, *after), dim, 0)


def summed_on_arrival(shard, axis, dim):
    blocks = split_up(shard, dim, lax.axis_size(axis))
    arrived = lax.all_to_all(blocks, axis, split_axis=0, concat_axis=0, tiled=True)
    return arrived.astype(jnp.float32).sum(axis=0)


def locate_pages(page_table, lengths, pages_here):
    rows_here, table_width = page_table.shape
    peers = lax.axis_size("req")
    entry = jnp.arange(table_width, dtype=jnp.int32)[None, :]
    live = jnp.clip(lengths[:, None] - 16 * entry, 0, 16)
    row = jnp.arange(rows_here, dtype=jnp.int32)[:, None]
    code = jnp.where(live > 0, row * 16 + live, 0).reshape(-1)
    ids = page_table.reshape(-1)
    highs = peers * pages_here // 128
    in_high = (ids[None, :] >> 7) == jnp.arange(highs, dtype=jnp.int32)[:, None]
    in_low = (ids[:, None] & 127) == jnp.arange(128, dtype=jnp.int32)[None, :]
    coded = jnp.where(in_low, code[:, None], 0).astype(jnp.bfloat16)
    blocks = jnp.dot(in_high.astype(jnp.bfloat16), coded, preferred_element_type=jnp.float32)
    blocks = blocks.reshape(peers, pages_here // 128, 128)
    found = lax.all_to_all(blocks, "req", split_axis=0, concat_axis=0, tiled=True).astype(jnp.int32)
    source = jnp.arange(peers, dtype=jnp.int32)[:, None, None]
    value = jnp.sum(jnp.where(found > 0, source * 256 + found - 1, 0), axis=0)
    return value.astype(jnp.float32)


def on_device(
    queries,
    k_codes,
    value_quantized_codes,
    key_page_scale,
    value_page_scale,
    lengths,
    page_table,
    out_weight,
):
    pages_here, page_size, kv_local, head_size = k_codes.shape
    rows_here, heads_local = queries.shape[:2]
    sources = lax.axis_size("req")
    code = locate_pages(page_table, lengths, pages_here)
    every_query = lax.all_gather(queries.reshape(rows_here, -1), "req", axis=0, tiled=True)
    part, weight = local_attention(
        code,
        key_page_scale.T,
        value_page_scale.T,
        every_query,
        k_codes.reshape(-1, head_size),
        value_quantized_codes.reshape(-1, head_size),
    )
    part_in = lax.all_to_all(
        part.reshape(sources, rows_here, heads_local * head_size),
        "req",
        split_axis=0,
        concat_axis=0,
        tiled=True,
    )
    weight_in = lax.all_to_all(
        weight[:, :heads_local].reshape(sources, rows_here, heads_local),
        "req",
        split_axis=0,
        concat_axis=0,
        tiled=True,
    )
    share = jnp.exp2(weight_in - jnp.max(weight_in, axis=0)[None])
    share = share / jnp.sum(share, axis=0)[None]
    part_in = part_in.astype(jnp.float32).reshape(sources, rows_here, heads_local, head_size)
    attention = jnp.sum(part_in * share[..., None], axis=0).reshape(rows_here, -1)
    attention = attention.astype(jnp.bfloat16)
    terms = jnp.dot(collect(attention, "req", 0), out_weight, preferred_element_type=jnp.float32)
    return summed_on_arrival(terms.astype(jnp.bfloat16), "head", 1).astype(jnp.bfloat16)


def solution(mesh):
    in_specs = (
        P("req", "head", None),
        P("req", None, "head", None),
        P("req", None, "head", None),
        P("req", "head"),
        P("req", "head"),
        P("req"),
        P("req", None),
        P("head", "req"),
    )
    out_specs = P(None, ("req", "head"))
    return jax.shard_map(
        on_device, mesh=mesh, in_specs=in_specs, out_specs=out_specs, check_vma=False
    )
```

```python
import functools
import math

import jax
import jax.numpy as jnp
from jax import lax
from jax.experimental import pallas as pl
from jax.experimental.pallas import tpu as pltpu
from jax.sharding import PartitionSpec as P

LOG2E = 1.4426950408889634


MESH = pl.DeviceIdType.MESH


def place():
    me = lax.axis_index("req")
    return lax.div(me, 8), lax.rem(lax.div(me, 2), 4), lax.rem(me, 2)


def off(i, d):
    return lax.rem(i + d + 4, 4)


def chip(x, y, c):
    return {"req": (x * 4 + y) * 2 + c}


class Copies:
    def __init__(self, send_sems, recv_sems):
        self.sems, self.count, self.sent = (send_sems, recv_sems), 0, []

    def send(self, source, target, device, landing):
        pair = (self.sems[0].at[self.count], self.sems[1].at[self.count])
        self.count += 1
        copy = pltpu.make_async_remote_copy(source, target, *pair, device, device_id_type=MESH)
        copy.start()
        self.sent.append(copy)
        return pltpu.make_async_remote_copy(source, landing, *pair, device, device_id_type=MESH)

    def drain(self):
        for copy in self.sent:
            copy.wait_send()


def greet(x, y, c, others=()):
    barrier = pltpu.get_barrier_semaphore()
    peers = [chip(off(x, d), y, c) for d in (1, 2, 3)]
    peers += [chip(x, off(y, d), c) for d in (1, 2, 3)]
    peers += [chip(x, y, 1 - c)] + list(others)
    for peer in peers:
        pl.semaphore_signal(barrier, inc=1, device_id=peer, device_id_type=MESH)
    pl.semaphore_wait(barrier, len(peers))


def gather_first(copies, own, view, x, y, c, halves):
    left, right = halves
    waits = []
    for d in (2, 1, 3):
        waits.append(
            copies.send(
                own.at[:, left], view(x, y, c, left), chip(x, off(y, d), c),
                view(x, off(y, -d), c, left),
            )
        )
        waits.append(
            copies.send(
                own.at[:, right], view(x, y, c, right), chip(off(x, d), y, c),
                view(off(x, -d), y, c, right),
            )
        )
    return waits


def gather_second(copies, view, x, y, c, halves):
    left, right = halves
    every = slice(None)
    waits = []
    for d in (2, 1, 3):
        waits.append(
            copies.send(
                view(x, every, c, left), view(x, every, c, left), chip(off(x, d), y, c),
                view(off(x, -d), every, c, left),
            )
        )
        waits.append(
            copies.send(
                view(every, y, c, right), view(every, y, c, right), chip(x, off(y, d), c),
                view(every, off(y, -d), c, right),
            )
        )
    return waits


def gather_third(copies, waits, view, x, y, c, halves):
    left, right = halves
    every = slice(None)
    twin = chip(x, y, 1 - c)
    last = []

    def pass_on(piece, theirs):
        last.append(copies.send(piece, piece, twin, theirs))

    pass_on(view(x, every, c, left), view(x, every, 1 - c, left))
    pass_on(view(every, y, c, right), view(every, y, 1 - c, right))
    for k, d in enumerate((2, 1, 3)):
        waits[2 * k].wait_recv()
        row = off(x, -d)
        pass_on(view(row, every, c, left), view(row, every, 1 - c, left))
        waits[2 * k + 1].wait_recv()
        row = off(y, -d)
        pass_on(view(every, row, c, right), view(every, row, 1 - c, right))
    return last


def gather_kernel(
    lengths_ref, q_ref, table_ref, all_ref, code_ref,
    table_out, sum_y, sum_c, in_x, in_y, in_c, send_sems, recv_sems,
):
    f32, bf16 = jnp.float32, jnp.bfloat16
    x, y, c = place()
    rows, width = q_ref.shape
    halves = (slice(0, width // 2), slice(width // 2, width))

    def view(i, j, k, cols):
        return all_ref.at[k, i, j, :, cols]

    greet(x, y, c)
    copies = Copies(send_sems, recv_sems)
    first = gather_first(copies, q_ref, view, x, y, c, halves)
    all_ref[c, x, y] = q_ref[...]
    lane = lax.broadcasted_iota(jnp.int32, (1, 128), 1)
    high_id = lax.broadcasted_iota(jnp.int32, (256, 128), 0)
    low_id = lax.broadcasted_iota(jnp.int32, (128, 128), 0)
    highs, lows = [], []
    for r in range(rows):
        live = jnp.clip(lengths_ref[r] - 16 * lane, 0, 16)
        coded = jnp.where(live > 0, live + 16 * r, 0).astype(f32)
        ids = table_ref[r : r + 1, :]
        highs.append(jnp.where(high_id == (ids >> 7), 1.0, 0.0).astype(bf16))
        lows.append(jnp.where(low_id == (ids & 127), coded, 0.0).astype(bf16))
    found = lax.dot_general(
        jnp.concatenate(highs, axis=1), jnp.concatenate(lows, axis=1),
        (((1,), (1,)), ((), ())), preferred_element_type=f32,
    )
    base = ((c * 16 + x * 4 + y) * 256).astype(f32)
    table_out[...] = jnp.where(found > 0.0, found + base, 0.0).reshape(4, 4, 2, 8, 128)
    got = [
        copies.send(
            table_out.at[off(x, d)], in_x.at[d - 1], chip(off(x, d), y, c), in_x.at[d - 1]
        )
        for d in (2, 1, 3)
    ]
    for wait in first:
        wait.wait_recv()
    second = gather_second(copies, view, x, y, c, halves)
    for wait in got:
        wait.wait_recv()
    sum_y[...] = table_out[x] + in_x[0] + in_x[1] + in_x[2]
    got = [
        copies.send(sum_y.at[off(y, d)], in_y.at[d - 1], chip(x, off(y, d), c), in_y.at[d - 1])
        for d in (2, 1, 3)
    ]
    for wait in got:
        wait.wait_recv()
    sum_c[...] = sum_y[y] + in_y[0] + in_y[1] + in_y[2]
    got = copies.send(sum_c.at[1 - c], in_c, chip(x, y, 1 - c), in_c)
    third = gather_third(copies, second, view, x, y, c, halves)
    got.wait_recv()
    code_ref[...] = sum_c[c] + in_c[...] - 1.0
    for wait in third:
        wait.wait_recv()
    copies.drain()


def gather_inputs(lengths, queries, page_table):
    rows, width = queries.shape
    f32 = jnp.float32
    vmem = pl.BlockSpec(memory_space=pltpu.VMEM)
    return pl.pallas_call(
        gather_kernel,
        out_shape=(
            jax.ShapeDtypeStruct((2, 4, 4, rows, width), queries.dtype),
            jax.ShapeDtypeStruct((8, 128), f32),
        ),
        in_specs=[pl.BlockSpec(memory_space=pltpu.SMEM), vmem, vmem],
        out_specs=(vmem, vmem),
        scratch_shapes=[
            pltpu.VMEM((4, 4, 2, 8, 128), f32),
            pltpu.VMEM((4, 2, 8, 128), f32),
            pltpu.VMEM((2, 8, 128), f32),
            pltpu.VMEM((3, 4, 2, 8, 128), f32),
            pltpu.VMEM((3, 2, 8, 128), f32),
            pltpu.VMEM((8, 128), f32),
            pltpu.SemaphoreType.DMA((27,)),
            pltpu.SemaphoreType.DMA((27,)),
        ],
        compiler_params=pltpu.CompilerParams(
            collective_id=1, has_side_effects=True, vmem_limit_bytes=32 * 1024 * 1024
        ),
        name="gather_inputs",
    )(lengths, queries, page_table)


def unpack_log(aux):
    aux = aux.astype(jnp.float32)
    return aux + pltpu.roll(aux, 112, 1) + pltpu.roll(aux, 96, 1)


def pack_log(value):
    f32, bf16 = jnp.float32, jnp.bfloat16
    high = value.astype(bf16).astype(f32)
    middle = (value - high).astype(bf16).astype(f32)
    low = value - high - middle
    lane = lax.broadcasted_iota(jnp.int32, value.shape, 1)
    low = jnp.where(lane < 48, pltpu.roll(low, 32, 1), 0.0)
    low = jnp.where(lane < 32, pltpu.roll(middle, 16, 1), low)
    return jnp.where(lane < 16, high, low).astype(bf16)


def merged(blocks, first_head):
    logs = [unpack_log(b[:, 1024:1152]) for b in blocks]
    top = functools.reduce(jnp.maximum, logs)
    shares = [jnp.exp2(g - top) for g in logs]
    total = functools.reduce(jnp.add, shares)
    inverse = 1.0 / total
    shares = [s * inverse for s in shares]
    columns = []
    for h in range(8):
        at = first_head + h
        columns.append(
            functools.reduce(
                jnp.add,
                [
                    b[:, h * 128 : (h + 1) * 128].astype(jnp.float32) * s[:, at : at + 1]
                    for b, s in zip(blocks, shares)
                ],
            ).astype(jnp.bfloat16)
        )
    return columns, top + jnp.log2(total)


def store_merged(target, index, start, blocks, first_head):
    columns, log = merged(blocks, first_head)
    for h, column in enumerate(columns):
        target[index + (slice(None), slice(start + h * 128, start + (h + 1) * 128))] = column
    if target.shape[-1] != 2048:
        target[index + (slice(None), slice(start + 1024, start + 1152))] = pack_log(log)


def combine_kernel(
    part_ref, weight_ref, out_ref,
    twin_in, now, in_left, in_right, left_now, right_now, in_left2, in_right2,
    own, all_ref, terms, turned, send_sems, recv_sems,
):
    f32, bf16 = jnp.float32, jnp.bfloat16
    x, y, c = place()
    z = lax.axis_index("head")
    every = slice(None)
    wide = 1152
    left, right = slice(0, wide), slice(wide, 2 * wide)
    greet(x, y, c, [{"head": off(z, d)} for d in (1, 2, 3)])
    copies = Copies(send_sems, recv_sems)
    twin = [
        copies.send(part_ref.at[1 - c, i], twin_in.at[i], chip(x, y, 1 - c), twin_in.at[i])
        for i in range(4)
    ]
    for k in range(16):
        turned[:, k * 128 : (k + 1) * 128] = weight_ref[k * 128 : (k + 1) * 128, :].T
    for i in range(4):
        twin[i].wait_recv()

        def body(j, carry):
            for start, head in ((0, 0), (wide, 8)):
                cols = slice(start, start + wide)
                store_merged(
                    now, (i, j), start, [part_ref[c, i, j, :, cols], twin_in[i, j, :, cols]], head
                )
            return carry

        lax.fori_loop(0, 4, body, 0)
    waits = []
    for d in (2, 1, 3):
        waits.append(
            copies.send(
                now.at[off(x, d), :, :, left], in_left.at[d - 1], chip(off(x, d), y, c),
                in_left.at[d - 1],
            )
        )
        waits.append(
            copies.send(
                now.at[:, off(y, d), :, right], in_right.at[d - 1], chip(x, off(y, d), c),
                in_right.at[d - 1],
            )
        )
    for wait in waits:
        wait.wait_recv()

    def body(j, carry):
        store_merged(
            left_now, (j,), 0, [now[x, j, :, left]] + [in_left[d, j] for d in range(3)], 0
        )
        store_merged(
            right_now, (j,), 0, [now[j, y, :, right]] + [in_right[d, j] for d in range(3)], 8
        )
        return carry

    lax.fori_loop(0, 4, body, 0)
    waits = []
    for d in (2, 1, 3):
        waits.append(
            copies.send(
                left_now.at[off(y, d)], in_left2.at[d - 1], chip(x, off(y, d), c),
                in_left2.at[d - 1],
            )
        )
        waits.append(
            copies.send(
                right_now.at[off(x, d)], in_right2.at[d - 1], chip(off(x, d), y, c),
                in_right2.at[d - 1],
            )
        )
    for wait in waits:
        wait.wait_recv()
    store_merged(own, (), 0, [left_now[y]] + [in_left2[d] for d in range(3)], 0)
    store_merged(own, (), 1024, [right_now[x]] + [in_right2[d] for d in range(3)], 8)

    def view(i, j, k, cols):
        return all_ref.at[i, j, k, :, cols]

    halves = (slice(0, 1024), slice(1024, 2048))
    first = gather_first(copies, own, view, x, y, c, halves)
    all_ref[x, y, c] = own[...]
    for wait in first:
        wait.wait_recv()
    second = gather_second(copies, view, x, y, c, halves)
    for wait in gather_third(copies, second, view, x, y, c, halves):
        wait.wait_recv()
    attention = all_ref[...].reshape(512, 2048)
    terms[...] = (
        lax.dot_general(
            turned[...], attention, (((1,), (1,)), ((), ())), preferred_element_type=f32
        )
        .astype(bf16)
        .reshape(4, 64, 512)
    )
    waits = [
        copies.send(terms.at[off(z, d)], out_ref.at[d], {"head": off(z, d)}, out_ref.at[d])
        for d in (2, 1, 3)
    ]
    out_ref[0] = terms[z]
    for wait in waits:
        wait.wait_recv()
    copies.drain()


def combine(part, weight):
    bf16 = jnp.bfloat16
    vmem = pl.BlockSpec(memory_space=pltpu.VMEM)
    return pl.pallas_call(
        combine_kernel,
        out_shape=jax.ShapeDtypeStruct((4, 64, 512), bf16),
        in_specs=[vmem, vmem],
        out_specs=vmem,
        scratch_shapes=[
            pltpu.VMEM((4, 4, 16, 2304), bf16),
            pltpu.VMEM((4, 4, 16, 2304), bf16),
            pltpu.VMEM((3, 4, 16, 1152), bf16),
            pltpu.VMEM((3, 4, 16, 1152), bf16),
            pltpu.VMEM((4, 16, 1152), bf16),
            pltpu.VMEM((4, 16, 1152), bf16),
            pltpu.VMEM((3, 16, 1152), bf16),
            pltpu.VMEM((3, 16, 1152), bf16),
            pltpu.VMEM((16, 2048), bf16),
            pltpu.VMEM((4, 4, 2, 16, 2048), bf16),
            pltpu.VMEM((4, 64, 512), bf16),
            pltpu.VMEM((256, 2048), bf16),
            pltpu.SemaphoreType.DMA((39,)),
            pltpu.SemaphoreType.DMA((39,)),
        ],
        compiler_params=pltpu.CompilerParams(
            collective_id=2, has_side_effects=True, vmem_limit_bytes=40 * 1024 * 1024
        ),
        name="combine",
    )(part, weight)


def local_kernel(
    steps, code_ref, ks_ref, vs_ref, q_ref, k_ref, v_ref,
    att_ref,
    rows_ref, live_ref, ks0_ref, ks1_ref, vs0_ref, vs1_ref,
    pick_ref, pickt_ref, qs_ref, po_ref, pm_ref, ps_ref,
):
    step = pl.program_id(0)
    f32, bf16 = jnp.float32, jnp.bfloat16
    requests = q_ref.shape[0]
    pages = k_ref.shape[0] // 32
    heads = q_ref.shape[1] // 128
    half = heads // 2
    blocks = pages // 128
    scale = LOG2E / math.sqrt(128.0)
    for b in range(blocks):
        at = step * blocks + b
        code = code_ref[pl.ds(at, 1), :]
        lanes = pl.ds(pl.multiple_of(at * 128, 128), 128)
        owner_row = jnp.floor(code * (1.0 / 16.0))
        rows_ref[0:1, :] = owner_row
        rows_ref[1:2, :] = code - 16.0 * owner_row + 1.0
        rows_ref[2:4, :] = ks_ref[:, lanes] * scale
        rows_ref[4:6, :] = vs_ref[:, lanes]
        cols = rows_ref[...].T
        here = pl.ds(b * 128, 128)
        wide = lambda i: jnp.broadcast_to(cols[:, i : i + 1], (128, 128))
        live_ref[here, :] = wide(1)
        ks0_ref[here, :] = wide(2)
        ks1_ref[here, :] = wide(3)
        vs0_ref[here, :] = wide(4)
        vs1_ref[here, :] = wide(5)
        owner = wide(0)
        where_to = pl.ds(pl.multiple_of(step * pages + b * 128, 128), 128)
        lane = lax.broadcasted_iota(jnp.int32, (128, 128), 1).astype(f32)
        for c in range(requests // 128):
            pick_ref[where_to, c * 128 : (c + 1) * 128] = jnp.where(
                owner == lane + float(c * 128), 1.0, 0.0
            ).astype(bf16)
        row = lax.broadcasted_iota(jnp.int32, (requests, 128), 0).astype(f32)
        pickt_ref[:, lanes] = jnp.where(row == owner_row, 1.0, 0.0).astype(bf16)
    mine = pl.ds(pl.multiple_of(step * pages, pages), pages)
    pick = pick_ref[mine, :]
    for n in range(heads // 2):
        got = jnp.dot(pick, q_ref[:, n * 256 : (n + 1) * 256], preferred_element_type=f32)
        for j in range(2):
            h = 2 * n + j
            qs_ref[:, h * 8 : (h + 1) * 8, :] = got[:, j * 128 : (j + 1) * 128].reshape(
                pages // 8, 8, 128
            )
    lane = lax.broadcasted_iota(jnp.int32, (8, 256), 1)
    sub = lax.broadcasted_iota(jnp.int32, (8, 256), 0)
    own = (lane >> 5) == sub
    token = ((lane & 31) >> 1).astype(f32)
    far = jnp.float32(1e9)
    token0 = jnp.where(own & ((lane & 1) == 0), token, far)
    token1 = jnp.where(own & ((lane & 1) == 1), token, far)
    lane8 = lax.broadcasted_iota(jnp.int32, (8, 128), 1)
    ones = jnp.ones((256, 128), bf16)

    def tile(g):
        p8 = pl.ds(pl.multiple_of(g * 8, 8), 8)
        kv_rows = pl.ds(pl.multiple_of(g * 256, 256), 256)
        q = qs_ref[g].astype(bf16)
        s = lax.dot_general(
            q, k_ref[kv_rows, :], (((1,), (1,)), ((), ())), preferred_element_type=f32
        )
        live = live_ref[p8, :]
        live = jnp.concatenate([live, live], axis=1)
        parts = []
        peaks = []
        for half_id, (token_id, ks) in enumerate(((token0, ks0_ref), (token1, ks1_ref))):
            keep = (token_id < live)[None]
            k8 = ks[p8, :]
            k8 = jnp.concatenate([k8, k8], axis=1)[None]
            part = s[half_id * 64 : (half_id + 1) * 64].reshape(8, 8, 256)
            part = jnp.where(keep, part * k8, -1e30)
            top = jnp.max(part, axis=2, keepdims=True)
            parts.append(jnp.exp2(part - top).reshape(64, 256).astype(bf16))
            peaks.append(top)
        weights = jnp.concatenate(parts, axis=0)
        both = jnp.concatenate([v_ref[kv_rows, :], ones], axis=1)
        out = jnp.dot(weights, both, preferred_element_type=f32)
        pm = jnp.zeros((8, 128), f32)
        ps = jnp.zeros((8, 128), f32)
        rows = pl.ds(pl.multiple_of(step * pages + g * 8, 8), 8)
        for h in range(heads):
            vs = (vs0_ref if h < half else vs1_ref)[p8, :]
            po_ref[rows, h * 128 : (h + 1) * 128] = out[h * 8 : (h + 1) * 8, 0:128] * vs
            ps = jnp.where(lane8 == h, out[h * 8 : (h + 1) * 8, 128:256], ps)
            pm = jnp.where(lane8 == h, peaks[h // half][h % half], pm)
        pm_ref[rows, :] = pm
        ps_ref[rows, :] = ps

    group = 4

    def body(i, carry):
        for u in range(group):
            tile(i * group + u)
        return carry

    lax.fori_loop(0, pages // 8 // group, body, 0)

    @pl.when(step == steps - 1)
    def _():
        pm = pm_ref[...]
        first = jnp.dot(
            pickt_ref[...], jnp.exp2(pm * (1.0 / 16.0)).astype(bf16), preferred_element_type=f32
        )
        some = first > 0.0
        coarse = jnp.where(some, 16.0 * jnp.log2(jnp.where(some, first, 1.0)), 0.0).astype(bf16)
        back = jnp.dot(pick_ref[...], coarse, preferred_element_type=f32)
        second = jnp.dot(
            pickt_ref[...], jnp.exp2((pm - back) * 0.5).astype(bf16), preferred_element_type=f32
        )
        fine = coarse.astype(f32) + 2.0 * jnp.log2(jnp.where(some, second, 1.0))
        shift = fine.astype(bf16)
        factor = jnp.exp2(pm - jnp.dot(pick_ref[...], shift, preferred_element_type=f32))
        sums = ps_ref[...] * factor
        high = sums.astype(bf16)
        low = (sums - high.astype(f32)).astype(bf16)
        den = jnp.dot(pickt_ref[...], high, preferred_element_type=f32)
        den = den + jnp.dot(pickt_ref[...], low, preferred_element_type=f32)
        safe = jnp.where(some, den, 1.0)
        log = pack_log(jnp.where(some, shift.astype(f32) + jnp.log2(safe), -1e30))
        for start in (0, 1152):
            att_ref[:, start + 1024 : start + 1152] = log
        ps_ref[...] = factor
        inverse = 1.0 / safe
        for n in range(heads // 2):
            cols = []
            for j in range(2):
                h = 2 * n + j
                cols.append(
                    (po_ref[:, h * 128 : (h + 1) * 128] * ps_ref[:, h : h + 1]).astype(bf16)
                )
            total = jnp.dot(
                pickt_ref[...], jnp.concatenate(cols, axis=1), preferred_element_type=f32
            )
            for j in range(2):
                h = 2 * n + j
                at = h * 128 + 128 * (h // half)
                att_ref[:, at : at + 128] = (
                    total[:, j * 128 : (j + 1) * 128] * inverse[:, h : h + 1]
                ).astype(bf16)


def local_attention(code, ks, vs, every_query, keys, values):
    total_pages = keys.shape[0] // 32
    steps = 4
    pages = total_pages // steps
    requests, width = every_query.shape
    vmem = pl.BlockSpec(memory_space=pltpu.VMEM)
    f32, bf16 = jnp.float32, jnp.bfloat16
    return pl.pallas_call(
        functools.partial(local_kernel, steps),
        grid=(steps,),
        out_shape=jax.ShapeDtypeStruct((requests, width + 256), bf16),
        in_specs=[vmem, vmem, vmem, vmem]
        + [pl.BlockSpec((pages * 32, 128), lambda t: (t, 0))] * 2,
        out_specs=vmem,
        scratch_shapes=[pltpu.VMEM((8, 128), f32)]
        + [pltpu.VMEM((pages, 128), f32)] * 5
        + [
            pltpu.VMEM((total_pages, requests), bf16),
            pltpu.VMEM((requests, total_pages), bf16),
            pltpu.VMEM((pages // 8, 128, 128), f32),
            pltpu.VMEM((total_pages, width), f32),
            pltpu.VMEM((total_pages, 128), f32),
            pltpu.VMEM((total_pages, 128), f32),
        ],
        compiler_params=pltpu.CompilerParams(vmem_limit_bytes=60 * 1024 * 1024),
        name="local_attention",
    )(code, ks, vs, every_query, keys, values)


def on_device(
    queries,
    k_codes,
    value_quantized_codes,
    key_page_scale,
    value_page_scale,
    lengths,
    page_table,
    out_weight,
):
    head_size = k_codes.shape[-1]
    rows_here = queries.shape[0]
    every_query, code = gather_inputs(lengths, queries.reshape(rows_here, -1), page_table)
    part = local_attention(
        code,
        key_page_scale.T,
        value_page_scale.T,
        every_query.reshape(32 * rows_here, -1),
        k_codes.reshape(-1, head_size),
        value_quantized_codes.reshape(-1, head_size),
    )
    terms = combine(part.reshape(2, 4, 4, rows_here, -1), out_weight)
    return jnp.sum(terms.astype(jnp.float32), axis=0).astype(jnp.bfloat16).T


def solution(mesh):
    in_specs = (
        P("req", "head", None),
        P("req", None, "head", None),
        P("req", None, "head", None),
        P("req", "head"),
        P("req", "head"),
        P("req"),
        P("req", None),
        P("head", "req"),
    )
    out_specs = P(None, ("req", "head"))
    return jax.shard_map(
        on_device, mesh=mesh, in_specs=in_specs, out_specs=out_specs, check_vma=False
    )
```

```python
import functools
import math

import jax
import jax.numpy as jnp
from jax import lax
from jax.experimental import pallas as pl
from jax.experimental.pallas import tpu as pltpu
from jax.sharding import PartitionSpec as P

LOG2E = 1.4426950408889634
UNROLL = 8


def pack_log(value):
    f32, bf16 = jnp.float32, jnp.bfloat16
    high = value.astype(bf16).astype(f32)
    middle = (value - high).astype(bf16).astype(f32)
    low = value - high - middle
    lane = lax.broadcasted_iota(jnp.int32, value.shape, 1)
    low = jnp.where(lane < 48, pltpu.roll(low, 32, 1), 0.0)
    low = jnp.where(lane < 32, pltpu.roll(middle, 16, 1), low)
    return jnp.where(lane < 16, high, low).astype(bf16)


def in_two(value):
    f32, bf16 = jnp.float32, jnp.bfloat16
    high = value.astype(bf16).astype(f32)
    lane = lax.broadcasted_iota(jnp.int32, value.shape, 1)
    return jnp.where(lane < 16, high, pltpu.roll(value - high, 16, 1)).astype(bf16)


def of_two(value):
    return value + pltpu.roll(value, 112, 1)


def page_columns(code_ref, ks_ref, vs_ref, rows_ref, wide_ref, pick_ref, pickt_ref):
    f32, bf16 = jnp.float32, jnp.bfloat16
    requests = pickt_ref.shape[0]
    scale = LOG2E / math.sqrt(128.0)

    def body(b, carry):
        code = code_ref[pl.ds(b, 1), :]
        lanes = pl.ds(pl.multiple_of(b * 128, 128), 128)
        owner_row = jnp.floor(code * (1.0 / 16.0))
        rows_ref[0:1, :] = owner_row
        rows_ref[1:2, :] = code - 16.0 * owner_row + 1.0
        rows_ref[2:4, :] = ks_ref[:, lanes] * scale
        rows_ref[4:6, :] = vs_ref[:, lanes]
        cols = rows_ref[...].T
        for i in range(5):
            wide_ref[i, lanes, :] = jnp.broadcast_to(cols[:, i + 1 : i + 2], (128, 128))
        owner = jnp.broadcast_to(cols[:, 0:1], (128, 128))
        lane = lax.broadcasted_iota(jnp.int32, (128, 128), 1).astype(f32)
        for c in range(requests // 128):
            pick_ref[lanes, c * 128 : (c + 1) * 128] = jnp.where(
                owner == lane + float(c * 128), 1.0, 0.0
            ).astype(bf16)
        row = lax.broadcasted_iota(jnp.int32, (requests, 128), 0).astype(f32)
        pickt_ref[:, lanes] = jnp.where(row == owner_row, 1.0, 0.0).astype(bf16)
        return carry

    lax.fori_loop(0, code_ref.shape[0], body, 0)


def page_queries(q_ref, pick_ref, qs_ref):
    f32, bf16 = jnp.float32, jnp.bfloat16
    tiles = qs_ref.shape[0]

    def body(n, carry):
        cols = pl.ds(pl.multiple_of(n * 256, 256), 256)
        queries = q_ref[:, :, :, :, cols].reshape(pick_ref.shape[1], 256)
        got = jnp.dot(pick_ref[...], queries, preferred_element_type=f32)
        pair = [got[:, j * 128 : (j + 1) * 128].reshape(tiles, 8, 128) for j in range(2)]
        qs_ref[:, pl.ds(pl.multiple_of(n * 16, 16), 16), :] = jnp.concatenate(
            pair, axis=1
        ).astype(bf16)
        return carry

    lax.fori_loop(0, q_ref.shape[-1] // 256, body, 0)


def page_sums(k_ref, v_ref, wide_ref, qs_ref, s_ref, p_ref, po_ref, pm_ref, ps_ref):
    f32, bf16 = jnp.float32, jnp.bfloat16
    heads, half = 16, 8
    groups = qs_ref.shape[0] // UNROLL
    lane = lax.broadcasted_iota(jnp.int32, (8, 256), 1)
    sub = lax.broadcasted_iota(jnp.int32, (8, 256), 0)
    own = (lane >> 5) == sub
    token = ((lane & 31) >> 1).astype(f32)
    far = jnp.float32(1e9)
    tokens = [jnp.where(own & ((lane & 1) == j), token, far) for j in range(2)]
    lane8 = lax.broadcasted_iota(jnp.int32, (8, 128), 1)
    ones = jnp.ones((256, 128), bf16)

    def eight(g):
        return pl.ds(pl.multiple_of(g * 8, 8), 8)

    def kv_rows(g):
        return pl.ds(pl.multiple_of(g * 256, 256), 256)

    def values(u, g):
        both = jnp.concatenate([v_ref[kv_rows(g), :], ones], axis=1)
        out = jnp.dot(p_ref[u], both, preferred_element_type=f32)
        ps = jnp.zeros((8, 128), f32)
        for h in range(heads):
            rows = slice(h * 8, h * 8 + 8)
            po_ref[eight(g), h * 128 : (h + 1) * 128] = (
                out[rows, 0:128] * wide_ref[3 + h // half, eight(g), :]
            )
            ps = jnp.where(lane8 == h, out[rows, 128:256], ps)
        ps_ref[eight(g), :] = ps

    def soften(u, g):
        live = wide_ref[0, eight(g), :]
        live = jnp.concatenate([live, live], axis=1)
        pm = jnp.zeros((8, 128), f32)
        for j in range(2):
            keep = (tokens[j] < live)[None]
            scale = wide_ref[1 + j, eight(g), :]
            scale = jnp.concatenate([scale, scale], axis=1)[None]
            part = s_ref[u, j * 64 : (j + 1) * 64, :].reshape(8, 8, 256)
            part = jnp.where(keep, part * scale, -1e30)
            top = jnp.max(part, axis=2, keepdims=True)
            p_ref[u, j * 64 : (j + 1) * 64, :] = (
                jnp.exp2(part - top).reshape(64, 256).astype(bf16)
            )
            for h in range(8):
                pm = jnp.where(lane8 == j * 8 + h, top[h], pm)
        pm_ref[eight(g), :] = pm

    def scores(u, g):
        s_ref[u] = lax.dot_general(
            qs_ref[g], k_ref[kv_rows(g), :], (((1,), (1,)), ((), ())), preferred_element_type=f32
        )

    def body(i, carry):
        for u in range(UNROLL):
            values(u, jnp.maximum(i - 2, 0) * UNROLL + u)
            soften(u, jnp.clip(i - 1, 0, groups - 1) * UNROLL + u)
            scores(u, jnp.minimum(i, groups - 1) * UNROLL + u)
        return carry

    lax.fori_loop(0, groups + 2, body, 0)


def unpack_log(aux):
    aux = aux.astype(jnp.float32)
    return aux + pltpu.roll(aux, 112, 1) + pltpu.roll(aux, 96, 1)


def request_weights(pick_ref, pickt_ref, pm_ref, ps_ref):
    f32, bf16 = jnp.float32, jnp.bfloat16
    pm = pm_ref[...]
    rough = jnp.dot(
        pickt_ref[...], jnp.exp2(pm * (1.0 / 12.0)).astype(bf16), preferred_element_type=f32
    )
    some = rough > 0.0
    shift = jnp.where(some, 12.0 * jnp.log2(jnp.where(some, rough, 1.0)) - 42.0, 0.0).astype(bf16)
    near = pm - jnp.dot(pick_ref[...], shift, preferred_element_type=f32)
    den = of_two(
        jnp.dot(pickt_ref[...], in_two(ps_ref[...] * jnp.exp2(near)), preferred_element_type=f32)
    )
    log = shift.astype(f32) + jnp.log2(jnp.where(some, den, 1.0))
    log = pack_log(jnp.where(some, log, -1e30))
    back = unpack_log(jnp.dot(pick_ref[...], log, preferred_element_type=f32))
    ps_ref[...] = jnp.exp2(jnp.minimum(pm - back, 64.0))
    return log


def request_sums(n, pickt_ref, po_ref, ps_ref):
    f32, bf16 = jnp.float32, jnp.bfloat16
    cols = [
        (po_ref[:, h * 128 : (h + 1) * 128] * ps_ref[:, h : h + 1]).astype(bf16)
        for h in (2 * n, 2 * n + 1)
    ]
    return jnp.dot(
        pickt_ref[...], jnp.concatenate(cols, axis=1), preferred_element_type=f32
    ).astype(bf16)


MESH = pl.DeviceIdType.MESH


def place():
    me = lax.axis_index("req")
    return lax.div(me, 8), lax.rem(lax.div(me, 2), 4), lax.rem(me, 2)


def off(i, d):
    return lax.rem(i + d + 4, 4)


def chip(x, y, c):
    return {"req": (x * 4 + y) * 2 + c}


class Copies:
    def __init__(self, send_sems, recv_sems):
        self.sems, self.count, self.sent = (send_sems, recv_sems), 0, []

    def send(self, source, target, device, landing):
        pair = (self.sems[0].at[self.count], self.sems[1].at[self.count])
        self.count += 1
        copy = pltpu.make_async_remote_copy(source, target, *pair, device, device_id_type=MESH)
        copy.start()
        self.sent.append(copy)
        return pltpu.make_async_remote_copy(source, landing, *pair, device, device_id_type=MESH)

    def drain(self):
        for copy in self.sent:
            copy.wait_send()


def greet(x, y, c, others=()):
    barrier = pltpu.get_barrier_semaphore()
    peers = [chip(off(x, d), y, c) for d in (1, 2, 3)]
    peers += [chip(x, off(y, d), c) for d in (1, 2, 3)]
    peers += [chip(x, y, 1 - c)] + list(others)
    for peer in peers:
        pl.semaphore_signal(barrier, inc=1, device_id=peer, device_id_type=MESH)
    pl.semaphore_wait(barrier, len(peers))


def gather_first(copies, own, view, x, y, c, halves):
    left, right = halves
    waits = []
    for d in (2, 1, 3):
        waits.append(
            copies.send(
                own.at[:, left], view(x, y, c, left), chip(x, off(y, d), c),
                view(x, off(y, -d), c, left),
            )
        )
        waits.append(
            copies.send(
                own.at[:, right], view(x, y, c, right), chip(off(x, d), y, c),
                view(off(x, -d), y, c, right),
            )
        )
    return waits


def gather_second(copies, view, x, y, c, halves):
    left, right = halves
    every = slice(None)
    waits = []
    for d in (2, 1, 3):
        waits.append(
            copies.send(
                view(x, every, c, left), view(x, every, c, left), chip(off(x, d), y, c),
                view(off(x, -d), every, c, left),
            )
        )
        waits.append(
            copies.send(
                view(every, y, c, right), view(every, y, c, right), chip(x, off(y, d), c),
                view(every, off(y, -d), c, right),
            )
        )
    return waits


def gather_third(copies, waits, view, x, y, c, halves):
    left, right = halves
    every = slice(None)
    twin = chip(x, y, 1 - c)
    last = []

    def pass_on(piece, theirs):
        last.append(copies.send(piece, piece, twin, theirs))

    pass_on(view(x, every, c, left), view(x, every, 1 - c, left))
    pass_on(view(every, y, c, right), view(every, y, 1 - c, right))
    for k, d in enumerate((2, 1, 3)):
        waits[2 * k].wait_recv()
        row = off(x, -d)
        pass_on(view(row, every, c, left), view(row, every, 1 - c, left))
        waits[2 * k + 1].wait_recv()
        row = off(y, -d)
        pass_on(view(every, row, c, right), view(every, row, 1 - c, right))
    return last


def merged(blocks, first_head):
    logs = [unpack_log(b[:, 1024:1152]) for b in blocks]
    top = functools.reduce(jnp.maximum, logs)
    shares = [jnp.exp2(g - top) for g in logs]
    total = functools.reduce(jnp.add, shares)
    inverse = 1.0 / total
    shares = [s * inverse for s in shares]
    columns = []
    for h in range(8):
        at = first_head + h
        columns.append(
            functools.reduce(
                jnp.add,
                [
                    b[:, h * 128 : (h + 1) * 128].astype(jnp.float32) * s[:, at : at + 1]
                    for b, s in zip(blocks, shares)
                ],
            ).astype(jnp.bfloat16)
        )
    return columns, top + jnp.log2(total)


def store_merged(target, index, start, blocks, first_head):
    columns, log = merged(blocks, first_head)
    for h, column in enumerate(columns):
        target[index + (slice(None), slice(start + h * 128, start + (h + 1) * 128))] = column
    if target.shape[-1] != 2048:
        target[index + (slice(None), slice(start + 1024, start + 1152))] = pack_log(log)


def whole_kernel(
    lengths_ref, q_ref, table_ref, ks_ref, vs_ref, k_hbm, v_hbm, weight_ref, out_ref,
    k_ref, v_ref, every_ref, code_ref, table_out, sum_y, sum_c, in_x, in_y, in_c,
    rows_ref, wide_ref, pick_ref, pickt_ref, qs_ref, s_ref, p_ref, po_ref, pm_ref, ps_ref,
    part_ref, twin_in, now, in_left, in_right, left_now, right_now, in_left2, in_right2,
    own, all_ref, terms, turned, load_sems, send_sems, recv_sems,
):
    f32, bf16 = jnp.float32, jnp.bfloat16
    x, y, c = place()
    z = lax.axis_index("head")
    every = slice(None)
    wide = 1152
    left, right = slice(0, wide), slice(wide, 2 * wide)
    rows, width = q_ref.shape
    halves = (slice(0, width // 2), slice(width // 2, width))
    loads = [
        pltpu.make_async_copy(k_hbm, k_ref, load_sems.at[0]),
        pltpu.make_async_copy(v_hbm, v_ref, load_sems.at[1]),
    ]
    for load in loads:
        load.start()

    def view_all(i, j, k, cols):
        return every_ref.at[k, i, j, :, cols]

    greet(x, y, c, [{"head": off(z, d)} for d in (1, 2, 3)])
    copies = Copies(send_sems, recv_sems)
    first = gather_first(copies, q_ref, view_all, x, y, c, halves)
    every_ref[c, x, y] = q_ref[...]
    lane = lax.broadcasted_iota(jnp.int32, (1, 128), 1)
    high_id = lax.broadcasted_iota(jnp.int32, (256, 128), 0)
    low_id = lax.broadcasted_iota(jnp.int32, (128, 128), 0)
    highs, lows = [], []
    for r in range(rows):
        live = jnp.clip(lengths_ref[r] - 16 * lane, 0, 16)
        coded = jnp.where(live > 0, live + 16 * r, 0).astype(f32)
        ids = table_ref[r : r + 1, :]
        highs.append(jnp.where(high_id == (ids >> 7), 1.0, 0.0).astype(bf16))
        lows.append(jnp.where(low_id == (ids & 127), coded, 0.0).astype(bf16))
    found = lax.dot_general(
        jnp.concatenate(highs, axis=1), jnp.concatenate(lows, axis=1),
        (((1,), (1,)), ((), ())), preferred_element_type=f32,
    )
    base = ((c * 16 + x * 4 + y) * 256).astype(f32)
    table_out[...] = jnp.where(found > 0.0, found + base, 0.0).reshape(4, 4, 2, 8, 128)
    got = [
        copies.send(
            table_out.at[off(x, d)], in_x.at[d - 1], chip(off(x, d), y, c), in_x.at[d - 1]
        )
        for d in (2, 1, 3)
    ]
    for wait in first:
        wait.wait_recv()
    second = gather_second(copies, view_all, x, y, c, halves)
    for wait in got:
        wait.wait_recv()
    sum_y[...] = table_out[x] + in_x[0] + in_x[1] + in_x[2]
    got = [
        copies.send(sum_y.at[off(y, d)], in_y.at[d - 1], chip(x, off(y, d), c), in_y.at[d - 1])
        for d in (2, 1, 3)
    ]
    for wait in got:
        wait.wait_recv()
    sum_c[...] = sum_y[y] + in_y[0] + in_y[1] + in_y[2]
    got = copies.send(sum_c.at[1 - c], in_c, chip(x, y, 1 - c), in_c)
    got.wait_recv()
    code_ref[...] = sum_c[c] + in_c[...] - 1.0
    page_columns(code_ref, ks_ref, vs_ref, rows_ref, wide_ref, pick_ref, pickt_ref)
    for k in range(16):
        turned[:, k * 128 : (k + 1) * 128] = weight_ref[k * 128 : (k + 1) * 128, :].T
    for wait in gather_third(copies, second, view_all, x, y, c, halves):
        wait.wait_recv()
    page_queries(every_ref, pick_ref, qs_ref)
    for load in loads:
        load.wait()
    page_sums(k_ref, v_ref, wide_ref, qs_ref, s_ref, p_ref, po_ref, pm_ref, ps_ref)
    log = request_weights(pick_ref, pickt_ref, pm_ref, ps_ref).reshape(2, 4, 4, rows, 128)
    part_ref[:, :, :, :, 1024:1152] = log
    part_ref[:, :, :, :, 1152 + 1024 :] = log
    for n in range(8):
        at = n * 256 + 128 * (n // 4)
        part_ref[:, :, :, :, at : at + 256] = request_sums(
            n, pickt_ref, po_ref, ps_ref
        ).reshape(2, 4, 4, rows, 256)


    twin = [
        copies.send(part_ref.at[1 - c, i], twin_in.at[i], chip(x, y, 1 - c), twin_in.at[i])
        for i in range(4)
    ]
    for i in range(4):
        twin[i].wait_recv()

        def body(j, carry):
            for start, head in ((0, 0), (wide, 8)):
                cols = slice(start, start + wide)
                store_merged(
                    now, (i, j), start, [part_ref[c, i, j, :, cols], twin_in[i, j, :, cols]], head
                )
            return carry

        lax.fori_loop(0, 4, body, 0)
    waits = []
    for d in (2, 1, 3):
        waits.append(
            copies.send(
                now.at[off(x, d), :, :, left], in_left.at[d - 1], chip(off(x, d), y, c),
                in_left.at[d - 1],
            )
        )
        waits.append(
            copies.send(
                now.at[:, off(y, d), :, right], in_right.at[d - 1], chip(x, off(y, d), c),
                in_right.at[d - 1],
            )
        )
    for wait in waits:
        wait.wait_recv()

    def body(j, carry):
        store_merged(
            left_now, (j,), 0, [now[x, j, :, left]] + [in_left[d, j] for d in range(3)], 0
        )
        store_merged(
            right_now, (j,), 0, [now[j, y, :, right]] + [in_right[d, j] for d in range(3)], 8
        )
        return carry

    lax.fori_loop(0, 4, body, 0)
    waits = []
    for d in (2, 1, 3):
        waits.append(
            copies.send(
                left_now.at[off(y, d)], in_left2.at[d - 1], chip(x, off(y, d), c),
                in_left2.at[d - 1],
            )
        )
        waits.append(
            copies.send(
                right_now.at[off(x, d)], in_right2.at[d - 1], chip(off(x, d), y, c),
                in_right2.at[d - 1],
            )
        )
    for wait in waits:
        wait.wait_recv()
    store_merged(own, (), 0, [left_now[y]] + [in_left2[d] for d in range(3)], 0)
    store_merged(own, (), 1024, [right_now[x]] + [in_right2[d] for d in range(3)], 8)

    def view(i, j, k, cols):
        return all_ref.at[i, j, k, :, cols]

    first = gather_first(copies, own, view, x, y, c, halves)
    all_ref[x, y, c] = own[...]
    for wait in first:
        wait.wait_recv()
    second = gather_second(copies, view, x, y, c, halves)
    for wait in gather_third(copies, second, view, x, y, c, halves):
        wait.wait_recv()
    attention = all_ref[...].reshape(512, 2048)
    terms[...] = (
        lax.dot_general(
            turned[...], attention, (((1,), (1,)), ((), ())), preferred_element_type=f32
        )
        .astype(bf16)
        .reshape(4, 64, 512)
    )
    waits = [
        copies.send(terms.at[off(z, d)], out_ref.at[d], {"head": off(z, d)}, out_ref.at[d])
        for d in (2, 1, 3)
    ]
    out_ref[0] = terms[z]
    for wait in waits:
        wait.wait_recv()
    copies.drain()


def whole(lengths, queries, page_table, ks, vs, keys, values, weight):
    f32, bf16 = jnp.float32, jnp.bfloat16
    rows, width = queries.shape
    pages = keys.shape[0] // 32
    requests = 32 * rows
    vmem = pl.BlockSpec(memory_space=pltpu.VMEM)
    hbm = pl.BlockSpec(memory_space=pl.ANY)
    return pl.pallas_call(
        whole_kernel,
        out_shape=jax.ShapeDtypeStruct((4, 64, 512), bf16),
        in_specs=[pl.BlockSpec(memory_space=pltpu.SMEM), vmem, vmem, vmem, vmem, hbm, hbm, vmem],
        out_specs=vmem,
        scratch_shapes=[
            pltpu.VMEM(keys.shape, bf16),
            pltpu.VMEM(keys.shape, bf16),
            pltpu.VMEM((2, 4, 4, rows, width), bf16),
            pltpu.VMEM((8, 128), f32),
            pltpu.VMEM((4, 4, 2, 8, 128), f32),
            pltpu.VMEM((4, 2, 8, 128), f32),
            pltpu.VMEM((2, 8, 128), f32),
            pltpu.VMEM((3, 4, 2, 8, 128), f32),
            pltpu.VMEM((3, 2, 8, 128), f32),
            pltpu.VMEM((8, 128), f32),
            pltpu.VMEM((8, 128), f32),
            pltpu.VMEM((5, pages, 128), f32),
            pltpu.VMEM((pages, requests), bf16),
            pltpu.VMEM((requests, pages), bf16),
            pltpu.VMEM((pages // 8, 128, 128), bf16),
            pltpu.VMEM((UNROLL, 128, 256), f32),
            pltpu.VMEM((UNROLL, 128, 256), bf16),
            pltpu.VMEM((pages, width), f32),
            pltpu.VMEM((pages, 128), f32),
            pltpu.VMEM((pages, 128), f32),
            pltpu.VMEM((2, 4, 4, 16, 2304), bf16),
            pltpu.VMEM((4, 4, 16, 2304), bf16),
            pltpu.VMEM((4, 4, 16, 2304), bf16),
            pltpu.VMEM((3, 4, 16, 1152), bf16),
            pltpu.VMEM((3, 4, 16, 1152), bf16),
            pltpu.VMEM((4, 16, 1152), bf16),
            pltpu.VMEM((4, 16, 1152), bf16),
            pltpu.VMEM((3, 16, 1152), bf16),
            pltpu.VMEM((3, 16, 1152), bf16),
            pltpu.VMEM((16, 2048), bf16),
            pltpu.VMEM((4, 4, 2, 16, 2048), bf16),
            pltpu.VMEM((4, 64, 512), bf16),
            pltpu.VMEM((256, 2048), bf16),
            pltpu.SemaphoreType.DMA((2,)),
            pltpu.SemaphoreType.DMA((66,)),
            pltpu.SemaphoreType.DMA((66,)),
        ],
        compiler_params=pltpu.CompilerParams(
            collective_id=1, has_side_effects=True, vmem_limit_bytes=60 * 1024 * 1024
        ),
        name="whole",
    )(lengths, queries, page_table, ks, vs, keys, values, weight)


def on_device(
    queries,
    k_codes,
    value_quantized_codes,
    key_page_scale,
    value_page_scale,
    lengths,
    page_table,
    out_weight,
):
    head_size = k_codes.shape[-1]
    terms = whole(
        lengths,
        queries.reshape(queries.shape[0], -1),
        page_table,
        key_page_scale.T,
        value_page_scale.T,
        k_codes.reshape(-1, head_size),
        value_quantized_codes.reshape(-1, head_size),
        out_weight,
    )
    return jnp.sum(terms.astype(jnp.float32), axis=0).astype(jnp.bfloat16).T


def solution(mesh):
    in_specs = (
        P("req", "head", None),
        P("req", None, "head", None),
        P("req", None, "head", None),
        P("req", "head"),
        P("req", "head"),
        P("req"),
        P("req", None),
        P("head", "req"),
    )
    out_specs = P(None, ("req", "head"))
    return jax.shard_map(
        on_device, mesh=mesh, in_specs=in_specs, out_specs=out_specs, check_vma=False
    )
```

```python
import functools
import math

import jax
import jax.numpy as jnp
from jax import lax
from jax.experimental import pallas as pl
from jax.experimental.pallas import tpu as pltpu
from jax.sharding import PartitionSpec as P

LOG2E = 1.4426950408889634
UNROLL = 8


def pack_log(value):
    f32, bf16 = jnp.float32, jnp.bfloat16
    high = value.astype(bf16).astype(f32)
    middle = (value - high).astype(bf16).astype(f32)
    low = value - high - middle
    lane = lax.broadcasted_iota(jnp.int32, value.shape, 1)
    low = jnp.where(lane < 48, pltpu.roll(low, 32, 1), 0.0)
    low = jnp.where(lane < 32, pltpu.roll(middle, 16, 1), low)
    return jnp.where(lane < 16, high, low).astype(bf16)


def in_two(value):
    f32, bf16 = jnp.float32, jnp.bfloat16
    high = value.astype(bf16).astype(f32)
    lane = lax.broadcasted_iota(jnp.int32, value.shape, 1)
    return jnp.where(lane < 16, high, pltpu.roll(value - high, 16, 1)).astype(bf16)


def of_two(value):
    return value + pltpu.roll(value, 112, 1)


def page_columns(code_ref, ks_ref, vs_ref, rows_ref, wide_ref, pick_ref, pickt_ref):
    f32, bf16 = jnp.float32, jnp.bfloat16
    requests = pickt_ref.shape[0]
    scale = LOG2E / math.sqrt(128.0)

    def body(b, carry):
        code = code_ref[pl.ds(b, 1), :]
        lanes = pl.ds(pl.multiple_of(b * 128, 128), 128)
        owner_row = jnp.floor(code * (1.0 / 16.0))
        rows_ref[0:1, :] = owner_row
        rows_ref[1:2, :] = code - 16.0 * owner_row + 1.0
        rows_ref[2:4, :] = ks_ref[:, lanes] * scale
        rows_ref[4:6, :] = vs_ref[:, lanes]
        cols = rows_ref[...].T
        for i in range(5):
            wide_ref[i, lanes, :] = jnp.broadcast_to(cols[:, i + 1 : i + 2], (128, 128))
        owner = jnp.broadcast_to(cols[:, 0:1], (128, 128))
        lane = lax.broadcasted_iota(jnp.int32, (128, 128), 1).astype(f32)
        for c in range(requests // 128):
            pick_ref[lanes, c * 128 : (c + 1) * 128] = jnp.where(
                owner == lane + float(c * 128), 1.0, 0.0
            ).astype(bf16)
        row = lax.broadcasted_iota(jnp.int32, (requests, 128), 0).astype(f32)
        pickt_ref[:, lanes] = jnp.where(row == owner_row, 1.0, 0.0).astype(bf16)
        return carry

    lax.fori_loop(0, code_ref.shape[0], body, 0)


def page_queries(q_ref, pick_ref, qs_ref):
    f32, bf16 = jnp.float32, jnp.bfloat16
    tiles = qs_ref.shape[0]

    def body(n, carry):
        cols = pl.ds(pl.multiple_of(n * 256, 256), 256)
        queries = q_ref[:, :, :, :, cols].reshape(pick_ref.shape[1], 256)
        got = jnp.dot(pick_ref[...], queries, preferred_element_type=f32)
        pair = [got[:, j * 128 : (j + 1) * 128].reshape(tiles, 8, 128) for j in range(2)]
        qs_ref[:, pl.ds(pl.multiple_of(n * 16, 16), 16), :] = jnp.concatenate(
            pair, axis=1
        ).astype(bf16)
        return carry

    lax.fori_loop(0, q_ref.shape[-1] // 256, body, 0)


def page_sums(k_ref, v_ref, wide_ref, qs_ref, s_ref, p_ref, po_ref, pm_ref, ps_ref):
    f32, bf16 = jnp.float32, jnp.bfloat16
    heads, half = 16, 8
    groups = qs_ref.shape[0] // UNROLL
    lane = lax.broadcasted_iota(jnp.int32, (8, 256), 1)
    sub = lax.broadcasted_iota(jnp.int32, (8, 256), 0)
    own = (lane >> 5) == sub
    token = ((lane & 31) >> 1).astype(f32)
    far = jnp.float32(1e9)
    tokens = [jnp.where(own & ((lane & 1) == j), token, far) for j in range(2)]
    lane8 = lax.broadcasted_iota(jnp.int32, (8, 128), 1)
    ones = jnp.ones((256, 128), bf16)

    def eight(g):
        return pl.ds(pl.multiple_of(g * 8, 8), 8)

    def kv_rows(g):
        return pl.ds(pl.multiple_of(g * 256, 256), 256)

    def values(u, g):
        both = jnp.concatenate([v_ref[kv_rows(g), :], ones], axis=1)
        out = jnp.dot(p_ref[u], both, preferred_element_type=f32)
        ps = jnp.zeros((8, 128), f32)
        for h in range(heads):
            rows = slice(h * 8, h * 8 + 8)
            po_ref[eight(g), h * 128 : (h + 1) * 128] = (
                out[rows, 0:128] * wide_ref[3 + h // half, eight(g), :]
            )
            ps = jnp.where(lane8 == h, out[rows, 128:256], ps)
        ps_ref[eight(g), :] = ps

    def soften(u, g):
        live = wide_ref[0, eight(g), :]
        live = jnp.concatenate([live, live], axis=1)
        pm = jnp.zeros((8, 128), f32)
        for j in range(2):
            keep = (tokens[j] < live)[None]
            scale = wide_ref[1 + j, eight(g), :]
            scale = jnp.concatenate([scale, scale], axis=1)[None]
            part = s_ref[u, j * 64 : (j + 1) * 64, :].reshape(8, 8, 256)
            part = jnp.where(keep, part * scale, -1e30)
            top = jnp.max(part, axis=2, keepdims=True)
            p_ref[u, j * 64 : (j + 1) * 64, :] = (
                jnp.exp2(part - top).reshape(64, 256).astype(bf16)
            )
            for h in range(8):
                pm = jnp.where(lane8 == j * 8 + h, top[h], pm)
        pm_ref[eight(g), :] = pm

    def scores(u, g):
        s_ref[u] = lax.dot_general(
            qs_ref[g], k_ref[kv_rows(g), :], (((1,), (1,)), ((), ())), preferred_element_type=f32
        )

    def body(i, carry):
        for u in range(UNROLL):
            values(u, jnp.maximum(i - 2, 0) * UNROLL + u)
            soften(u, jnp.clip(i - 1, 0, groups - 1) * UNROLL + u)
            scores(u, jnp.minimum(i, groups - 1) * UNROLL + u)
        return carry

    lax.fori_loop(0, groups + 2, body, 0)


def unpack_log(aux):
    aux = aux.astype(jnp.float32)
    return aux + pltpu.roll(aux, 112, 1) + pltpu.roll(aux, 96, 1)


def request_weights(pick_ref, pickt_ref, pm_ref, ps_ref):
    f32, bf16 = jnp.float32, jnp.bfloat16
    pm = pm_ref[...]
    rough = jnp.dot(
        pickt_ref[...], jnp.exp2(pm * (1.0 / 12.0)).astype(bf16), preferred_element_type=f32
    )
    some = rough > 0.0
    shift = jnp.where(some, 12.0 * jnp.log2(jnp.where(some, rough, 1.0)) - 42.0, 0.0).astype(bf16)
    near = pm - jnp.dot(pick_ref[...], shift, preferred_element_type=f32)
    den = of_two(
        jnp.dot(pickt_ref[...], in_two(ps_ref[...] * jnp.exp2(near)), preferred_element_type=f32)
    )
    log = shift.astype(f32) + jnp.log2(jnp.where(some, den, 1.0))
    log = pack_log(jnp.where(some, log, -1e30))
    back = unpack_log(jnp.dot(pick_ref[...], log, preferred_element_type=f32))
    ps_ref[...] = jnp.exp2(jnp.minimum(pm - back, 64.0))
    return log


def request_sums(n, pickt_ref, po_ref, ps_ref):
    f32, bf16 = jnp.float32, jnp.bfloat16
    cols = [
        (po_ref[:, h * 128 : (h + 1) * 128] * ps_ref[:, h : h + 1]).astype(bf16)
        for h in (2 * n, 2 * n + 1)
    ]
    return jnp.dot(
        pickt_ref[...], jnp.concatenate(cols, axis=1), preferred_element_type=f32
    ).astype(bf16)


MESH = pl.DeviceIdType.MESH


def place():
    me = lax.axis_index("req")
    return lax.div(me, 8), lax.rem(lax.div(me, 2), 4), lax.rem(me, 2)


def off(i, d):
    return lax.rem(i + d + 4, 4)


def chip(x, y, c):
    return {"req": (x * 4 + y) * 2 + c}


class Copies:
    def __init__(self, send_sems, recv_sems):
        self.sems, self.count, self.sent = (send_sems, recv_sems), 0, []

    def send(self, source, target, device, landing):
        pair = (self.sems[0].at[self.count], self.sems[1].at[self.count])
        self.count += 1
        copy = pltpu.make_async_remote_copy(source, target, *pair, device, device_id_type=MESH)
        copy.start()
        self.sent.append(copy)
        return pltpu.make_async_remote_copy(source, landing, *pair, device, device_id_type=MESH)

    def drain(self):
        for copy in self.sent:
            copy.wait_send()


def greet(peers):
    barrier = pltpu.get_barrier_semaphore()
    for peer in peers:
        pl.semaphore_signal(barrier, inc=1, device_id=peer, device_id_type=MESH)
    return lambda: pl.semaphore_wait(barrier, len(peers))


def gather_first(copies, own, view, x, y, c, halves):
    left, right = halves
    waits = []
    for d in (2, 1, 3):
        waits.append(
            copies.send(
                own.at[:, left], view(x, y, c, left), chip(x, off(y, d), c),
                view(x, off(y, -d), c, left),
            )
        )
        waits.append(
            copies.send(
                own.at[:, right], view(x, y, c, right), chip(off(x, d), y, c),
                view(off(x, -d), y, c, right),
            )
        )
    return waits


def gather_second(copies, view, x, y, c, halves):
    left, right = halves
    every = slice(None)
    waits = []
    for d in (2, 1, 3):
        waits.append(
            copies.send(
                view(x, every, c, left), view(x, every, c, left), chip(off(x, d), y, c),
                view(off(x, -d), every, c, left),
            )
        )
        waits.append(
            copies.send(
                view(every, y, c, right), view(every, y, c, right), chip(x, off(y, d), c),
                view(every, off(y, -d), c, right),
            )
        )
    return waits


def pass_own(copies, view, x, y, c, halves):
    left, right = halves
    every = slice(None)
    twin = chip(x, y, 1 - c)
    return [
        copies.send(view(x, every, c, left), view(x, every, c, left), twin,
                    view(x, every, 1 - c, left)),
        copies.send(view(every, y, c, right), view(every, y, c, right), twin,
                    view(every, y, 1 - c, right)),
    ]


def pass_on(copies, waits, view, x, y, c, halves):
    left, right = halves
    every = slice(None)
    twin = chip(x, y, 1 - c)
    last = []
    for k, d in enumerate((2, 1, 3)):
        waits[2 * k].wait_recv()
        i = off(x, -d)
        piece = view(i, every, c, left)
        last.append(copies.send(piece, piece, twin, view(i, every, 1 - c, left)))
        waits[2 * k + 1].wait_recv()
        j = off(y, -d)
        piece = view(every, j, c, right)
        last.append(copies.send(piece, piece, twin, view(every, j, 1 - c, right)))
    return last


def wait_all(waits):
    for wait in waits:
        wait.wait_recv()


def shares_of(logs):
    top = functools.reduce(jnp.maximum, logs)
    shares = [jnp.exp2(g - top) for g in logs]
    total = functools.reduce(jnp.add, shares)
    inverse = 1.0 / total
    return [s * inverse for s in shares], pack_log(top + jnp.log2(total))


def blended(blocks, shares, head):
    terms = [b.astype(jnp.float32) * s[:, head : head + 1] for b, s in zip(blocks, shares)]
    return functools.reduce(jnp.add, terms).astype(jnp.bfloat16)


def whole_kernel(
    lengths_ref, q_ref, table_ref, ks_ref, vs_ref, k_hbm, v_hbm, weight_ref, out_ref,
    k_ref, v_ref, every_ref, code_ref, table_out, sum_y, sum_c, in_x, in_y, in_c,
    rows_ref, wide_ref, pick_ref, pickt_ref, qs_ref, s_ref, p_ref, po_ref, pm_ref, ps_ref,
    part_ref, log_ref, twin_in, log_in, now, now_log, share0,
    in_left, in_right, log_left, log_right, share_left, share_right,
    left_now, right_now, left_log, right_log,
    in_left2, in_right2, log_left2, log_right2, share_left2, share_right2,
    own, all_ref, terms, turned, load_sems, send_sems, recv_sems,
):
    f32, bf16 = jnp.float32, jnp.bfloat16
    x, y, c = place()
    z = lax.axis_index("head")
    rows, width = q_ref.shape
    chunks = [
        (slice(k * 512, k * 512 + 512), slice(1024 + k * 512, 1536 + k * 512)) for k in range(2)
    ]
    loads = [
        pltpu.make_async_copy(k_hbm, k_ref, load_sems.at[0]),
        pltpu.make_async_copy(v_hbm, v_ref, load_sems.at[1]),
    ]
    for load in loads:
        load.start()

    def view_all(i, j, k, cols):
        return every_ref.at[k, i, j, :, cols]

    peers = [chip(off(x, d), y, c) for d in (1, 2, 3)]
    peers += [chip(x, off(y, d), c) for d in (1, 2, 3)]
    peers += [chip(x, y, 1 - c)] + [{"head": off(z, d)} for d in (1, 2, 3)]
    met = greet(peers)
    copies = Copies(send_sems, recv_sems)
    lane = lax.broadcasted_iota(jnp.int32, (1, 128), 1)
    high_id = lax.broadcasted_iota(jnp.int32, (256, 128), 0)
    low_id = lax.broadcasted_iota(jnp.int32, (128, 128), 0)
    highs, lows = [], []
    for r in range(rows):
        live = jnp.clip(lengths_ref[r] - 16 * lane, 0, 16)
        coded = jnp.where(live > 0, live + 16 * r, 0).astype(f32)
        ids = table_ref[r : r + 1, :]
        highs.append(jnp.where(high_id == (ids >> 7), 1.0, 0.0).astype(bf16))
        lows.append(jnp.where(low_id == (ids & 127), coded, 0.0).astype(bf16))
    found = lax.dot_general(
        jnp.concatenate(highs, axis=1), jnp.concatenate(lows, axis=1),
        (((1,), (1,)), ((), ())), preferred_element_type=f32,
    )
    base = ((c * 16 + x * 4 + y) * 256).astype(f32)
    table_out[...] = jnp.where(found > 0.0, found + base, 0.0).reshape(4, 4, 2, 8, 128)
    every_ref[c, x, y] = q_ref[...]
    met()
    got = [
        copies.send(
            table_out.at[off(x, d)], in_x.at[d - 1], chip(off(x, d), y, c), in_x.at[d - 1]
        )
        for d in (2, 1, 3)
    ]
    first = [gather_first(copies, q_ref, view_all, x, y, c, halves) for halves in chunks]
    wait_all(got)
    sum_y[...] = table_out[x] + in_x[0] + in_x[1] + in_x[2]
    got = [
        copies.send(sum_y.at[off(y, d)], in_y.at[d - 1], chip(x, off(y, d), c), in_y.at[d - 1])
        for d in (2, 1, 3)
    ]
    second, third = [], []
    for halves, waits in zip(chunks, first):
        wait_all(waits)
        second.append(gather_second(copies, view_all, x, y, c, halves))
        third += pass_own(copies, view_all, x, y, c, halves)
    wait_all(got)
    sum_c[...] = sum_y[y] + in_y[0] + in_y[1] + in_y[2]
    copies.send(sum_c.at[1 - c], in_c, chip(x, y, 1 - c), in_c).wait_recv()
    code_ref[...] = sum_c[c] + in_c[...] - 1.0
    page_columns(code_ref, ks_ref, vs_ref, rows_ref, wide_ref, pick_ref, pickt_ref)
    for k in range(16):
        turned[:, k * 128 : (k + 1) * 128] = weight_ref[k * 128 : (k + 1) * 128, :].T
    for halves, waits in zip(chunks, second):
        third += pass_on(copies, waits, view_all, x, y, c, halves)
    wait_all(third)
    page_queries(every_ref, pick_ref, qs_ref)
    for load in loads:
        load.wait()
    page_sums(k_ref, v_ref, wide_ref, qs_ref, s_ref, p_ref, po_ref, pm_ref, ps_ref)
    log_ref[...] = request_weights(pick_ref, pickt_ref, pm_ref, ps_ref).reshape(
        2, 4, 4, rows, 128
    )
    twin = chip(x, y, 1 - c)
    log_wait = copies.send(log_ref.at[1 - c], log_in, twin, log_in)

    def sums(*pairs):
        for n in pairs:
            part_ref[:, :, :, :, n * 256 : n * 256 + 256] = request_sums(
                n, pickt_ref, po_ref, ps_ref
            ).reshape(2, 4, 4, rows, 256)

    def to_twin(halves):
        return [
            copies.send(
                part_ref.at[1 - c, :, :, :, cols], twin_in.at[:, :, :, cols], twin,
                twin_in.at[:, :, :, cols],
            )
            for cols in halves
        ]

    def first_shares(j, carry):
        for i in range(4):
            shares, log = shares_of([unpack_log(log_ref[c, i, j]), unpack_log(log_in[i, j])])
            now_log[i, j] = log
            for k in range(2):
                share0[k, i, j] = shares[k]
        return carry

    def across(k, waits):
        wait_all(waits)

        def body(i, carry):
            for j in range(4):
                shares = [share0[0, i, j], share0[1, i, j]]
                for h in range(4):
                    for side in range(2):
                        at = side * 1024 + k * 512 + h * 128
                        cols = slice(at, at + 128)
                        now[i, j, :, cols] = blended(
                            [part_ref[c, i, j, :, cols], twin_in[i, j, :, cols]],
                            shares, side * 8 + k * 4 + h,
                        )
            return carry

        lax.fori_loop(0, 4, body, 0)
        left, right = chunks[k]
        near = chunks[k][0]
        waits, logs = [], []
        for d in (2, 1, 3):
            to_x, to_y = chip(off(x, d), y, c), chip(x, off(y, d), c)
            if k == 0:
                logs.append(
                    copies.send(
                        now_log.at[off(x, d)], log_left.at[d - 1], to_x, log_left.at[d - 1]
                    )
                )
                logs.append(
                    copies.send(
                        now_log.at[:, off(y, d)], log_right.at[d - 1], to_y, log_right.at[d - 1]
                    )
                )
            here = in_left.at[d - 1, :, :, near]
            waits.append(copies.send(now.at[off(x, d), :, :, left], here, to_x, here))
            here = in_right.at[d - 1, :, :, near]
            waits.append(copies.send(now.at[:, off(y, d), :, right], here, to_y, here))
        return waits, logs

    def second_shares(j, carry):
        logs = [now_log[x, j]] + [log_left[d, j] for d in range(3)]
        shares, log = shares_of([unpack_log(g) for g in logs])
        left_log[j] = log
        for k in range(4):
            share_left[k, j] = shares[k]
        logs = [now_log[j, y]] + [log_right[d, j] for d in range(3)]
        shares, log = shares_of([unpack_log(g) for g in logs])
        right_log[j] = log
        for k in range(4):
            share_right[k, j] = shares[k]
        return carry

    def along(k, waits):
        wait_all(waits)

        def body(j, carry):
            shares = [share_left[i, j] for i in range(4)]
            for h in range(4):
                at = k * 512 + h * 128
                cols = slice(at, at + 128)
                blocks = [now[x, j, :, cols]] + [in_left[d, j, :, cols] for d in range(3)]
                left_now[j, :, cols] = blended(blocks, shares, k * 4 + h)
            shares = [share_right[i, j] for i in range(4)]
            for h in range(4):
                at = k * 512 + h * 128
                cols = slice(at, at + 128)
                blocks = [now[j, y, :, 1024 + at : 1152 + at]]
                blocks += [in_right[d, j, :, cols] for d in range(3)]
                right_now[j, :, cols] = blended(blocks, shares, 8 + k * 4 + h)
            return carry

        lax.fori_loop(0, 4, body, 0)
        near = chunks[k][0]
        waits, logs = [], []
        for d in (2, 1, 3):
            to_x, to_y = chip(off(x, d), y, c), chip(x, off(y, d), c)
            if k == 0:
                logs.append(
                    copies.send(
                        left_log.at[off(y, d)], log_left2.at[d - 1], to_y, log_left2.at[d - 1]
                    )
                )
                logs.append(
                    copies.send(
                        right_log.at[off(x, d)], log_right2.at[d - 1], to_x, log_right2.at[d - 1]
                    )
                )
            here = in_left2.at[d - 1, :, near]
            waits.append(copies.send(left_now.at[off(y, d), :, near], here, to_y, here))
            here = in_right2.at[d - 1, :, near]
            waits.append(copies.send(right_now.at[off(x, d), :, near], here, to_x, here))
        return waits, logs

    def third_shares():
        logs = [left_log[y]] + [log_left2[d] for d in range(3)]
        shares, _ = shares_of([unpack_log(g) for g in logs])
        for k in range(4):
            share_left2[k] = shares[k]
        logs = [right_log[x]] + [log_right2[d] for d in range(3)]
        shares, _ = shares_of([unpack_log(g) for g in logs])
        for k in range(4):
            share_right2[k] = shares[k]

    def view(i, j, k, cols):
        return all_ref.at[i, j, k, :, cols]

    def finish(k, waits):
        wait_all(waits)
        for h in range(4):
            at = k * 512 + h * 128
            cols = slice(at, at + 128)
            blocks = [left_now[y, :, cols]] + [in_left2[d, :, cols] for d in range(3)]
            shares = [share_left2[i] for i in range(4)]
            own[:, cols] = blended(blocks, shares, k * 4 + h)
            blocks = [right_now[x, :, cols]] + [in_right2[d, :, cols] for d in range(3)]
            shares = [share_right2[i] for i in range(4)]
            own[:, 1024 + at : 1152 + at] = blended(blocks, shares, 8 + k * 4 + h)
        return gather_first(copies, own, view, x, y, c, chunks[k])

    sums(0, 1, 4, 5)
    twin0 = to_twin(chunks[0])
    sums(2, 3)
    log_wait.wait_recv()
    lax.fori_loop(0, 4, first_shares, 0)
    across0, logs = across(0, twin0)
    sums(6, 7)
    twin1 = to_twin(chunks[1])
    across1, _ = across(1, twin1)
    wait_all(logs)
    lax.fori_loop(0, 4, second_shares, 0)
    along0, logs = along(0, across0)
    along1, _ = along(1, across1)
    wait_all(logs)
    third_shares()
    first = [finish(0, along0), finish(1, along1)]
    all_ref[x, y, c] = own[...]
    second, third = [], []
    for halves, waits in zip(chunks, first):
        wait_all(waits)
        second.append(gather_second(copies, view, x, y, c, halves))
        third += pass_own(copies, view, x, y, c, halves)
    for halves, waits in zip(chunks, second):
        third += pass_on(copies, waits, view, x, y, c, halves)
    wait_all(third)
    attention = all_ref[...].reshape(512, 2048)
    terms[...] = (
        lax.dot_general(
            turned[...], attention, (((1,), (1,)), ((), ())), preferred_element_type=f32
        )
        .astype(bf16)
        .reshape(4, 64, 512)
    )
    waits = [
        copies.send(terms.at[off(z, d)], out_ref.at[d], {"head": off(z, d)}, out_ref.at[d])
        for d in (2, 1, 3)
    ]
    out_ref[0] = terms[z]
    wait_all(waits)
    copies.drain()


def whole(lengths, queries, page_table, ks, vs, keys, values, weight):
    f32, bf16 = jnp.float32, jnp.bfloat16
    rows, width = queries.shape
    pages = keys.shape[0] // 32
    requests = 32 * rows
    vmem = pl.BlockSpec(memory_space=pltpu.VMEM)
    hbm = pl.BlockSpec(memory_space=pl.ANY)
    return pl.pallas_call(
        whole_kernel,
        out_shape=jax.ShapeDtypeStruct((4, 64, 512), bf16),
        in_specs=[pl.BlockSpec(memory_space=pltpu.SMEM), vmem, vmem, vmem, vmem, hbm, hbm, vmem],
        out_specs=vmem,
        scratch_shapes=[
            pltpu.VMEM(keys.shape, bf16),
            pltpu.VMEM(keys.shape, bf16),
            pltpu.VMEM((2, 4, 4, rows, width), bf16),
            pltpu.VMEM((8, 128), f32),
            pltpu.VMEM((4, 4, 2, 8, 128), f32),
            pltpu.VMEM((4, 2, 8, 128), f32),
            pltpu.VMEM((2, 8, 128), f32),
            pltpu.VMEM((3, 4, 2, 8, 128), f32),
            pltpu.VMEM((3, 2, 8, 128), f32),
            pltpu.VMEM((8, 128), f32),
            pltpu.VMEM((8, 128), f32),
            pltpu.VMEM((5, pages, 128), f32),
            pltpu.VMEM((pages, requests), bf16),
            pltpu.VMEM((requests, pages), bf16),
            pltpu.VMEM((pages // 8, 128, 128), bf16),
            pltpu.VMEM((UNROLL, 128, 256), f32),
            pltpu.VMEM((UNROLL, 128, 256), bf16),
            pltpu.VMEM((pages, width), f32),
            pltpu.VMEM((pages, 128), f32),
            pltpu.VMEM((pages, 128), f32),
            pltpu.VMEM((2, 4, 4, 16, 2048), bf16),
            pltpu.VMEM((2, 4, 4, 16, 128), bf16),
            pltpu.VMEM((4, 4, 16, 2048), bf16),
            pltpu.VMEM((4, 4, 16, 128), bf16),
            pltpu.VMEM((4, 4, 16, 2048), bf16),
            pltpu.VMEM((4, 4, 16, 128), bf16),
            pltpu.VMEM((2, 4, 4, 16, 128), f32),
            pltpu.VMEM((3, 4, 16, 1024), bf16),
            pltpu.VMEM((3, 4, 16, 1024), bf16),
            pltpu.VMEM((3, 4, 16, 128), bf16),
            pltpu.VMEM((3, 4, 16, 128), bf16),
            pltpu.VMEM((4, 4, 16, 128), f32),
            pltpu.VMEM((4, 4, 16, 128), f32),
            pltpu.VMEM((4, 16, 1024), bf16),
            pltpu.VMEM((4, 16, 1024), bf16),
            pltpu.VMEM((4, 16, 128), bf16),
            pltpu.VMEM((4, 16, 128), bf16),
            pltpu.VMEM((3, 16, 1024), bf16),
            pltpu.VMEM((3, 16, 1024), bf16),
            pltpu.VMEM((3, 16, 128), bf16),
            pltpu.VMEM((3, 16, 128), bf16),
            pltpu.VMEM((4, 16, 128), f32),
            pltpu.VMEM((4, 16, 128), f32),
            pltpu.VMEM((16, 2048), bf16),
            pltpu.VMEM((4, 4, 2, 16, 2048), bf16),
            pltpu.VMEM((4, 64, 512), bf16),
            pltpu.VMEM((256, 2048), bf16),
            pltpu.SemaphoreType.DMA((2,)),
            pltpu.SemaphoreType.DMA((131,)),
            pltpu.SemaphoreType.DMA((131,)),
        ],
        compiler_params=pltpu.CompilerParams(
            collective_id=1, has_side_effects=True, vmem_limit_bytes=60 * 1024 * 1024
        ),
        name="whole",
    )(lengths, queries, page_table, ks, vs, keys, values, weight)


def on_device(
    queries,
    k_codes,
    value_quantized_codes,
    key_page_scale,
    value_page_scale,
    lengths,
    page_table,
    out_weight,
):
    head_size = k_codes.shape[-1]
    terms = whole(
        lengths,
        queries.reshape(queries.shape[0], -1),
        page_table,
        key_page_scale.T,
        value_page_scale.T,
        k_codes.reshape(-1, head_size),
        value_quantized_codes.reshape(-1, head_size),
        out_weight,
    )
    return jnp.sum(terms.astype(jnp.float32), axis=0).astype(jnp.bfloat16).T


def solution(mesh):
    in_specs = (
        P("req", "head", None),
        P("req", None, "head", None),
        P("req", None, "head", None),
        P("req", "head"),
        P("req", "head"),
        P("req"),
        P("req", None),
        P("head", "req"),
    )
    out_specs = P(None, ("req", "head"))
    return jax.shard_map(
        on_device, mesh=mesh, in_specs=in_specs, out_specs=out_specs, check_vma=False
    )
```

```python
import functools
import math

import jax
import jax.numpy as jnp
from jax import lax
from jax.experimental import pallas as pl
from jax.experimental.pallas import tpu as pltpu
from jax.sharding import PartitionSpec as P

LOG2E = 1.4426950408889634
UNROLL = 8


def pack_log(value):
    f32, bf16 = jnp.float32, jnp.bfloat16
    high = value.astype(bf16).astype(f32)
    middle = (value - high).astype(bf16).astype(f32)
    low = value - high - middle
    lane = lax.broadcasted_iota(jnp.int32, value.shape, 1)
    low = jnp.where(lane < 48, pltpu.roll(low, 32, 1), 0.0)
    low = jnp.where(lane < 32, pltpu.roll(middle, 16, 1), low)
    return jnp.where(lane < 16, high, low).astype(bf16)


def in_two(value):
    f32, bf16 = jnp.float32, jnp.bfloat16
    high = value.astype(bf16).astype(f32)
    lane = lax.broadcasted_iota(jnp.int32, value.shape, 1)
    return jnp.where(lane < 16, high, pltpu.roll(value - high, 16, 1)).astype(bf16)


def of_two(value):
    return value + pltpu.roll(value, 112, 1)


def page_columns(code_ref, ks_ref, vs_ref, rows_ref, wide_ref, pick_ref, pickt_ref):
    f32, bf16 = jnp.float32, jnp.bfloat16
    requests = pickt_ref.shape[0]
    scale = LOG2E / math.sqrt(128.0)

    def body(b, carry):
        code = code_ref[pl.ds(b, 1), :]
        lanes = pl.ds(pl.multiple_of(b * 128, 128), 128)
        owner_row = jnp.floor(code * (1.0 / 16.0))
        rows_ref[0:1, :] = owner_row
        rows_ref[1:2, :] = code - 16.0 * owner_row + 1.0
        rows_ref[2:4, :] = ks_ref[:, lanes] * scale
        rows_ref[4:6, :] = vs_ref[:, lanes]
        cols = rows_ref[...].T
        for i in range(5):
            wide_ref[i, lanes, :] = jnp.broadcast_to(cols[:, i + 1 : i + 2], (128, 128))
        owner = jnp.broadcast_to(cols[:, 0:1], (128, 128))
        lane = lax.broadcasted_iota(jnp.int32, (128, 128), 1).astype(f32)
        for c in range(requests // 128):
            pick_ref[lanes, c * 128 : (c + 1) * 128] = jnp.where(
                owner == lane + float(c * 128), 1.0, 0.0
            ).astype(bf16)
        row = lax.broadcasted_iota(jnp.int32, (requests, 128), 0).astype(f32)
        pickt_ref[:, lanes] = jnp.where(row == owner_row, 1.0, 0.0).astype(bf16)
        return carry

    lax.fori_loop(0, code_ref.shape[0], body, 0)


def page_queries(k, q_ref, pick_ref, qs_ref):
    f32, bf16 = jnp.float32, jnp.bfloat16
    tiles = qs_ref.shape[0]

    def body(i, carry):
        for u in range(2):
            n = i * 4 + 2 * k + u
            cols = pl.ds(pl.multiple_of(n * 256, 256), 256)
            queries = q_ref[:, :, :, :, cols].reshape(pick_ref.shape[1], 256)
            got = jnp.dot(pick_ref[...], queries, preferred_element_type=f32)
            pair = [got[:, j * 128 : (j + 1) * 128].reshape(tiles, 8, 128) for j in range(2)]
            qs_ref[:, pl.ds(pl.multiple_of(n * 16, 16), 16), :] = jnp.concatenate(
                pair, axis=1
            ).astype(bf16)
        return carry

    lax.fori_loop(0, 2, body, 0)


def page_sums(k_ref, v_ref, wide_ref, qs_ref, s_ref, p_ref, po_ref, pm_ref, ps_ref):
    f32, bf16 = jnp.float32, jnp.bfloat16
    heads, half = 16, 8
    groups = qs_ref.shape[0] // UNROLL
    lane = lax.broadcasted_iota(jnp.int32, (8, 256), 1)
    sub = lax.broadcasted_iota(jnp.int32, (8, 256), 0)
    own = (lane >> 5) == sub
    token = ((lane & 31) >> 1).astype(f32)
    far = jnp.float32(1e9)
    tokens = [jnp.where(own & ((lane & 1) == j), token, far) for j in range(2)]
    lane8 = lax.broadcasted_iota(jnp.int32, (8, 128), 1)
    ones = jnp.ones((256, 128), bf16)

    def eight(g):
        return pl.ds(pl.multiple_of(g * 8, 8), 8)

    def kv_rows(g):
        return pl.ds(pl.multiple_of(g * 256, 256), 256)

    def values(u, g):
        both = jnp.concatenate([v_ref[kv_rows(g), :], ones], axis=1)
        out = jnp.dot(p_ref[u], both, preferred_element_type=f32)
        ps = jnp.zeros((8, 128), f32)
        for h in range(heads):
            rows = slice(h * 8, h * 8 + 8)
            po_ref[eight(g), h * 128 : (h + 1) * 128] = (
                out[rows, 0:128] * wide_ref[3 + h // half, eight(g), :]
            )
            ps = jnp.where(lane8 == h, out[rows, 128:256], ps)
        ps_ref[eight(g), :] = ps

    def soften(u, g):
        live = wide_ref[0, eight(g), :]
        live = jnp.concatenate([live, live], axis=1)
        pm = jnp.zeros((8, 128), f32)
        for j in range(2):
            keep = (tokens[j] < live)[None]
            scale = wide_ref[1 + j, eight(g), :]
            scale = jnp.concatenate([scale, scale], axis=1)[None]
            part = s_ref[u, j * 64 : (j + 1) * 64, :].reshape(8, 8, 256)
            part = jnp.where(keep, part * scale, -1e30)
            top = jnp.max(part, axis=2, keepdims=True)
            p_ref[u, j * 64 : (j + 1) * 64, :] = (
                jnp.exp2(part - top).reshape(64, 256).astype(bf16)
            )
            for h in range(8):
                pm = jnp.where(lane8 == j * 8 + h, top[h], pm)
        pm_ref[eight(g), :] = pm

    def scores(u, g):
        s_ref[u] = lax.dot_general(
            qs_ref[g], k_ref[kv_rows(g), :], (((1,), (1,)), ((), ())), preferred_element_type=f32
        )

    def body(i, carry):
        for u in range(UNROLL):
            values(u, jnp.maximum(i - 2, 0) * UNROLL + u)
            soften(u, jnp.clip(i - 1, 0, groups - 1) * UNROLL + u)
            scores(u, jnp.minimum(i, groups - 1) * UNROLL + u)
        return carry

    lax.fori_loop(0, groups + 2, body, 0)


def unpack_log(aux):
    aux = aux.astype(jnp.float32)
    return aux + pltpu.roll(aux, 112, 1) + pltpu.roll(aux, 96, 1)


def request_weights(pick_ref, pickt_ref, pm_ref, ps_ref):
    f32, bf16 = jnp.float32, jnp.bfloat16
    pm = pm_ref[...]
    rough = jnp.dot(
        pickt_ref[...], jnp.exp2(pm * (1.0 / 12.0)).astype(bf16), preferred_element_type=f32
    )
    some = rough > 0.0
    shift = jnp.where(some, 12.0 * jnp.log2(jnp.where(some, rough, 1.0)) - 42.0, 0.0).astype(bf16)
    near = pm - jnp.dot(pick_ref[...], shift, preferred_element_type=f32)
    den = of_two(
        jnp.dot(pickt_ref[...], in_two(ps_ref[...] * jnp.exp2(near)), preferred_element_type=f32)
    )
    log = shift.astype(f32) + jnp.log2(jnp.where(some, den, 1.0))
    log = pack_log(jnp.where(some, log, -1e30))
    back = unpack_log(jnp.dot(pick_ref[...], log, preferred_element_type=f32))
    ps_ref[...] = jnp.exp2(jnp.minimum(pm - back, 64.0))
    return log


def request_sums(n, pickt_ref, po_ref, ps_ref):
    f32, bf16 = jnp.float32, jnp.bfloat16
    cols = [
        (po_ref[:, h * 128 : (h + 1) * 128] * ps_ref[:, h : h + 1]).astype(bf16)
        for h in (2 * n, 2 * n + 1)
    ]
    return jnp.dot(
        pickt_ref[...], jnp.concatenate(cols, axis=1), preferred_element_type=f32
    ).astype(bf16)


MESH = pl.DeviceIdType.MESH


def place():
    me = lax.axis_index("req")
    return lax.div(me, 8), lax.rem(lax.div(me, 2), 4), lax.rem(me, 2)


def off(i, d):
    return lax.rem(i + d + 4, 4)


def chip(x, y, c):
    return {"req": (x * 4 + y) * 2 + c}


class Copies:
    def __init__(self, send_sems, recv_sems):
        self.sems, self.count, self.sent = (send_sems, recv_sems), 0, []

    def send(self, source, target, device, landing):
        pair = (self.sems[0].at[self.count], self.sems[1].at[self.count])
        self.count += 1
        copy = pltpu.make_async_remote_copy(source, target, *pair, device, device_id_type=MESH)
        copy.start()
        self.sent.append(copy)
        return pltpu.make_async_remote_copy(source, landing, *pair, device, device_id_type=MESH)

    def drain(self):
        for copy in self.sent:
            copy.wait_send()


def greet(peers):
    barrier = pltpu.get_barrier_semaphore()
    for peer in peers:
        pl.semaphore_signal(barrier, inc=1, device_id=peer, device_id_type=MESH)
    return lambda: pl.semaphore_wait(barrier, len(peers))


def gather_first(copies, own, view, x, y, c, halves):
    left, right = halves
    waits = []
    for d in (2, 1, 3):
        waits.append(
            copies.send(
                own.at[:, left], view(x, y, c, left), chip(x, off(y, d), c),
                view(x, off(y, -d), c, left),
            )
        )
        waits.append(
            copies.send(
                own.at[:, right], view(x, y, c, right), chip(off(x, d), y, c),
                view(off(x, -d), y, c, right),
            )
        )
    return waits


def gather_second(copies, view, x, y, c, halves):
    left, right = halves
    every = slice(None)
    waits = []
    for d in (2, 1, 3):
        waits.append(
            copies.send(
                view(x, every, c, left), view(x, every, c, left), chip(off(x, d), y, c),
                view(off(x, -d), every, c, left),
            )
        )
        waits.append(
            copies.send(
                view(every, y, c, right), view(every, y, c, right), chip(x, off(y, d), c),
                view(every, off(y, -d), c, right),
            )
        )
    return waits


def pass_own(copies, view, x, y, c, halves):
    left, right = halves
    every = slice(None)
    twin = chip(x, y, 1 - c)
    return [
        copies.send(view(x, every, c, left), view(x, every, c, left), twin,
                    view(x, every, 1 - c, left)),
        copies.send(view(every, y, c, right), view(every, y, c, right), twin,
                    view(every, y, 1 - c, right)),
    ]


def pass_on(copies, waits, view, x, y, c, halves):
    left, right = halves
    every = slice(None)
    twin = chip(x, y, 1 - c)
    last = []
    for k, d in enumerate((2, 1, 3)):
        waits[2 * k].wait_recv()
        i = off(x, -d)
        piece = view(i, every, c, left)
        last.append(copies.send(piece, piece, twin, view(i, every, 1 - c, left)))
        waits[2 * k + 1].wait_recv()
        j = off(y, -d)
        piece = view(every, j, c, right)
        last.append(copies.send(piece, piece, twin, view(every, j, 1 - c, right)))
    return last


def wait_all(waits):
    for wait in waits:
        wait.wait_recv()


def shares_of(logs):
    top = functools.reduce(jnp.maximum, logs)
    shares = [jnp.exp2(g - top) for g in logs]
    total = functools.reduce(jnp.add, shares)
    inverse = 1.0 / total
    return [s * inverse for s in shares], pack_log(top + jnp.log2(total))


def blended(blocks, shares, head):
    terms = [b.astype(jnp.float32) * s[:, head : head + 1] for b, s in zip(blocks, shares)]
    return functools.reduce(jnp.add, terms).astype(jnp.bfloat16)


def whole_kernel(
    lengths_ref, queries_ref, table_ref, ks_ref, vs_ref, k_hbm, v_hbm, weight_hbm, out_ref,
    k_ref, v_ref, weight_ref, wide_q, q_ref, every_ref, code_ref, table_out, sum_y, sum_c, in_x, in_y, in_c,
    rows_ref, wide_ref, pick_ref, pickt_ref, qs_ref, s_ref, p_ref, po_ref, pm_ref, ps_ref,
    part_ref, log_ref, twin_in, log_in, now, now_log, share0,
    in_left, in_right, log_left, log_right, share_left, share_right,
    left_now, right_now, left_log, right_log,
    in_left2, in_right2, log_left2, log_right2, share_left2, share_right2,
    own, all_ref, half_terms, terms, terms_in, turned, load_sems, send_sems, recv_sems,
):
    f32, bf16 = jnp.float32, jnp.bfloat16
    x, y, c = place()
    z = lax.axis_index("head")
    rows = q_ref.shape[0]
    chunks = [
        (slice(k * 512, k * 512 + 512), slice(1024 + k * 512, 1536 + k * 512)) for k in range(2)
    ]
    loads = [
        pltpu.make_async_copy(k_hbm, k_ref, load_sems.at[0]),
        pltpu.make_async_copy(v_hbm, v_ref, load_sems.at[1]),
    ]
    load_weight = pltpu.make_async_copy(weight_hbm, weight_ref, load_sems.at[2])
    load_weight.start()
    for load in loads:
        load.start()

    def view_all(i, j, k, cols):
        return every_ref.at[k, i, j, :, cols]

    peers = [chip(off(x, d), y, c) for d in (1, 2, 3)]
    peers += [chip(x, off(y, d), c) for d in (1, 2, 3)]
    peers += [chip(x, y, 1 - c)] + [{"head": off(z, d)} for d in (1, 2, 3)]
    met = greet(peers)
    wide_q[...] = queries_ref[...].astype(f32).reshape(wide_q.shape)
    for h in range(16):
        q_ref[:, h * 128 : (h + 1) * 128] = wide_q[pl.ds(h, rows, stride=16), :].astype(bf16)
    copies = Copies(send_sems, recv_sems)
    lane = lax.broadcasted_iota(jnp.int32, (1, 128), 1)
    high_id = lax.broadcasted_iota(jnp.int32, (256, 128), 0)
    low_id = lax.broadcasted_iota(jnp.int32, (128, 128), 0)
    highs, lows = [], []
    for r in range(rows):
        live = jnp.clip(lengths_ref[r] - 16 * lane, 0, 16)
        coded = jnp.where(live > 0, live + 16 * r, 0).astype(f32)
        ids = table_ref[r : r + 1, :]
        highs.append(jnp.where(high_id == (ids >> 7), 1.0, 0.0).astype(bf16))
        lows.append(jnp.where(low_id == (ids & 127), coded, 0.0).astype(bf16))
    found = lax.dot_general(
        jnp.concatenate(highs, axis=1), jnp.concatenate(lows, axis=1),
        (((1,), (1,)), ((), ())), preferred_element_type=f32,
    )
    base = ((c * 16 + x * 4 + y) * 256).astype(f32)
    table_out[...] = jnp.where(found > 0.0, found + base, 0.0).reshape(4, 4, 2, 8, 128)
    every_ref[c, x, y] = q_ref[...]
    met()
    got = [
        copies.send(
            table_out.at[off(x, d)], in_x.at[d - 1], chip(off(x, d), y, c), in_x.at[d - 1]
        )
        for d in (2, 1, 3)
    ]
    first = [gather_first(copies, q_ref, view_all, x, y, c, halves) for halves in chunks]
    wait_all(got)
    sum_y[...] = table_out[x] + in_x[0] + in_x[1] + in_x[2]
    got = [
        copies.send(sum_y.at[off(y, d)], in_y.at[d - 1], chip(x, off(y, d), c), in_y.at[d - 1])
        for d in (2, 1, 3)
    ]
    second, third = [], []
    for halves, waits in zip(chunks, first):
        wait_all(waits)
        second.append(gather_second(copies, view_all, x, y, c, halves))
        third.append(pass_own(copies, view_all, x, y, c, halves))
    wait_all(got)
    sum_c[...] = sum_y[y] + in_y[0] + in_y[1] + in_y[2]
    copies.send(sum_c.at[1 - c], in_c, chip(x, y, 1 - c), in_c).wait_recv()
    code_ref[...] = sum_c[c] + in_c[...] - 1.0
    page_columns(code_ref, ks_ref, vs_ref, rows_ref, wide_ref, pick_ref, pickt_ref)
    load_weight.wait()
    for k in range(16):
        turned[:, k * 128 : (k + 1) * 128] = weight_ref[k * 128 : (k + 1) * 128, :].T
    third[0] += pass_on(copies, second[0], view_all, x, y, c, chunks[0])
    wait_all(third[0])
    page_queries(0, every_ref, pick_ref, qs_ref)
    third[1] += pass_on(copies, second[1], view_all, x, y, c, chunks[1])
    wait_all(third[1])
    page_queries(1, every_ref, pick_ref, qs_ref)
    for load in loads:
        load.wait()
    page_sums(k_ref, v_ref, wide_ref, qs_ref, s_ref, p_ref, po_ref, pm_ref, ps_ref)
    log_ref[...] = request_weights(pick_ref, pickt_ref, pm_ref, ps_ref).reshape(
        2, 4, 4, rows, 128
    )
    twin = chip(x, y, 1 - c)
    log_wait = copies.send(log_ref.at[1 - c], log_in, twin, log_in)

    def sums(*pairs):
        for n in pairs:
            part_ref[:, :, :, :, n * 256 : n * 256 + 256] = request_sums(
                n, pickt_ref, po_ref, ps_ref
            ).reshape(2, 4, 4, rows, 256)

    def to_twin(halves):
        return [
            copies.send(
                part_ref.at[1 - c, :, :, :, cols], twin_in.at[:, :, :, cols], twin,
                twin_in.at[:, :, :, cols],
            )
            for cols in halves
        ]

    def first_shares(j, carry):
        for i in range(4):
            shares, log = shares_of([unpack_log(log_ref[c, i, j]), unpack_log(log_in[i, j])])
            now_log[i, j] = log
            for k in range(2):
                share0[k, i, j] = shares[k]
        return carry

    def across(k, waits):
        wait_all(waits)

        def body(i, carry):
            for j in range(4):
                shares = [share0[0, i, j], share0[1, i, j]]
                for h in range(4):
                    for side in range(2):
                        at = side * 1024 + k * 512 + h * 128
                        cols = slice(at, at + 128)
                        now[i, j, :, cols] = blended(
                            [part_ref[c, i, j, :, cols], twin_in[i, j, :, cols]],
                            shares, side * 8 + k * 4 + h,
                        )
            return carry

        lax.fori_loop(0, 4, body, 0)
        left, right = chunks[k]
        near = chunks[k][0]
        waits, logs = [], []
        for d in (2, 1, 3):
            to_x, to_y = chip(off(x, d), y, c), chip(x, off(y, d), c)
            if k == 0:
                logs.append(
                    copies.send(
                        now_log.at[off(x, d)], log_left.at[d - 1], to_x, log_left.at[d - 1]
                    )
                )
                logs.append(
                    copies.send(
                        now_log.at[:, off(y, d)], log_right.at[d - 1], to_y, log_right.at[d - 1]
                    )
                )
            here = in_left.at[d - 1, :, :, near]
            waits.append(copies.send(now.at[off(x, d), :, :, left], here, to_x, here))
            here = in_right.at[d - 1, :, :, near]
            waits.append(copies.send(now.at[:, off(y, d), :, right], here, to_y, here))
        return waits, logs

    def second_shares(j, carry):
        logs = [now_log[x, j]] + [log_left[d, j] for d in range(3)]
        shares, log = shares_of([unpack_log(g) for g in logs])
        left_log[j] = log
        for k in range(4):
            share_left[k, j] = shares[k]
        logs = [now_log[j, y]] + [log_right[d, j] for d in range(3)]
        shares, log = shares_of([unpack_log(g) for g in logs])
        right_log[j] = log
        for k in range(4):
            share_right[k, j] = shares[k]
        return carry

    def along(k, waits):
        wait_all(waits)

        def body(j, carry):
            shares = [share_left[i, j] for i in range(4)]
            for h in range(4):
                at = k * 512 + h * 128
                cols = slice(at, at + 128)
                blocks = [now[x, j, :, cols]] + [in_left[d, j, :, cols] for d in range(3)]
                left_now[j, :, cols] = blended(blocks, shares, k * 4 + h)
            shares = [share_right[i, j] for i in range(4)]
            for h in range(4):
                at = k * 512 + h * 128
                cols = slice(at, at + 128)
                blocks = [now[j, y, :, 1024 + at : 1152 + at]]
                blocks += [in_right[d, j, :, cols] for d in range(3)]
                right_now[j, :, cols] = blended(blocks, shares, 8 + k * 4 + h)
            return carry

        lax.fori_loop(0, 4, body, 0)
        near = chunks[k][0]
        waits, logs = [], []
        for d in (2, 1, 3):
            to_x, to_y = chip(off(x, d), y, c), chip(x, off(y, d), c)
            if k == 0:
                logs.append(
                    copies.send(
                        left_log.at[off(y, d)], log_left2.at[d - 1], to_y, log_left2.at[d - 1]
                    )
                )
                logs.append(
                    copies.send(
                        right_log.at[off(x, d)], log_right2.at[d - 1], to_x, log_right2.at[d - 1]
                    )
                )
            here = in_left2.at[d - 1, :, near]
            waits.append(copies.send(left_now.at[off(y, d), :, near], here, to_y, here))
            here = in_right2.at[d - 1, :, near]
            waits.append(copies.send(right_now.at[off(x, d), :, near], here, to_x, here))
        return waits, logs

    def third_shares():
        logs = [left_log[y]] + [log_left2[d] for d in range(3)]
        shares, _ = shares_of([unpack_log(g) for g in logs])
        for k in range(4):
            share_left2[k] = shares[k]
        logs = [right_log[x]] + [log_right2[d] for d in range(3)]
        shares, _ = shares_of([unpack_log(g) for g in logs])
        for k in range(4):
            share_right2[k] = shares[k]

    def view(i, j, k, cols):
        return all_ref.at[i, j, k, :, cols]

    def finish(k, waits):
        wait_all(waits)
        for h in range(4):
            at = k * 512 + h * 128
            cols = slice(at, at + 128)
            blocks = [left_now[y, :, cols]] + [in_left2[d, :, cols] for d in range(3)]
            shares = [share_left2[i] for i in range(4)]
            own[:, cols] = blended(blocks, shares, k * 4 + h)
            blocks = [right_now[x, :, cols]] + [in_right2[d, :, cols] for d in range(3)]
            shares = [share_right2[i] for i in range(4)]
            own[:, 1024 + at : 1152 + at] = blended(blocks, shares, 8 + k * 4 + h)
        return gather_first(copies, own, view, x, y, c, chunks[k])

    sums(0, 1, 4, 5)
    twin0 = to_twin(chunks[0])
    sums(2, 3)
    log_wait.wait_recv()
    lax.fori_loop(0, 4, first_shares, 0)
    across0, logs = across(0, twin0)
    sums(6, 7)
    twin1 = to_twin(chunks[1])
    across1, _ = across(1, twin1)
    wait_all(logs)
    lax.fori_loop(0, 4, second_shares, 0)
    along0, logs = along(0, across0)
    along1, _ = along(1, across1)
    wait_all(logs)
    third_shares()
    first = [finish(0, along0), finish(1, along1)]
    all_ref[x, y, c] = own[...]
    second, third = [], []
    for halves, waits in zip(chunks, first):
        wait_all(waits)
        second.append(gather_second(copies, view, x, y, c, halves))
        third.append(pass_own(copies, view, x, y, c, halves))

    def product(k, i):
        total = jnp.zeros((256, 256), f32)
        for cols in chunks[k]:
            total = total + lax.dot_general(
                turned[:, cols], all_ref[2 * i : 2 * i + 2, :, :, :, cols].reshape(256, 512),
                (((1,), (1,)), ((), ())), preferred_element_type=f32,
            )
        return total

    third[0] += pass_on(copies, second[0], view, x, y, c, chunks[0])
    wait_all(third[0])
    for i in range(2):
        half_terms[:, i * 256 : i * 256 + 256] = product(0, i)
    third[1] += pass_on(copies, second[1], view, x, y, c, chunks[1])
    wait_all(third[1])
    waits = []
    for i in range(2):
        cols = slice(i * 256, i * 256 + 256)
        terms[:, :, cols] = (
            (half_terms[:, cols] + product(1, i)).astype(bf16).reshape(4, 64, 256)
        )
        for d in (2, 1, 3):
            here = terms_in.at[d - 1, :, cols]
            waits.append(
                copies.send(terms.at[off(z, d), :, cols], here, {"head": off(z, d)}, here)
            )
    wait_all(waits)
    total = terms[z].astype(f32)
    for d in range(3):
        total = total + terms_in[d].astype(f32)
    out_ref[...] = total.astype(bf16)
    copies.drain()


def whole(lengths, queries, page_table, ks, vs, keys, values, weight):
    f32, bf16 = jnp.float32, jnp.bfloat16
    rows = queries.shape[0]
    width = queries.shape[1] * queries.shape[2]
    pages = keys.shape[0] // 32
    requests = 32 * rows
    vmem = pl.BlockSpec(memory_space=pltpu.VMEM)
    hbm = pl.BlockSpec(memory_space=pl.ANY)
    return pl.pallas_call(
        whole_kernel,
        out_shape=jax.ShapeDtypeStruct((64, 512), bf16),
        in_specs=[pl.BlockSpec(memory_space=pltpu.SMEM), vmem, vmem, vmem, vmem, hbm, hbm, hbm],
        out_specs=vmem,
        scratch_shapes=[
            pltpu.VMEM(keys.shape, bf16),
            pltpu.VMEM(keys.shape, bf16),
            pltpu.VMEM(weight.shape, bf16),
            pltpu.VMEM((rows * 16, 128), f32),
            pltpu.VMEM((rows, width), bf16),
            pltpu.VMEM((2, 4, 4, rows, width), bf16),
            pltpu.VMEM((8, 128), f32),
            pltpu.VMEM((4, 4, 2, 8, 128), f32),
            pltpu.VMEM((4, 2, 8, 128), f32),
            pltpu.VMEM((2, 8, 128), f32),
            pltpu.VMEM((3, 4, 2, 8, 128), f32),
            pltpu.VMEM((3, 2, 8, 128), f32),
            pltpu.VMEM((8, 128), f32),
            pltpu.VMEM((8, 128), f32),
            pltpu.VMEM((5, pages, 128), f32),
            pltpu.VMEM((pages, requests), bf16),
            pltpu.VMEM((requests, pages), bf16),
            pltpu.VMEM((pages // 8, 128, 128), bf16),
            pltpu.VMEM((UNROLL, 128, 256), f32),
            pltpu.VMEM((UNROLL, 128, 256), bf16),
            pltpu.VMEM((pages, width), f32),
            pltpu.VMEM((pages, 128), f32),
            pltpu.VMEM((pages, 128), f32),
            pltpu.VMEM((2, 4, 4, 16, 2048), bf16),
            pltpu.VMEM((2, 4, 4, 16, 128), bf16),
            pltpu.VMEM((4, 4, 16, 2048), bf16),
            pltpu.VMEM((4, 4, 16, 128), bf16),
            pltpu.VMEM((4, 4, 16, 2048), bf16),
            pltpu.VMEM((4, 4, 16, 128), bf16),
            pltpu.VMEM((2, 4, 4, 16, 128), f32),
            pltpu.VMEM((3, 4, 16, 1024), bf16),
            pltpu.VMEM((3, 4, 16, 1024), bf16),
            pltpu.VMEM((3, 4, 16, 128), bf16),
            pltpu.VMEM((3, 4, 16, 128), bf16),
            pltpu.VMEM((4, 4, 16, 128), f32),
            pltpu.VMEM((4, 4, 16, 128), f32),
            pltpu.VMEM((4, 16, 1024), bf16),
            pltpu.VMEM((4, 16, 1024), bf16),
            pltpu.VMEM((4, 16, 128), bf16),
            pltpu.VMEM((4, 16, 128), bf16),
            pltpu.VMEM((3, 16, 1024), bf16),
            pltpu.VMEM((3, 16, 1024), bf16),
            pltpu.VMEM((3, 16, 128), bf16),
            pltpu.VMEM((3, 16, 128), bf16),
            pltpu.VMEM((4, 16, 128), f32),
            pltpu.VMEM((4, 16, 128), f32),
            pltpu.VMEM((16, 2048), bf16),
            pltpu.VMEM((4, 4, 2, 16, 2048), bf16),
            pltpu.VMEM((256, 512), f32),
            pltpu.VMEM((4, 64, 512), bf16),
            pltpu.VMEM((3, 64, 512), bf16),
            pltpu.VMEM((256, 2048), bf16),
            pltpu.SemaphoreType.DMA((3,)),
            pltpu.SemaphoreType.DMA((134,)),
            pltpu.SemaphoreType.DMA((134,)),
        ],
        compiler_params=pltpu.CompilerParams(
            collective_id=1, has_side_effects=True, vmem_limit_bytes=60 * 1024 * 1024
        ),
        name="whole",
    )(lengths, queries, page_table, ks, vs, keys, values, weight)


def on_device(
    queries,
    k_codes,
    value_quantized_codes,
    key_page_scale,
    value_page_scale,
    lengths,
    page_table,
    out_weight,
):
    head_size = k_codes.shape[-1]
    return whole(
        lengths,
        queries,
        page_table,
        key_page_scale.T,
        value_page_scale.T,
        k_codes.reshape(-1, head_size),
        value_quantized_codes.reshape(-1, head_size),
        out_weight,
    ).T


def solution(mesh):
    in_specs = (
        P("req", "head", None),
        P("req", None, "head", None),
        P("req", None, "head", None),
        P("req", "head"),
        P("req", "head"),
        P("req"),
        P("req", None),
        P("head", "req"),
    )
    out_specs = P(None, ("req", "head"))
    return jax.shard_map(
        on_device, mesh=mesh, in_specs=in_specs, out_specs=out_specs, check_vma=False
    )
```

```python
import functools
import math

import jax
import jax.numpy as jnp
from jax import lax
from jax.experimental import pallas as pl
from jax.experimental.pallas import tpu as pltpu
from jax.sharding import PartitionSpec as P

LOG2E = 1.4426950408889634
UNROLL = 8


def pack_log(value):
    f32, bf16 = jnp.float32, jnp.bfloat16
    high = value.astype(bf16).astype(f32)
    middle = (value - high).astype(bf16).astype(f32)
    low = value - high - middle
    lane = lax.broadcasted_iota(jnp.int32, value.shape, 1)
    low = jnp.where(lane < 48, pltpu.roll(low, 32, 1), 0.0)
    low = jnp.where(lane < 32, pltpu.roll(middle, 16, 1), low)
    return jnp.where(lane < 16, high, low).astype(bf16)


def in_two(value):
    f32, bf16 = jnp.float32, jnp.bfloat16
    high = value.astype(bf16).astype(f32)
    lane = lax.broadcasted_iota(jnp.int32, value.shape, 1)
    return jnp.where(lane < 16, high, pltpu.roll(value - high, 16, 1)).astype(bf16)


def of_two(value):
    return value + pltpu.roll(value, 112, 1)


def page_columns(code_ref, ks_ref, vs_ref, rows_ref, wide_ref, pick_ref, pickt_ref):
    f32, bf16 = jnp.float32, jnp.bfloat16
    requests = pickt_ref.shape[0]
    scale = LOG2E / math.sqrt(128.0)

    def body(b, carry):
        code = code_ref[pl.ds(b, 1), :]
        lanes = pl.ds(pl.multiple_of(b * 128, 128), 128)
        owner_row = jnp.floor(code * (1.0 / 16.0))
        rows_ref[0:1, :] = owner_row
        rows_ref[1:2, :] = code - 16.0 * owner_row + 1.0
        rows_ref[2:4, :] = ks_ref[:, lanes] * scale
        rows_ref[4:6, :] = vs_ref[:, lanes]
        cols = rows_ref[...].T
        for i in range(5):
            wide_ref[i, lanes, :] = jnp.broadcast_to(cols[:, i + 1 : i + 2], (128, 128))
        owner = jnp.broadcast_to(cols[:, 0:1], (128, 128))
        lane = lax.broadcasted_iota(jnp.int32, (128, 128), 1).astype(f32)
        for c in range(requests // 128):
            pick_ref[lanes, c * 128 : (c + 1) * 128] = jnp.where(
                owner == lane + float(c * 128), 1.0, 0.0
            ).astype(bf16)
        row = lax.broadcasted_iota(jnp.int32, (requests, 128), 0).astype(f32)
        pickt_ref[:, lanes] = jnp.where(row == owner_row, 1.0, 0.0).astype(bf16)
        return carry

    lax.fori_loop(0, code_ref.shape[0], body, 0)


def page_queries(k, q_ref, pick_ref, qs_ref):
    f32, bf16 = jnp.float32, jnp.bfloat16
    tiles = qs_ref.shape[0]

    def body(i, carry):
        for u in range(2):
            n = i * 4 + 2 * k + u
            cols = pl.ds(pl.multiple_of(n * 256, 256), 256)
            queries = q_ref[:, :, :, :, cols].reshape(pick_ref.shape[1], 256)
            got = jnp.dot(pick_ref[...], queries, preferred_element_type=f32)
            pair = [got[:, j * 128 : (j + 1) * 128].reshape(tiles, 8, 128) for j in range(2)]
            qs_ref[:, pl.ds(pl.multiple_of(n * 16, 16), 16), :] = jnp.concatenate(
                pair, axis=1
            ).astype(bf16)
        return carry

    lax.fori_loop(0, 2, body, 0)


def page_sums(k_ref, v_ref, wide_ref, qs_ref, s_ref, p_ref, po_ref, pm_ref, ps_ref):
    f32, bf16 = jnp.float32, jnp.bfloat16
    heads, half = 16, 8
    groups = qs_ref.shape[0] // UNROLL
    lane = lax.broadcasted_iota(jnp.int32, (8, 256), 1)
    sub = lax.broadcasted_iota(jnp.int32, (8, 256), 0)
    own = (lane >> 5) == sub
    token = ((lane & 31) >> 1).astype(f32)
    far = jnp.float32(1e9)
    tokens = [jnp.where(own & ((lane & 1) == j), token, far) for j in range(2)]
    lane8 = lax.broadcasted_iota(jnp.int32, (8, 128), 1)
    ones = jnp.ones((256, 128), bf16)

    def eight(g):
        return pl.ds(pl.multiple_of(g * 8, 8), 8)

    def kv_rows(g):
        return pl.ds(pl.multiple_of(g * 256, 256), 256)

    def values(u, g):
        both = jnp.concatenate([v_ref[kv_rows(g), :], ones], axis=1)
        out = jnp.dot(p_ref[u], both, preferred_element_type=f32)
        ps = jnp.zeros((8, 128), f32)
        for h in range(heads):
            rows = slice(h * 8, h * 8 + 8)
            po_ref[eight(g), h * 128 : (h + 1) * 128] = (
                out[rows, 0:128] * wide_ref[3 + h // half, eight(g), :]
            )
            ps = jnp.where(lane8 == h, out[rows, 128:256], ps)
        ps_ref[eight(g), :] = ps

    def soften(u, g):
        live = wide_ref[0, eight(g), :]
        live = jnp.concatenate([live, live], axis=1)
        pm = jnp.zeros((8, 128), f32)
        for j in range(2):
            keep = (tokens[j] < live)[None]
            scale = wide_ref[1 + j, eight(g), :]
            scale = jnp.concatenate([scale, scale], axis=1)[None]
            part = s_ref[u, j * 64 : (j + 1) * 64, :].reshape(8, 8, 256)
            part = jnp.where(keep, part * scale, -1e30)
            top = jnp.max(part, axis=2, keepdims=True)
            p_ref[u, j * 64 : (j + 1) * 64, :] = (
                jnp.exp2(part - top).reshape(64, 256).astype(bf16)
            )
            for h in range(8):
                pm = jnp.where(lane8 == j * 8 + h, top[h], pm)
        pm_ref[eight(g), :] = pm

    def scores(u, g):
        s_ref[u] = lax.dot_general(
            qs_ref[g], k_ref[kv_rows(g), :], (((1,), (1,)), ((), ())), preferred_element_type=f32
        )

    def body(i, carry):
        for u in range(UNROLL):
            values(u, jnp.maximum(i - 2, 0) * UNROLL + u)
            soften(u, jnp.clip(i - 1, 0, groups - 1) * UNROLL + u)
            scores(u, jnp.minimum(i, groups - 1) * UNROLL + u)
        return carry

    lax.fori_loop(0, groups + 2, body, 0)


def unpack_log(aux):
    aux = aux.astype(jnp.float32)
    return aux + pltpu.roll(aux, 112, 1) + pltpu.roll(aux, 96, 1)


def request_weights(pick_ref, pickt_ref, pm_ref, ps_ref):
    f32, bf16 = jnp.float32, jnp.bfloat16
    pm = pm_ref[...]
    rough = jnp.dot(
        pickt_ref[...], jnp.exp2(pm * (1.0 / 12.0)).astype(bf16), preferred_element_type=f32
    )
    some = rough > 0.0
    shift = jnp.where(some, 12.0 * jnp.log2(jnp.where(some, rough, 1.0)) - 42.0, 0.0).astype(bf16)
    near = pm - jnp.dot(pick_ref[...], shift, preferred_element_type=f32)
    den = of_two(
        jnp.dot(pickt_ref[...], in_two(ps_ref[...] * jnp.exp2(near)), preferred_element_type=f32)
    )
    log = shift.astype(f32) + jnp.log2(jnp.where(some, den, 1.0))
    log = pack_log(jnp.where(some, log, -1e30))
    back = unpack_log(jnp.dot(pick_ref[...], log, preferred_element_type=f32))
    ps_ref[...] = jnp.exp2(jnp.minimum(pm - back, 64.0))
    return log


def request_sums(n, pickt_ref, po_ref, ps_ref):
    f32, bf16 = jnp.float32, jnp.bfloat16
    cols = [
        (po_ref[:, h * 128 : (h + 1) * 128] * ps_ref[:, h : h + 1]).astype(bf16)
        for h in range(4 * n, 4 * n + 4)
    ]
    return jnp.dot(
        pickt_ref[...], jnp.concatenate(cols, axis=1), preferred_element_type=f32
    ).astype(bf16)


MESH = pl.DeviceIdType.MESH


def place():
    me = lax.axis_index("req")
    return lax.div(me, 8), lax.rem(lax.div(me, 2), 4), lax.rem(me, 2)


def off(i, d):
    return lax.rem(i + d + 4, 4)


def chip(x, y, c):
    return {"req": (x * 4 + y) * 2 + c}


class Copies:
    def __init__(self, send_sems, recv_sems):
        self.sems, self.count, self.sent = (send_sems, recv_sems), 0, []

    def send(self, source, target, device, landing):
        pair = (self.sems[0].at[self.count], self.sems[1].at[self.count])
        self.count += 1
        copy = pltpu.make_async_remote_copy(source, target, *pair, device, device_id_type=MESH)
        copy.start()
        self.sent.append(copy)
        return pltpu.make_async_remote_copy(source, landing, *pair, device, device_id_type=MESH)

    def drain(self):
        for copy in self.sent:
            copy.wait_send()


def greet(peers):
    barrier = pltpu.get_barrier_semaphore()
    for peer in peers:
        pl.semaphore_signal(barrier, inc=1, device_id=peer, device_id_type=MESH)
    return lambda: pl.semaphore_wait(barrier, len(peers))


def gather_first(copies, own, view, x, y, c, halves):
    left, right = halves
    waits = []
    for d in (2, 1, 3):
        waits.append(
            copies.send(
                own.at[:, left], view(x, y, c, left), chip(x, off(y, d), c),
                view(x, off(y, -d), c, left),
            )
        )
        waits.append(
            copies.send(
                own.at[:, right], view(x, y, c, right), chip(off(x, d), y, c),
                view(off(x, -d), y, c, right),
            )
        )
    return waits


def gather_second(copies, view, x, y, c, halves):
    left, right = halves
    every = slice(None)
    waits = []
    for d in (2, 1, 3):
        waits.append(
            copies.send(
                view(x, every, c, left), view(x, every, c, left), chip(off(x, d), y, c),
                view(off(x, -d), every, c, left),
            )
        )
        waits.append(
            copies.send(
                view(every, y, c, right), view(every, y, c, right), chip(x, off(y, d), c),
                view(every, off(y, -d), c, right),
            )
        )
    return waits


def pass_own(copies, view, x, y, c, halves):
    left, right = halves
    every = slice(None)
    twin = chip(x, y, 1 - c)
    return [
        copies.send(view(x, every, c, left), view(x, every, c, left), twin,
                    view(x, every, 1 - c, left)),
        copies.send(view(every, y, c, right), view(every, y, c, right), twin,
                    view(every, y, 1 - c, right)),
    ]


def pass_on(copies, waits, view, x, y, c, halves):
    left, right = halves
    every = slice(None)
    twin = chip(x, y, 1 - c)
    last = []
    for k, d in enumerate((2, 1, 3)):
        waits[2 * k].wait_recv()
        i = off(x, -d)
        piece = view(i, every, c, left)
        last.append(copies.send(piece, piece, twin, view(i, every, 1 - c, left)))
        waits[2 * k + 1].wait_recv()
        j = off(y, -d)
        piece = view(every, j, c, right)
        last.append(copies.send(piece, piece, twin, view(every, j, 1 - c, right)))
    return last


def wait_all(waits):
    for wait in waits:
        wait.wait_recv()


def shares_of(logs):
    top = functools.reduce(jnp.maximum, logs)
    shares = [jnp.exp2(g - top) for g in logs]
    total = functools.reduce(jnp.add, shares)
    inverse = 1.0 / total
    return [s * inverse for s in shares], pack_log(top + jnp.log2(total))


def blended(blocks, shares, head):
    terms = [b.astype(jnp.float32) * s[:, head : head + 1] for b, s in zip(blocks, shares)]
    return functools.reduce(jnp.add, terms).astype(jnp.bfloat16)


def whole_kernel(
    lengths_ref, queries_ref, table_ref, ks_ref, vs_ref, k_hbm, v_hbm, weight_hbm, out_ref,
    k_ref, v_ref, weight_ref, wide_q, q_ref, every_ref, code_ref, table_out, sum_y, sum_c, in_x, in_y, in_c,
    rows_ref, wide_ref, pick_ref, pickt_ref, qs_ref, s_ref, p_ref, po_ref, pm_ref, ps_ref,
    part_ref, log_ref, twin_in, log_in, now, now_log, share0,
    in_left, in_right, log_left, log_right, share_left, share_right,
    left_now, right_now, left_log, right_log,
    in_left2, in_right2, log_left2, log_right2, share_left2, share_right2,
    own, all_ref, half_terms, terms, terms_in, turned, load_sems, send_sems, recv_sems,
):
    f32, bf16 = jnp.float32, jnp.bfloat16
    x, y, c = place()
    z = lax.axis_index("head")
    rows = q_ref.shape[0]
    chunks = [
        (slice(k * 512, k * 512 + 512), slice(1024 + k * 512, 1536 + k * 512)) for k in range(2)
    ]
    loads = [
        pltpu.make_async_copy(k_hbm, k_ref, load_sems.at[0]),
        pltpu.make_async_copy(v_hbm, v_ref, load_sems.at[1]),
    ]
    load_weight = pltpu.make_async_copy(weight_hbm, weight_ref, load_sems.at[2])
    load_weight.start()
    for load in loads:
        load.start()

    def view_all(i, j, k, cols):
        return every_ref.at[k, i, j, :, cols]

    peers = [chip(off(x, d), y, c) for d in (1, 2, 3)]
    peers += [chip(x, off(y, d), c) for d in (1, 2, 3)]
    peers += [chip(x, y, 1 - c)] + [{"head": off(z, d)} for d in (1, 2, 3)]
    met = greet(peers)
    wide_q[...] = queries_ref[...].astype(f32).reshape(wide_q.shape)
    for h in range(16):
        q_ref[:, h * 128 : (h + 1) * 128] = wide_q[pl.ds(h, rows, stride=16), :].astype(bf16)
    copies = Copies(send_sems, recv_sems)
    lane = lax.broadcasted_iota(jnp.int32, (1, 128), 1)
    high_id = lax.broadcasted_iota(jnp.int32, (256, 128), 0)
    low_id = lax.broadcasted_iota(jnp.int32, (128, 128), 0)
    highs, lows = [], []
    for r in range(rows):
        live = jnp.clip(lengths_ref[r] - 16 * lane, 0, 16)
        coded = jnp.where(live > 0, live + 16 * r, 0).astype(f32)
        ids = table_ref[r : r + 1, :]
        highs.append(jnp.where(high_id == (ids >> 7), 1.0, 0.0).astype(bf16))
        lows.append(jnp.where(low_id == (ids & 127), coded, 0.0).astype(bf16))
    found = lax.dot_general(
        jnp.concatenate(highs, axis=1), jnp.concatenate(lows, axis=1),
        (((1,), (1,)), ((), ())), preferred_element_type=f32,
    )
    base = ((c * 16 + x * 4 + y) * 256).astype(f32)
    table_out[...] = jnp.where(found > 0.0, found + base, 0.0).reshape(4, 4, 2, 8, 128)
    every_ref[c, x, y] = q_ref[...]
    met()
    got = [
        copies.send(
            table_out.at[off(x, d)], in_x.at[d - 1], chip(off(x, d), y, c), in_x.at[d - 1]
        )
        for d in (2, 1, 3)
    ]
    first = [gather_first(copies, q_ref, view_all, x, y, c, halves) for halves in chunks]
    wait_all(got)
    sum_y[...] = table_out[x] + in_x[0] + in_x[1] + in_x[2]
    got = [
        copies.send(sum_y.at[off(y, d)], in_y.at[d - 1], chip(x, off(y, d), c), in_y.at[d - 1])
        for d in (2, 1, 3)
    ]
    second, third = [], []
    for halves, waits in zip(chunks, first):
        wait_all(waits)
        second.append(gather_second(copies, view_all, x, y, c, halves))
        third.append(pass_own(copies, view_all, x, y, c, halves))
    wait_all(got)
    sum_c[...] = sum_y[y] + in_y[0] + in_y[1] + in_y[2]
    copies.send(sum_c.at[1 - c], in_c, chip(x, y, 1 - c), in_c).wait_recv()
    code_ref[...] = sum_c[c] + in_c[...] - 1.0
    page_columns(code_ref, ks_ref, vs_ref, rows_ref, wide_ref, pick_ref, pickt_ref)
    third[0] += pass_on(copies, second[0], view_all, x, y, c, chunks[0])
    third[1] += pass_on(copies, second[1], view_all, x, y, c, chunks[1])
    wait_all(third[0])
    page_queries(0, every_ref, pick_ref, qs_ref)
    wait_all(third[1])
    page_queries(1, every_ref, pick_ref, qs_ref)
    for load in loads:
        load.wait()
    page_sums(k_ref, v_ref, wide_ref, qs_ref, s_ref, p_ref, po_ref, pm_ref, ps_ref)
    log_ref[...] = request_weights(pick_ref, pickt_ref, pm_ref, ps_ref).reshape(
        2, 4, 4, rows, 128
    )
    twin = chip(x, y, 1 - c)
    log_wait = copies.send(log_ref.at[1 - c], log_in, twin, log_in)

    def sums(*pairs):
        for n in pairs:
            part_ref[:, :, :, :, n * 512 : n * 512 + 512] = request_sums(
                n, pickt_ref, po_ref, ps_ref
            ).reshape(2, 4, 4, rows, 512)

    def to_twin(halves):
        return [
            copies.send(
                part_ref.at[1 - c, :, :, :, cols], twin_in.at[:, :, :, cols], twin,
                twin_in.at[:, :, :, cols],
            )
            for cols in halves
        ]

    def first_shares(j, carry):
        for i in range(4):
            shares, log = shares_of([unpack_log(log_ref[c, i, j]), unpack_log(log_in[i, j])])
            now_log[i, j] = log
            for k in range(2):
                share0[k, i, j] = shares[k]
        return carry

    def across(k, waits):
        wait_all(waits)

        def body(i, carry):
            for j in range(4):
                shares = [share0[0, i, j], share0[1, i, j]]
                for h in range(4):
                    for side in range(2):
                        at = side * 1024 + k * 512 + h * 128
                        cols = slice(at, at + 128)
                        now[i, j, :, cols] = blended(
                            [part_ref[c, i, j, :, cols], twin_in[i, j, :, cols]],
                            shares, side * 8 + k * 4 + h,
                        )
            return carry

        lax.fori_loop(0, 4, body, 0)
        left, right = chunks[k]
        near = chunks[k][0]
        waits, logs = [], []
        for d in (2, 1, 3):
            to_x, to_y = chip(off(x, d), y, c), chip(x, off(y, d), c)
            if k == 0:
                logs.append(
                    copies.send(
                        now_log.at[off(x, d)], log_left.at[d - 1], to_x, log_left.at[d - 1]
                    )
                )
                logs.append(
                    copies.send(
                        now_log.at[:, off(y, d)], log_right.at[d - 1], to_y, log_right.at[d - 1]
                    )
                )
            here = in_left.at[d - 1, :, :, near]
            waits.append(copies.send(now.at[off(x, d), :, :, left], here, to_x, here))
            here = in_right.at[d - 1, :, :, near]
            waits.append(copies.send(now.at[:, off(y, d), :, right], here, to_y, here))
        return waits, logs

    def second_shares(j, carry):
        logs = [now_log[x, j]] + [log_left[d, j] for d in range(3)]
        shares, log = shares_of([unpack_log(g) for g in logs])
        left_log[j] = log
        for k in range(4):
            share_left[k, j] = shares[k]
        logs = [now_log[j, y]] + [log_right[d, j] for d in range(3)]
        shares, log = shares_of([unpack_log(g) for g in logs])
        right_log[j] = log
        for k in range(4):
            share_right[k, j] = shares[k]
        return carry

    def along(k, waits):
        wait_all(waits)

        def body(j, carry):
            shares = [share_left[i, j] for i in range(4)]
            for h in range(4):
                at = k * 512 + h * 128
                cols = slice(at, at + 128)
                blocks = [now[x, j, :, cols]] + [in_left[d, j, :, cols] for d in range(3)]
                left_now[j, :, cols] = blended(blocks, shares, k * 4 + h)
            shares = [share_right[i, j] for i in range(4)]
            for h in range(4):
                at = k * 512 + h * 128
                cols = slice(at, at + 128)
                blocks = [now[j, y, :, 1024 + at : 1152 + at]]
                blocks += [in_right[d, j, :, cols] for d in range(3)]
                right_now[j, :, cols] = blended(blocks, shares, 8 + k * 4 + h)
            return carry

        lax.fori_loop(0, 4, body, 0)
        near = chunks[k][0]
        waits, logs = [], []
        for d in (2, 1, 3):
            to_x, to_y = chip(off(x, d), y, c), chip(x, off(y, d), c)
            if k == 0:
                logs.append(
                    copies.send(
                        left_log.at[off(y, d)], log_left2.at[d - 1], to_y, log_left2.at[d - 1]
                    )
                )
                logs.append(
                    copies.send(
                        right_log.at[off(x, d)], log_right2.at[d - 1], to_x, log_right2.at[d - 1]
                    )
                )
            here = in_left2.at[d - 1, :, near]
            waits.append(copies.send(left_now.at[off(y, d), :, near], here, to_y, here))
            here = in_right2.at[d - 1, :, near]
            waits.append(copies.send(right_now.at[off(x, d), :, near], here, to_x, here))
        return waits, logs

    def third_shares():
        logs = [left_log[y]] + [log_left2[d] for d in range(3)]
        shares, _ = shares_of([unpack_log(g) for g in logs])
        for k in range(4):
            share_left2[k] = shares[k]
        logs = [right_log[x]] + [log_right2[d] for d in range(3)]
        shares, _ = shares_of([unpack_log(g) for g in logs])
        for k in range(4):
            share_right2[k] = shares[k]

    def view(i, j, k, cols):
        return all_ref.at[i, j, k, :, cols]

    def finish(k, waits):
        wait_all(waits)
        for h in range(4):
            at = k * 512 + h * 128
            cols = slice(at, at + 128)
            blocks = [left_now[y, :, cols]] + [in_left2[d, :, cols] for d in range(3)]
            shares = [share_left2[i] for i in range(4)]
            own[:, cols] = blended(blocks, shares, k * 4 + h)
            blocks = [right_now[x, :, cols]] + [in_right2[d, :, cols] for d in range(3)]
            shares = [share_right2[i] for i in range(4)]
            own[:, 1024 + at : 1152 + at] = blended(blocks, shares, 8 + k * 4 + h)
        return gather_first(copies, own, view, x, y, c, chunks[k])

    sums(0, 2)
    twin0 = to_twin(chunks[0])
    sums(1)
    log_wait.wait_recv()
    lax.fori_loop(0, 4, first_shares, 0)
    across0, logs = across(0, twin0)
    sums(3)
    twin1 = to_twin(chunks[1])
    across1, _ = across(1, twin1)
    load_weight.wait()
    for k in range(16):
        turned[:, k * 128 : (k + 1) * 128] = weight_ref[k * 128 : (k + 1) * 128, :].T
    wait_all(logs)
    lax.fori_loop(0, 4, second_shares, 0)
    along0, logs = along(0, across0)
    along1, _ = along(1, across1)
    wait_all(logs)
    third_shares()
    first = [finish(0, along0), finish(1, along1)]
    all_ref[x, y, c] = own[...]
    second, third = [], []
    for halves, waits in zip(chunks, first):
        wait_all(waits)
        second.append(gather_second(copies, view, x, y, c, halves))
        third.append(pass_own(copies, view, x, y, c, halves))

    def product(k, i):
        total = jnp.zeros((256, 256), f32)
        for cols in chunks[k]:
            total = total + lax.dot_general(
                turned[:, cols], all_ref[2 * i : 2 * i + 2, :, :, :, cols].reshape(256, 512),
                (((1,), (1,)), ((), ())), preferred_element_type=f32,
            )
        return total

    third[0] += pass_on(copies, second[0], view, x, y, c, chunks[0])
    third[1] += pass_on(copies, second[1], view, x, y, c, chunks[1])
    wait_all(third[0])
    for i in range(2):
        half_terms[:, i * 256 : i * 256 + 256] = product(0, i)
    wait_all(third[1])
    waits = []
    for i in range(2):
        cols = slice(i * 256, i * 256 + 256)
        terms[:, :, cols] = (
            (half_terms[:, cols] + product(1, i)).astype(bf16).reshape(4, 64, 256)
        )
        for d in (2, 1, 3):
            here = terms_in.at[d - 1, :, cols]
            waits.append(
                copies.send(terms.at[off(z, d), :, cols], here, {"head": off(z, d)}, here)
            )
    wait_all(waits)
    total = terms[z].astype(f32)
    for d in range(3):
        total = total + terms_in[d].astype(f32)
    out_ref[...] = total.astype(bf16)
    copies.drain()


def whole(lengths, queries, page_table, ks, vs, keys, values, weight):
    f32, bf16 = jnp.float32, jnp.bfloat16
    rows = queries.shape[0]
    width = queries.shape[1] * queries.shape[2]
    pages = keys.shape[0] // 32
    requests = 32 * rows
    vmem = pl.BlockSpec(memory_space=pltpu.VMEM)
    hbm = pl.BlockSpec(memory_space=pl.ANY)
    return pl.pallas_call(
        whole_kernel,
        out_shape=jax.ShapeDtypeStruct((64, 512), bf16),
        in_specs=[pl.BlockSpec(memory_space=pltpu.SMEM), vmem, vmem, vmem, vmem, hbm, hbm, hbm],
        out_specs=vmem,
        scratch_shapes=[
            pltpu.VMEM(keys.shape, bf16),
            pltpu.VMEM(keys.shape, bf16),
            pltpu.VMEM(weight.shape, bf16),
            pltpu.VMEM((rows * 16, 128), f32),
            pltpu.VMEM((rows, width), bf16),
            pltpu.VMEM((2, 4, 4, rows, width), bf16),
            pltpu.VMEM((8, 128), f32),
            pltpu.VMEM((4, 4, 2, 8, 128), f32),
            pltpu.VMEM((4, 2, 8, 128), f32),
            pltpu.VMEM((2, 8, 128), f32),
            pltpu.VMEM((3, 4, 2, 8, 128), f32),
            pltpu.VMEM((3, 2, 8, 128), f32),
            pltpu.VMEM((8, 128), f32),
            pltpu.VMEM((8, 128), f32),
            pltpu.VMEM((5, pages, 128), f32),
            pltpu.VMEM((pages, requests), bf16),
            pltpu.VMEM((requests, pages), bf16),
            pltpu.VMEM((pages // 8, 128, 128), bf16),
            pltpu.VMEM((UNROLL, 128, 256), f32),
            pltpu.VMEM((UNROLL, 128, 256), bf16),
            pltpu.VMEM((pages, width), f32),
            pltpu.VMEM((pages, 128), f32),
            pltpu.VMEM((pages, 128), f32),
            pltpu.VMEM((2, 4, 4, 16, 2048), bf16),
            pltpu.VMEM((2, 4, 4, 16, 128), bf16),
            pltpu.VMEM((4, 4, 16, 2048), bf16),
            pltpu.VMEM((4, 4, 16, 128), bf16),
            pltpu.VMEM((4, 4, 16, 2048), bf16),
            pltpu.VMEM((4, 4, 16, 128), bf16),
            pltpu.VMEM((2, 4, 4, 16, 128), f32),
            pltpu.VMEM((3, 4, 16, 1024), bf16),
            pltpu.VMEM((3, 4, 16, 1024), bf16),
            pltpu.VMEM((3, 4, 16, 128), bf16),
            pltpu.VMEM((3, 4, 16, 128), bf16),
            pltpu.VMEM((4, 4, 16, 128), f32),
            pltpu.VMEM((4, 4, 16, 128), f32),
            pltpu.VMEM((4, 16, 1024), bf16),
            pltpu.VMEM((4, 16, 1024), bf16),
            pltpu.VMEM((4, 16, 128), bf16),
            pltpu.VMEM((4, 16, 128), bf16),
            pltpu.VMEM((3, 16, 1024), bf16),
            pltpu.VMEM((3, 16, 1024), bf16),
            pltpu.VMEM((3, 16, 128), bf16),
            pltpu.VMEM((3, 16, 128), bf16),
            pltpu.VMEM((4, 16, 128), f32),
            pltpu.VMEM((4, 16, 128), f32),
            pltpu.VMEM((16, 2048), bf16),
            pltpu.VMEM((4, 4, 2, 16, 2048), bf16),
            pltpu.VMEM((256, 512), f32),
            pltpu.VMEM((4, 64, 512), bf16),
            pltpu.VMEM((3, 64, 512), bf16),
            pltpu.VMEM((256, 2048), bf16),
            pltpu.SemaphoreType.DMA((3,)),
            pltpu.SemaphoreType.DMA((134,)),
            pltpu.SemaphoreType.DMA((134,)),
        ],
        compiler_params=pltpu.CompilerParams(
            collective_id=1, has_side_effects=True, vmem_limit_bytes=60 * 1024 * 1024
        ),
        name="whole",
    )(lengths, queries, page_table, ks, vs, keys, values, weight)


def on_device(
    queries,
    k_codes,
    value_quantized_codes,
    key_page_scale,
    value_page_scale,
    lengths,
    page_table,
    out_weight,
):
    head_size = k_codes.shape[-1]
    return whole(
        lengths,
        queries,
        page_table,
        key_page_scale.T,
        value_page_scale.T,
        k_codes.reshape(-1, head_size),
        value_quantized_codes.reshape(-1, head_size),
        out_weight,
    ).T


def solution(mesh):
    in_specs = (
        P("req", "head", None),
        P("req", None, "head", None),
        P("req", None, "head", None),
        P("req", "head"),
        P("req", "head"),
        P("req"),
        P("req", None),
        P("head", "req"),
    )
    out_specs = P(None, ("req", "head"))
    return jax.shard_map(
        on_device, mesh=mesh, in_specs=in_specs, out_specs=out_specs, check_vma=False
    )
```

```python
import functools
import math

import jax
import jax.numpy as jnp
from jax import lax
from jax.experimental import pallas as pl
from jax.experimental.pallas import tpu as pltpu
from jax.sharding import PartitionSpec as P

LOG2E = 1.4426950408889634
UNROLL = 8


def pack_log(value):
    f32, bf16 = jnp.float32, jnp.bfloat16
    high = value.astype(bf16).astype(f32)
    middle = (value - high).astype(bf16).astype(f32)
    low = value - high - middle
    lane = lax.broadcasted_iota(jnp.int32, value.shape, 1)
    low = jnp.where(lane < 48, pltpu.roll(low, 32, 1), 0.0)
    low = jnp.where(lane < 32, pltpu.roll(middle, 16, 1), low)
    return jnp.where(lane < 16, high, low).astype(bf16)


def in_two(value):
    f32, bf16 = jnp.float32, jnp.bfloat16
    high = value.astype(bf16).astype(f32)
    lane = lax.broadcasted_iota(jnp.int32, value.shape, 1)
    return jnp.where(lane < 16, high, pltpu.roll(value - high, 16, 1)).astype(bf16)


def of_two(value):
    return value + pltpu.roll(value, 112, 1)


def page_columns(code_ref, ks_ref, vs_ref, rows_ref, wide_ref, pick_ref, pickt_ref):
    f32, bf16 = jnp.float32, jnp.bfloat16
    requests = pickt_ref.shape[0]
    scale = LOG2E / math.sqrt(128.0)

    def body(b, carry):
        code = code_ref[pl.ds(b, 1), :]
        lanes = pl.ds(pl.multiple_of(b * 128, 128), 128)
        owner_row = jnp.floor(code * (1.0 / 16.0))
        rows_ref[0:1, :] = owner_row
        rows_ref[1:2, :] = code - 16.0 * owner_row + 1.0
        rows_ref[2:4, :] = ks_ref[:, lanes] * scale
        rows_ref[4:6, :] = vs_ref[:, lanes]
        cols = rows_ref[...].T
        for i in range(5):
            wide_ref[i, lanes, :] = jnp.broadcast_to(cols[:, i + 1 : i + 2], (128, 128))
        owner = jnp.broadcast_to(cols[:, 0:1], (128, 128))
        lane = lax.broadcasted_iota(jnp.int32, (128, 128), 1).astype(f32)
        for c in range(requests // 128):
            pick_ref[lanes, c * 128 : (c + 1) * 128] = jnp.where(
                owner == lane + float(c * 128), 1.0, 0.0
            ).astype(bf16)
        row = lax.broadcasted_iota(jnp.int32, (requests, 128), 0).astype(f32)
        pickt_ref[:, lanes] = jnp.where(row == owner_row, 1.0, 0.0).astype(bf16)
        return carry

    lax.fori_loop(0, code_ref.shape[0], body, 0)


def page_queries(k, q_ref, pick_ref, qs_ref):
    f32, bf16 = jnp.float32, jnp.bfloat16
    tiles = qs_ref.shape[0]

    def body(i, carry):
        for u in range(2):
            n = i * 4 + 2 * k + u
            cols = pl.ds(pl.multiple_of(n * 256, 256), 256)
            queries = q_ref[:, :, :, :, cols].reshape(pick_ref.shape[1], 256)
            got = jnp.dot(pick_ref[...], queries, preferred_element_type=f32)
            pair = [got[:, j * 128 : (j + 1) * 128].reshape(tiles, 8, 128) for j in range(2)]
            qs_ref[:, pl.ds(pl.multiple_of(n * 16, 16), 16), :] = jnp.concatenate(
                pair, axis=1
            ).astype(bf16)
        return carry

    lax.fori_loop(0, 2, body, 0)


def page_sums(k_ref, v_ref, wide_ref, qs_ref, s_ref, p_ref, po_ref, pm_ref, ps_ref):
    f32, bf16 = jnp.float32, jnp.bfloat16
    heads, half = 16, 8
    groups = qs_ref.shape[0] // UNROLL
    lane = lax.broadcasted_iota(jnp.int32, (8, 256), 1)
    sub = lax.broadcasted_iota(jnp.int32, (8, 256), 0)
    own = (lane >> 5) == sub
    token = ((lane & 31) >> 1).astype(f32)
    far = jnp.float32(1e9)
    tokens = [jnp.where(own & ((lane & 1) == j), token, far) for j in range(2)]
    lane8 = lax.broadcasted_iota(jnp.int32, (8, 128), 1)
    ones = jnp.ones((256, 128), bf16)

    def eight(g):
        return pl.ds(pl.multiple_of(g * 8, 8), 8)

    def kv_rows(g):
        return pl.ds(pl.multiple_of(g * 256, 256), 256)

    def values(u, g):
        both = jnp.concatenate([v_ref[kv_rows(g), :], ones], axis=1)
        out = jnp.dot(p_ref[u], both, preferred_element_type=f32)
        ps = jnp.zeros((8, 128), f32)
        for h in range(heads):
            rows = slice(h * 8, h * 8 + 8)
            po_ref[eight(g), h * 128 : (h + 1) * 128] = (
                out[rows, 0:128] * wide_ref[3 + h // half, eight(g), :]
            )
            ps = jnp.where(lane8 == h, out[rows, 128:256], ps)
        ps_ref[eight(g), :] = ps

    def soften(u, g):
        live = wide_ref[0, eight(g), :]
        live = jnp.concatenate([live, live], axis=1)
        pm = jnp.zeros((8, 128), f32)
        for j in range(2):
            keep = (tokens[j] < live)[None]
            scale = wide_ref[1 + j, eight(g), :]
            scale = jnp.concatenate([scale, scale], axis=1)[None]
            part = s_ref[u, j * 64 : (j + 1) * 64, :].reshape(8, 8, 256)
            part = jnp.where(keep, part * scale, -1e30)
            top = jnp.max(part, axis=2, keepdims=True)
            p_ref[u, j * 64 : (j + 1) * 64, :] = (
                jnp.exp2(part - top).reshape(64, 256).astype(bf16)
            )
            for h in range(8):
                pm = jnp.where(lane8 == j * 8 + h, top[h], pm)
        pm_ref[eight(g), :] = pm

    def scores(u, g):
        s_ref[u] = lax.dot_general(
            qs_ref[g], k_ref[kv_rows(g), :], (((1,), (1,)), ((), ())), preferred_element_type=f32
        )

    def body(i, carry):
        for u in range(UNROLL):
            scores(u, jnp.minimum(i, groups - 1) * UNROLL + u)
        for u in range(UNROLL):
            values(u, jnp.maximum(i - 1, 0) * UNROLL + u)
        for u in range(UNROLL):
            soften(u, jnp.minimum(i, groups - 1) * UNROLL + u)
        return carry

    lax.fori_loop(0, groups + 1, body, 0)


def unpack_log(aux):
    aux = aux.astype(jnp.float32)
    return aux + pltpu.roll(aux, 112, 1) + pltpu.roll(aux, 96, 1)


def request_weights(pick_ref, pickt_ref, pm_ref, ps_ref):
    f32, bf16 = jnp.float32, jnp.bfloat16
    pm = pm_ref[...]
    rough = jnp.dot(
        pickt_ref[...], jnp.exp2(pm * (1.0 / 12.0)).astype(bf16), preferred_element_type=f32
    )
    some = rough > 0.0
    shift = jnp.where(some, 12.0 * jnp.log2(jnp.where(some, rough, 1.0)) - 42.0, 0.0).astype(bf16)
    near = pm - jnp.dot(pick_ref[...], shift, preferred_element_type=f32)
    den = of_two(
        jnp.dot(pickt_ref[...], in_two(ps_ref[...] * jnp.exp2(near)), preferred_element_type=f32)
    )
    log = shift.astype(f32) + jnp.log2(jnp.where(some, den, 1.0))
    log = pack_log(jnp.where(some, log, -1e30))
    back = unpack_log(jnp.dot(pick_ref[...], log, preferred_element_type=f32))
    ps_ref[...] = jnp.exp2(jnp.minimum(pm - back, 64.0))
    return log


def request_sums(n, pickt_ref, po_ref, ps_ref):
    f32, bf16 = jnp.float32, jnp.bfloat16
    cols = [
        (po_ref[:, h * 128 : (h + 1) * 128] * ps_ref[:, h : h + 1]).astype(bf16)
        for h in range(4 * n, 4 * n + 4)
    ]
    return jnp.dot(
        pickt_ref[...], jnp.concatenate(cols, axis=1), preferred_element_type=f32
    ).astype(bf16)


MESH = pl.DeviceIdType.MESH


def place():
    me = lax.axis_index("req")
    return lax.div(me, 8), lax.rem(lax.div(me, 2), 4), lax.rem(me, 2)


def off(i, d):
    return lax.rem(i + d + 4, 4)


def chip(x, y, c):
    return {"req": (x * 4 + y) * 2 + c}


class Copies:
    def __init__(self, send_sems, recv_sems):
        self.sems, self.count, self.sent = (send_sems, recv_sems), 0, []

    def send(self, source, target, device, landing):
        pair = (self.sems[0].at[self.count], self.sems[1].at[self.count])
        self.count += 1
        copy = pltpu.make_async_remote_copy(source, target, *pair, device, device_id_type=MESH)
        copy.start()
        self.sent.append(copy)
        return pltpu.make_async_remote_copy(source, landing, *pair, device, device_id_type=MESH)

    def drain(self):
        for copy in self.sent:
            copy.wait_send()


def greet(peers):
    barrier = pltpu.get_barrier_semaphore()
    for peer in peers:
        pl.semaphore_signal(barrier, inc=1, device_id=peer, device_id_type=MESH)
    return lambda: pl.semaphore_wait(barrier, len(peers))


def gather_first(copies, own, view, x, y, c, halves):
    left, right = halves
    waits = []
    for d in (2, 1, 3):
        waits.append(
            copies.send(
                own.at[:, left], view(x, y, c, left), chip(x, off(y, d), c),
                view(x, off(y, -d), c, left),
            )
        )
        waits.append(
            copies.send(
                own.at[:, right], view(x, y, c, right), chip(off(x, d), y, c),
                view(off(x, -d), y, c, right),
            )
        )
    return waits


def gather_second(copies, view, x, y, c, halves):
    left, right = halves
    every = slice(None)
    waits = []
    for d in (2, 1, 3):
        waits.append(
            copies.send(
                view(x, every, c, left), view(x, every, c, left), chip(off(x, d), y, c),
                view(off(x, -d), every, c, left),
            )
        )
        waits.append(
            copies.send(
                view(every, y, c, right), view(every, y, c, right), chip(x, off(y, d), c),
                view(every, off(y, -d), c, right),
            )
        )
    return waits


def pass_own(copies, view, x, y, c, halves):
    left, right = halves
    every = slice(None)
    twin = chip(x, y, 1 - c)
    return [
        copies.send(view(x, every, c, left), view(x, every, c, left), twin,
                    view(x, every, 1 - c, left)),
        copies.send(view(every, y, c, right), view(every, y, c, right), twin,
                    view(every, y, 1 - c, right)),
    ]


def pass_on(copies, waits, view, x, y, c, halves):
    left, right = halves
    every = slice(None)
    twin = chip(x, y, 1 - c)
    last = []
    for k, d in enumerate((2, 1, 3)):
        waits[2 * k].wait_recv()
        i = off(x, -d)
        piece = view(i, every, c, left)
        last.append(copies.send(piece, piece, twin, view(i, every, 1 - c, left)))
        waits[2 * k + 1].wait_recv()
        j = off(y, -d)
        piece = view(every, j, c, right)
        last.append(copies.send(piece, piece, twin, view(every, j, 1 - c, right)))
    return last


def wait_all(waits):
    for wait in waits:
        wait.wait_recv()


def shares_of(logs):
    top = functools.reduce(jnp.maximum, logs)
    shares = [jnp.exp2(g - top) for g in logs]
    total = functools.reduce(jnp.add, shares)
    inverse = 1.0 / total
    return [s * inverse for s in shares], pack_log(top + jnp.log2(total))


def blended(blocks, shares, head):
    terms = [b.astype(jnp.float32) * s[:, head : head + 1] for b, s in zip(blocks, shares)]
    return functools.reduce(jnp.add, terms).astype(jnp.bfloat16)


def whole_kernel(
    lengths_ref, queries_ref, table_ref, ks_ref, vs_ref, k_hbm, v_hbm, weight_hbm, out_ref,
    k_ref, v_ref, weight_ref, wide_q, q_ref, every_ref, code_ref, table_out, sum_y, sum_c, in_x, in_y, in_c,
    rows_ref, wide_ref, pick_ref, pickt_ref, qs_ref, s_ref, p_ref, po_ref, pm_ref, ps_ref,
    part_ref, log_ref, twin_in, log_in, now, now_log, share0,
    in_left, in_right, log_left, log_right, share_left, share_right,
    left_now, right_now, left_log, right_log,
    in_left2, in_right2, log_left2, log_right2, share_left2, share_right2,
    own, all_ref, half_terms, terms, terms_in, turned, load_sems, send_sems, recv_sems,
):
    f32, bf16 = jnp.float32, jnp.bfloat16
    x, y, c = place()
    z = lax.axis_index("head")
    rows = q_ref.shape[0]
    chunks = [
        (slice(k * 512, k * 512 + 512), slice(1024 + k * 512, 1536 + k * 512)) for k in range(2)
    ]
    loads = [
        pltpu.make_async_copy(k_hbm, k_ref, load_sems.at[0]),
        pltpu.make_async_copy(v_hbm, v_ref, load_sems.at[1]),
    ]
    load_weight = pltpu.make_async_copy(weight_hbm, weight_ref, load_sems.at[2])
    load_weight.start()
    for load in loads:
        load.start()

    def view_all(i, j, k, cols):
        return every_ref.at[k, i, j, :, cols]

    peers = [chip(off(x, d), y, c) for d in (1, 2, 3)]
    peers += [chip(x, off(y, d), c) for d in (1, 2, 3)]
    peers += [chip(x, y, 1 - c)] + [{"head": off(z, d)} for d in (1, 2, 3)]
    met = greet(peers)
    wide_q[...] = queries_ref[...].astype(f32).reshape(wide_q.shape)
    for h in range(16):
        q_ref[:, h * 128 : (h + 1) * 128] = wide_q[pl.ds(h, rows, stride=16), :].astype(bf16)
    copies = Copies(send_sems, recv_sems)
    lane = lax.broadcasted_iota(jnp.int32, (1, 128), 1)
    high_id = lax.broadcasted_iota(jnp.int32, (256, 128), 0)
    low_id = lax.broadcasted_iota(jnp.int32, (128, 128), 0)
    highs, lows = [], []
    for r in range(rows):
        live = jnp.clip(lengths_ref[r] - 16 * lane, 0, 16)
        coded = jnp.where(live > 0, live + 16 * r, 0).astype(f32)
        ids = table_ref[r : r + 1, :]
        highs.append(jnp.where(high_id == (ids >> 7), 1.0, 0.0).astype(bf16))
        lows.append(jnp.where(low_id == (ids & 127), coded, 0.0).astype(bf16))
    found = lax.dot_general(
        jnp.concatenate(highs, axis=1), jnp.concatenate(lows, axis=1),
        (((1,), (1,)), ((), ())), preferred_element_type=f32,
    )
    base = ((c * 16 + x * 4 + y) * 256).astype(f32)
    table_out[...] = jnp.where(found > 0.0, found + base, 0.0).reshape(4, 4, 2, 8, 128)
    every_ref[c, x, y] = q_ref[...]
    met()
    got = [
        copies.send(
            table_out.at[off(x, d)], in_x.at[d - 1], chip(off(x, d), y, c), in_x.at[d - 1]
        )
        for d in (2, 1, 3)
    ]
    first = [gather_first(copies, q_ref, view_all, x, y, c, halves) for halves in chunks]
    wait_all(got)
    sum_y[...] = table_out[x] + in_x[0] + in_x[1] + in_x[2]
    got = [
        copies.send(sum_y.at[off(y, d)], in_y.at[d - 1], chip(x, off(y, d), c), in_y.at[d - 1])
        for d in (2, 1, 3)
    ]
    second, third = [], []
    for halves, waits in zip(chunks, first):
        wait_all(waits)
        second.append(gather_second(copies, view_all, x, y, c, halves))
        third.append(pass_own(copies, view_all, x, y, c, halves))
    wait_all(got)
    sum_c[...] = sum_y[y] + in_y[0] + in_y[1] + in_y[2]
    copies.send(sum_c.at[1 - c], in_c, chip(x, y, 1 - c), in_c).wait_recv()
    code_ref[...] = sum_c[c] + in_c[...] - 1.0
    page_columns(code_ref, ks_ref, vs_ref, rows_ref, wide_ref, pick_ref, pickt_ref)
    third[0] += pass_on(copies, second[0], view_all, x, y, c, chunks[0])
    third[1] += pass_on(copies, second[1], view_all, x, y, c, chunks[1])
    wait_all(third[0])
    page_queries(0, every_ref, pick_ref, qs_ref)
    wait_all(third[1])
    page_queries(1, every_ref, pick_ref, qs_ref)
    for load in loads:
        load.wait()
    page_sums(k_ref, v_ref, wide_ref, qs_ref, s_ref, p_ref, po_ref, pm_ref, ps_ref)
    log_ref[...] = request_weights(pick_ref, pickt_ref, pm_ref, ps_ref).reshape(
        2, 4, 4, rows, 128
    )
    twin = chip(x, y, 1 - c)
    log_wait = copies.send(log_ref.at[1 - c], log_in, twin, log_in)

    def sums(*pairs):
        for n in pairs:
            part_ref[:, :, :, :, n * 512 : n * 512 + 512] = request_sums(
                n, pickt_ref, po_ref, ps_ref
            ).reshape(2, 4, 4, rows, 512)

    def to_twin(halves):
        return [
            copies.send(
                part_ref.at[1 - c, :, :, :, cols], twin_in.at[:, :, :, cols], twin,
                twin_in.at[:, :, :, cols],
            )
            for cols in halves
        ]

    def first_shares(j, carry):
        for i in range(4):
            shares, log = shares_of([unpack_log(log_ref[c, i, j]), unpack_log(log_in[i, j])])
            now_log[i, j] = log
            for k in range(2):
                share0[k, i, j] = shares[k]
        return carry

    def across(k, waits):
        wait_all(waits)

        def body(i, carry):
            for j in range(4):
                shares = [share0[0, i, j], share0[1, i, j]]
                for h in range(4):
                    for side in range(2):
                        at = side * 1024 + k * 512 + h * 128
                        cols = slice(at, at + 128)
                        now[i, j, :, cols] = blended(
                            [part_ref[c, i, j, :, cols], twin_in[i, j, :, cols]],
                            shares, side * 8 + k * 4 + h,
                        )
            return carry

        lax.fori_loop(0, 4, body, 0)
        left, right = chunks[k]
        near = chunks[k][0]
        waits, logs = [], []
        for d in (2, 1, 3):
            to_x, to_y = chip(off(x, d), y, c), chip(x, off(y, d), c)
            if k == 0:
                logs.append(
                    copies.send(
                        now_log.at[off(x, d)], log_left.at[d - 1], to_x, log_left.at[d - 1]
                    )
                )
                logs.append(
                    copies.send(
                        now_log.at[:, off(y, d)], log_right.at[d - 1], to_y, log_right.at[d - 1]
                    )
                )
            here = in_left.at[d - 1, :, :, near]
            waits.append(copies.send(now.at[off(x, d), :, :, left], here, to_x, here))
            here = in_right.at[d - 1, :, :, near]
            waits.append(copies.send(now.at[:, off(y, d), :, right], here, to_y, here))
        return waits, logs

    def second_shares(j, carry):
        logs = [now_log[x, j]] + [log_left[d, j] for d in range(3)]
        shares, log = shares_of([unpack_log(g) for g in logs])
        left_log[j] = log
        for k in range(4):
            share_left[k, j] = shares[k]
        logs = [now_log[j, y]] + [log_right[d, j] for d in range(3)]
        shares, log = shares_of([unpack_log(g) for g in logs])
        right_log[j] = log
        for k in range(4):
            share_right[k, j] = shares[k]
        return carry

    def along(k, waits):
        wait_all(waits)

        def body(j, carry):
            shares = [share_left[i, j] for i in range(4)]
            for h in range(4):
                at = k * 512 + h * 128
                cols = slice(at, at + 128)
                blocks = [now[x, j, :, cols]] + [in_left[d, j, :, cols] for d in range(3)]
                left_now[j, :, cols] = blended(blocks, shares, k * 4 + h)
            shares = [share_right[i, j] for i in range(4)]
            for h in range(4):
                at = k * 512 + h * 128
                cols = slice(at, at + 128)
                blocks = [now[j, y, :, 1024 + at : 1152 + at]]
                blocks += [in_right[d, j, :, cols] for d in range(3)]
                right_now[j, :, cols] = blended(blocks, shares, 8 + k * 4 + h)
            return carry

        lax.fori_loop(0, 4, body, 0)
        near = chunks[k][0]
        waits, logs = [], []
        for d in (2, 1, 3):
            to_x, to_y = chip(off(x, d), y, c), chip(x, off(y, d), c)
            if k == 0:
                logs.append(
                    copies.send(
                        left_log.at[off(y, d)], log_left2.at[d - 1], to_y, log_left2.at[d - 1]
                    )
                )
                logs.append(
                    copies.send(
                        right_log.at[off(x, d)], log_right2.at[d - 1], to_x, log_right2.at[d - 1]
                    )
                )
            here = in_left2.at[d - 1, :, near]
            waits.append(copies.send(left_now.at[off(y, d), :, near], here, to_y, here))
            here = in_right2.at[d - 1, :, near]
            waits.append(copies.send(right_now.at[off(x, d), :, near], here, to_x, here))
        return waits, logs

    def third_shares():
        logs = [left_log[y]] + [log_left2[d] for d in range(3)]
        shares, _ = shares_of([unpack_log(g) for g in logs])
        for k in range(4):
            share_left2[k] = shares[k]
        logs = [right_log[x]] + [log_right2[d] for d in range(3)]
        shares, _ = shares_of([unpack_log(g) for g in logs])
        for k in range(4):
            share_right2[k] = shares[k]

    def view(i, j, k, cols):
        return all_ref.at[i, j, k, :, cols]

    def finish(k, waits):
        wait_all(waits)
        for h in range(4):
            at = k * 512 + h * 128
            cols = slice(at, at + 128)
            blocks = [left_now[y, :, cols]] + [in_left2[d, :, cols] for d in range(3)]
            shares = [share_left2[i] for i in range(4)]
            own[:, cols] = blended(blocks, shares, k * 4 + h)
            blocks = [right_now[x, :, cols]] + [in_right2[d, :, cols] for d in range(3)]
            shares = [share_right2[i] for i in range(4)]
            own[:, 1024 + at : 1152 + at] = blended(blocks, shares, 8 + k * 4 + h)
        return gather_first(copies, own, view, x, y, c, chunks[k])

    sums(0, 2)
    twin0 = to_twin(chunks[0])
    sums(1)
    log_wait.wait_recv()
    lax.fori_loop(0, 4, first_shares, 0)
    across0, logs = across(0, twin0)
    sums(3)
    twin1 = to_twin(chunks[1])
    across1, _ = across(1, twin1)
    load_weight.wait()
    for k in range(16):
        turned[:, k * 128 : (k + 1) * 128] = weight_ref[k * 128 : (k + 1) * 128, :].T
    wait_all(logs)
    lax.fori_loop(0, 4, second_shares, 0)
    along0, logs = along(0, across0)
    along1, _ = along(1, across1)
    wait_all(logs)
    third_shares()
    first = [finish(0, along0), finish(1, along1)]
    all_ref[x, y, c] = own[...]
    second, third = [], []
    for halves, waits in zip(chunks, first):
        wait_all(waits)
        second.append(gather_second(copies, view, x, y, c, halves))
        third.append(pass_own(copies, view, x, y, c, halves))

    def product(k, i):
        total = jnp.zeros((256, 256), f32)
        for cols in chunks[k]:
            total = total + lax.dot_general(
                turned[:, cols], all_ref[2 * i : 2 * i + 2, :, :, :, cols].reshape(256, 512),
                (((1,), (1,)), ((), ())), preferred_element_type=f32,
            )
        return total

    third[0] += pass_on(copies, second[0], view, x, y, c, chunks[0])
    third[1] += pass_on(copies, second[1], view, x, y, c, chunks[1])
    wait_all(third[0])
    for i in range(2):
        half_terms[:, i * 256 : i * 256 + 256] = product(0, i)
    wait_all(third[1])
    waits = []
    for i in range(2):
        cols = slice(i * 256, i * 256 + 256)
        terms[:, :, cols] = (
            (half_terms[:, cols] + product(1, i)).astype(bf16).reshape(4, 64, 256)
        )
        for d in (2, 1, 3):
            here = terms_in.at[d - 1, :, cols]
            waits.append(
                copies.send(terms.at[off(z, d), :, cols], here, {"head": off(z, d)}, here)
            )
    wait_all(waits)
    total = terms[z].astype(f32)
    for d in range(3):
        total = total + terms_in[d].astype(f32)
    out_ref[...] = total.astype(bf16)
    copies.drain()


def whole(lengths, queries, page_table, ks, vs, keys, values, weight):
    f32, bf16 = jnp.float32, jnp.bfloat16
    rows = queries.shape[0]
    width = queries.shape[1] * queries.shape[2]
    pages = keys.shape[0] // 32
    requests = 32 * rows
    vmem = pl.BlockSpec(memory_space=pltpu.VMEM)
    hbm = pl.BlockSpec(memory_space=pl.ANY)
    return pl.pallas_call(
        whole_kernel,
        out_shape=jax.ShapeDtypeStruct((64, 512), bf16),
        in_specs=[pl.BlockSpec(memory_space=pltpu.SMEM), vmem, vmem, vmem, vmem, hbm, hbm, hbm],
        out_specs=vmem,
        scratch_shapes=[
            pltpu.VMEM(keys.shape, bf16),
            pltpu.VMEM(keys.shape, bf16),
            pltpu.VMEM(weight.shape, bf16),
            pltpu.VMEM((rows * 16, 128), f32),
            pltpu.VMEM((rows, width), bf16),
            pltpu.VMEM((2, 4, 4, rows, width), bf16),
            pltpu.VMEM((8, 128), f32),
            pltpu.VMEM((4, 4, 2, 8, 128), f32),
            pltpu.VMEM((4, 2, 8, 128), f32),
            pltpu.VMEM((2, 8, 128), f32),
            pltpu.VMEM((3, 4, 2, 8, 128), f32),
            pltpu.VMEM((3, 2, 8, 128), f32),
            pltpu.VMEM((8, 128), f32),
            pltpu.VMEM((8, 128), f32),
            pltpu.VMEM((5, pages, 128), f32),
            pltpu.VMEM((pages, requests), bf16),
            pltpu.VMEM((requests, pages), bf16),
            pltpu.VMEM((pages // 8, 128, 128), bf16),
            pltpu.VMEM((UNROLL, 128, 256), f32),
            pltpu.VMEM((UNROLL, 128, 256), bf16),
            pltpu.VMEM((pages, width), f32),
            pltpu.VMEM((pages, 128), f32),
            pltpu.VMEM((pages, 128), f32),
            pltpu.VMEM((2, 4, 4, 16, 2048), bf16),
            pltpu.VMEM((2, 4, 4, 16, 128), bf16),
            pltpu.VMEM((4, 4, 16, 2048), bf16),
            pltpu.VMEM((4, 4, 16, 128), bf16),
            pltpu.VMEM((4, 4, 16, 2048), bf16),
            pltpu.VMEM((4, 4, 16, 128), bf16),
            pltpu.VMEM((2, 4, 4, 16, 128), f32),
            pltpu.VMEM((3, 4, 16, 1024), bf16),
            pltpu.VMEM((3, 4, 16, 1024), bf16),
            pltpu.VMEM((3, 4, 16, 128), bf16),
            pltpu.VMEM((3, 4, 16, 128), bf16),
            pltpu.VMEM((4, 4, 16, 128), f32),
            pltpu.VMEM((4, 4, 16, 128), f32),
            pltpu.VMEM((4, 16, 1024), bf16),
            pltpu.VMEM((4, 16, 1024), bf16),
            pltpu.VMEM((4, 16, 128), bf16),
            pltpu.VMEM((4, 16, 128), bf16),
            pltpu.VMEM((3, 16, 1024), bf16),
            pltpu.VMEM((3, 16, 1024), bf16),
            pltpu.VMEM((3, 16, 128), bf16),
            pltpu.VMEM((3, 16, 128), bf16),
            pltpu.VMEM((4, 16, 128), f32),
            pltpu.VMEM((4, 16, 128), f32),
            pltpu.VMEM((16, 2048), bf16),
            pltpu.VMEM((4, 4, 2, 16, 2048), bf16),
            pltpu.VMEM((256, 512), f32),
            pltpu.VMEM((4, 64, 512), bf16),
            pltpu.VMEM((3, 64, 512), bf16),
            pltpu.VMEM((256, 2048), bf16),
            pltpu.SemaphoreType.DMA((3,)),
            pltpu.SemaphoreType.DMA((134,)),
            pltpu.SemaphoreType.DMA((134,)),
        ],
        compiler_params=pltpu.CompilerParams(
            collective_id=1, has_side_effects=True, vmem_limit_bytes=60 * 1024 * 1024
        ),
        name="whole",
    )(lengths, queries, page_table, ks, vs, keys, values, weight)


def on_device(
    queries,
    k_codes,
    value_quantized_codes,
    key_page_scale,
    value_page_scale,
    lengths,
    page_table,
    out_weight,
):
    head_size = k_codes.shape[-1]
    return whole(
        lengths,
        queries,
        page_table,
        key_page_scale.T,
        value_page_scale.T,
        k_codes.reshape(-1, head_size),
        value_quantized_codes.reshape(-1, head_size),
        out_weight,
    ).T


def solution(mesh):
    in_specs = (
        P("req", "head", None),
        P("req", None, "head", None),
        P("req", None, "head", None),
        P("req", "head"),
        P("req", "head"),
        P("req"),
        P("req", None),
        P("head", "req"),
    )
    out_specs = P(None, ("req", "head"))
    return jax.shard_map(
        on_device, mesh=mesh, in_specs=in_specs, out_specs=out_specs, check_vma=False
    )
```

```python
import functools
import math

import jax
import jax.numpy as jnp
from jax import lax
from jax.experimental import pallas as pl
from jax.experimental.pallas import tpu as pltpu
from jax.sharding import PartitionSpec as P

LOG2E = 1.4426950408889634
UNROLL = 8


def pack_log(value):
    f32, bf16 = jnp.float32, jnp.bfloat16
    high = value.astype(bf16).astype(f32)
    middle = (value - high).astype(bf16).astype(f32)
    low = value - high - middle
    lane = lax.broadcasted_iota(jnp.int32, value.shape, 1)
    low = jnp.where(lane < 48, pltpu.roll(low, 32, 1), 0.0)
    low = jnp.where(lane < 32, pltpu.roll(middle, 16, 1), low)
    return jnp.where(lane < 16, high, low).astype(bf16)


def in_two(value):
    f32, bf16 = jnp.float32, jnp.bfloat16
    high = value.astype(bf16).astype(f32)
    lane = lax.broadcasted_iota(jnp.int32, value.shape, 1)
    return jnp.where(lane < 16, high, pltpu.roll(value - high, 16, 1)).astype(bf16)


def of_two(value):
    return value + pltpu.roll(value, 112, 1)


def page_columns(code_ref, ks_ref, vs_ref, rows_ref, wide_ref, pick_ref, pickt_ref):
    f32, bf16 = jnp.float32, jnp.bfloat16
    requests = pickt_ref.shape[0]
    scale = LOG2E / math.sqrt(128.0)

    def body(b, carry):
        code = code_ref[pl.ds(b, 1), :]
        lanes = pl.ds(pl.multiple_of(b * 128, 128), 128)
        owner_row = jnp.floor(code * (1.0 / 16.0))
        rows_ref[0:1, :] = owner_row
        rows_ref[1:2, :] = code - 16.0 * owner_row + 1.0
        rows_ref[2:4, :] = ks_ref[:, lanes] * scale
        rows_ref[4:6, :] = vs_ref[:, lanes]
        cols = rows_ref[...].T
        for i in range(5):
            wide_ref[i, lanes, :] = jnp.broadcast_to(cols[:, i + 1 : i + 2], (128, 128))
        owner = jnp.broadcast_to(cols[:, 0:1], (128, 128))
        lane = lax.broadcasted_iota(jnp.int32, (128, 128), 1).astype(f32)
        for c in range(requests // 128):
            pick_ref[lanes, c * 128 : (c + 1) * 128] = jnp.where(
                owner == lane + float(c * 128), 1.0, 0.0
            ).astype(bf16)
        row = lax.broadcasted_iota(jnp.int32, (requests, 128), 0).astype(f32)
        pickt_ref[:, lanes] = jnp.where(row == owner_row, 1.0, 0.0).astype(bf16)
        return carry

    lax.fori_loop(0, code_ref.shape[0], body, 0)


def page_queries(k, q_ref, pick_ref, qs_ref):
    f32, bf16 = jnp.float32, jnp.bfloat16
    tiles = qs_ref.shape[0]

    for n in (2 * k, 2 * k + 1, 2 * k + 4, 2 * k + 5):
        queries = q_ref[:, :, :, :, n * 256 : n * 256 + 256].reshape(pick_ref.shape[1], 256)
        got = jnp.dot(pick_ref[...], queries, preferred_element_type=f32)
        pair = [got[:, j * 128 : (j + 1) * 128].reshape(tiles, 8, 128) for j in range(2)]
        qs_ref[:, n * 16 : n * 16 + 16, :] = jnp.concatenate(pair, axis=1).astype(bf16)


def page_sums(k_ref, v_ref, wide_ref, qs_ref, s_ref, p_ref, po_ref, pm_ref, ps_ref):
    f32, bf16 = jnp.float32, jnp.bfloat16
    heads, half = 16, 8
    groups = qs_ref.shape[0] // UNROLL
    lane = lax.broadcasted_iota(jnp.int32, (8, 256), 1)
    sub = lax.broadcasted_iota(jnp.int32, (8, 256), 0)
    own = (lane >> 5) == sub
    token = ((lane & 31) >> 1).astype(f32)
    far = jnp.float32(1e9)
    tokens = [jnp.where(own & ((lane & 1) == j), token, far) for j in range(2)]
    lane8 = lax.broadcasted_iota(jnp.int32, (8, 128), 1)
    ones = jnp.ones((256, 128), bf16)

    def eight(g):
        return pl.ds(pl.multiple_of(g * 8, 8), 8)

    def kv_rows(g):
        return pl.ds(pl.multiple_of(g * 256, 256), 256)

    def values(u, g):
        both = jnp.concatenate([v_ref[kv_rows(g), :], ones], axis=1)
        out = jnp.dot(p_ref[u], both, preferred_element_type=f32)
        ps = jnp.zeros((8, 128), f32)
        for h in range(heads):
            rows = slice(h * 8, h * 8 + 8)
            po_ref[eight(g), h * 128 : (h + 1) * 128] = (
                out[rows, 0:128] * wide_ref[3 + h // half, eight(g), :]
            )
            ps = jnp.where(lane8 == h, out[rows, 128:256], ps)
        ps_ref[eight(g), :] = ps

    def soften(u, g):
        live = wide_ref[0, eight(g), :]
        live = jnp.concatenate([live, live], axis=1)
        pm = jnp.zeros((8, 128), f32)
        for j in range(2):
            keep = (tokens[j] < live)[None]
            scale = wide_ref[1 + j, eight(g), :]
            scale = jnp.concatenate([scale, scale], axis=1)[None]
            part = s_ref[u, j * 64 : (j + 1) * 64, :].reshape(8, 8, 256)
            part = jnp.where(keep, part * scale, -1e30)
            top = jnp.max(part, axis=2, keepdims=True)
            p_ref[u, j * 64 : (j + 1) * 64, :] = (
                jnp.exp2(part - top).reshape(64, 256).astype(bf16)
            )
            for h in range(8):
                pm = jnp.where(lane8 == j * 8 + h, top[h], pm)
        pm_ref[eight(g), :] = pm

    def scores(u, g):
        s_ref[u] = lax.dot_general(
            qs_ref[g], k_ref[kv_rows(g), :], (((1,), (1,)), ((), ())), preferred_element_type=f32
        )

    def body(i, carry):
        for u in range(UNROLL):
            scores(u, jnp.minimum(i, groups - 1) * UNROLL + u)
        for u in range(UNROLL):
            values(u, jnp.maximum(i - 1, 0) * UNROLL + u)
        for u in range(UNROLL):
            soften(u, jnp.minimum(i, groups - 1) * UNROLL + u)
        return carry

    lax.fori_loop(0, groups + 1, body, 0)


def unpack_log(aux):
    aux = aux.astype(jnp.float32)
    return aux + pltpu.roll(aux, 112, 1) + pltpu.roll(aux, 96, 1)


def request_weights(pick_ref, pickt_ref, pm_ref, ps_ref):
    f32, bf16 = jnp.float32, jnp.bfloat16
    pm = pm_ref[...]
    rough = jnp.dot(
        pickt_ref[...], jnp.exp2(pm * (1.0 / 12.0)).astype(bf16), preferred_element_type=f32
    )
    some = rough > 0.0
    shift = jnp.where(some, 12.0 * jnp.log2(jnp.where(some, rough, 1.0)) - 42.0, 0.0).astype(bf16)
    near = pm - jnp.dot(pick_ref[...], shift, preferred_element_type=f32)
    den = of_two(
        jnp.dot(pickt_ref[...], in_two(ps_ref[...] * jnp.exp2(near)), preferred_element_type=f32)
    )
    log = shift.astype(f32) + jnp.log2(jnp.where(some, den, 1.0))
    log = pack_log(jnp.where(some, log, -1e30))
    back = unpack_log(jnp.dot(pick_ref[...], log, preferred_element_type=f32))
    ps_ref[...] = jnp.exp2(jnp.minimum(pm - back, 64.0))
    return log


def request_sums(n, pickt_ref, po_ref, ps_ref):
    f32, bf16 = jnp.float32, jnp.bfloat16
    share = ps_ref[...].astype(bf16)
    wide = (po_ref.shape[0], 128)
    cols = [
        (
            po_ref[:, h * 128 : (h + 1) * 128]
            * jnp.broadcast_to(share[:, h : h + 1], wide).astype(f32)
        ).astype(bf16)
        for h in range(4 * n, 4 * n + 4)
    ]
    return jnp.dot(
        pickt_ref[...], jnp.concatenate(cols, axis=1), preferred_element_type=f32
    ).astype(bf16)


MESH = pl.DeviceIdType.MESH


def place():
    me = lax.axis_index("req")
    return lax.div(me, 8), lax.rem(lax.div(me, 2), 4), lax.rem(me, 2)


def off(i, d):
    return lax.rem(i + d + 4, 4)


def chip(x, y, c):
    return {"req": (x * 4 + y) * 2 + c}


class Copies:
    def __init__(self, send_sems, recv_sems):
        self.sems, self.count, self.sent = (send_sems, recv_sems), 0, []

    def send(self, source, target, device, landing):
        pair = (self.sems[0].at[self.count], self.sems[1].at[self.count])
        self.count += 1
        copy = pltpu.make_async_remote_copy(source, target, *pair, device, device_id_type=MESH)
        copy.start()
        self.sent.append(copy)
        return pltpu.make_async_remote_copy(source, landing, *pair, device, device_id_type=MESH)

    def drain(self):
        for copy in self.sent:
            copy.wait_send()


def greet(peers):
    barrier = pltpu.get_barrier_semaphore()
    for peer in peers:
        pl.semaphore_signal(barrier, inc=1, device_id=peer, device_id_type=MESH)
    return lambda: pl.semaphore_wait(barrier, len(peers))


def gather_first(copies, own, view, x, y, c, halves):
    left, right = halves
    waits = []
    for d in (2, 1, 3):
        waits.append(
            copies.send(
                own.at[:, left], view(x, y, c, left), chip(x, off(y, d), c),
                view(x, off(y, -d), c, left),
            )
        )
        waits.append(
            copies.send(
                own.at[:, right], view(x, y, c, right), chip(off(x, d), y, c),
                view(off(x, -d), y, c, right),
            )
        )
    return waits


def gather_second(copies, view, x, y, c, halves):
    left, right = halves
    every = slice(None)
    waits = []
    for d in (2, 1, 3):
        waits.append(
            copies.send(
                view(x, every, c, left), view(x, every, c, left), chip(off(x, d), y, c),
                view(off(x, -d), every, c, left),
            )
        )
        waits.append(
            copies.send(
                view(every, y, c, right), view(every, y, c, right), chip(x, off(y, d), c),
                view(every, off(y, -d), c, right),
            )
        )
    return waits


def pass_own(copies, view, x, y, c, halves):
    left, right = halves
    every = slice(None)
    twin = chip(x, y, 1 - c)
    return [
        copies.send(view(x, every, c, left), view(x, every, c, left), twin,
                    view(x, every, 1 - c, left)),
        copies.send(view(every, y, c, right), view(every, y, c, right), twin,
                    view(every, y, 1 - c, right)),
    ]


def pass_on(copies, waits, view, x, y, c, halves):
    left, right = halves
    every = slice(None)
    twin = chip(x, y, 1 - c)
    last = []
    for k, d in enumerate((2, 1, 3)):
        waits[2 * k].wait_recv()
        i = off(x, -d)
        piece = view(i, every, c, left)
        last.append(copies.send(piece, piece, twin, view(i, every, 1 - c, left)))
        waits[2 * k + 1].wait_recv()
        j = off(y, -d)
        piece = view(every, j, c, right)
        last.append(copies.send(piece, piece, twin, view(every, j, 1 - c, right)))
    return last


def wait_all(waits):
    for wait in waits:
        wait.wait_recv()


def shares_of(logs):
    top = functools.reduce(jnp.maximum, logs)
    shares = [jnp.exp2(g - top) for g in logs]
    total = functools.reduce(jnp.add, shares)
    inverse = 1.0 / total
    return [s * inverse for s in shares], pack_log(top + jnp.log2(total))


def blended(blocks, shares, head):
    terms = [b.astype(jnp.float32) * s[:, head : head + 1] for b, s in zip(blocks, shares)]
    return functools.reduce(jnp.add, terms).astype(jnp.bfloat16)


def whole_kernel(
    lengths_ref, queries_ref, table_ref, ks_ref, vs_ref, k_hbm, v_hbm, weight_hbm, out_ref,
    k_ref, v_ref, weight_ref, wide_q, q_ref, every_ref, code_ref, table_out, sum_y, sum_c, in_x, in_y, in_c,
    rows_ref, wide_ref, pick_ref, pickt_ref, qs_ref, s_ref, p_ref, po_ref, pm_ref, ps_ref,
    part_ref, log_ref, twin_in, log_in, now, now_log, share0,
    in_left, in_right, log_left, log_right, share_left, share_right,
    left_now, right_now, left_log, right_log,
    in_left2, in_right2, log_left2, log_right2, share_left2, share_right2,
    own, all_ref, half_terms, terms, terms_in, turned, load_sems, send_sems, recv_sems,
):
    f32, bf16 = jnp.float32, jnp.bfloat16
    x, y, c = place()
    z = lax.axis_index("head")
    rows = q_ref.shape[0]
    chunks = [
        (slice(k * 512, k * 512 + 512), slice(1024 + k * 512, 1536 + k * 512)) for k in range(2)
    ]
    loads = [
        pltpu.make_async_copy(k_hbm, k_ref, load_sems.at[0]),
        pltpu.make_async_copy(v_hbm, v_ref, load_sems.at[1]),
    ]
    load_weight = pltpu.make_async_copy(weight_hbm, weight_ref, load_sems.at[2])
    load_weight.start()
    for load in loads:
        load.start()

    def view_all(i, j, k, cols):
        return every_ref.at[k, i, j, :, cols]

    peers = [chip(off(x, d), y, c) for d in (1, 2, 3)]
    peers += [chip(x, off(y, d), c) for d in (1, 2, 3)]
    peers += [chip(x, y, 1 - c)] + [{"head": off(z, d)} for d in (1, 2, 3)]
    met = greet(peers)
    wide_q[...] = queries_ref[...].astype(f32).reshape(wide_q.shape)
    for h in range(16):
        q_ref[:, h * 128 : (h + 1) * 128] = wide_q[pl.ds(h, rows, stride=16), :].astype(bf16)
    copies = Copies(send_sems, recv_sems)
    lane = lax.broadcasted_iota(jnp.int32, (1, 128), 1)
    high_id = lax.broadcasted_iota(jnp.int32, (256, 128), 0)
    low_id = lax.broadcasted_iota(jnp.int32, (128, 128), 0)
    highs, lows = [], []
    for r in range(rows):
        live = jnp.clip(lengths_ref[r] - 16 * lane, 0, 16)
        coded = jnp.where(live > 0, live + 16 * r, 0).astype(f32)
        ids = table_ref[r : r + 1, :]
        highs.append(jnp.where(high_id == (ids >> 7), 1.0, 0.0).astype(bf16))
        lows.append(jnp.where(low_id == (ids & 127), coded, 0.0).astype(bf16))
    found = lax.dot_general(
        jnp.concatenate(highs, axis=1), jnp.concatenate(lows, axis=1),
        (((1,), (1,)), ((), ())), preferred_element_type=f32,
    )
    base = ((c * 16 + x * 4 + y) * 256).astype(f32)
    table_out[...] = jnp.where(found > 0.0, found + base, 0.0).reshape(4, 4, 2, 8, 128)
    every_ref[c, x, y] = q_ref[...]
    met()
    got = [
        copies.send(
            table_out.at[off(x, d)], in_x.at[d - 1], chip(off(x, d), y, c), in_x.at[d - 1]
        )
        for d in (2, 1, 3)
    ]
    first = [gather_first(copies, q_ref, view_all, x, y, c, halves) for halves in chunks]
    wait_all(got)
    sum_y[...] = table_out[x] + in_x[0] + in_x[1] + in_x[2]
    got = [
        copies.send(sum_y.at[off(y, d)], in_y.at[d - 1], chip(x, off(y, d), c), in_y.at[d - 1])
        for d in (2, 1, 3)
    ]
    second, third = [], []
    for halves, waits in zip(chunks, first):
        wait_all(waits)
        second.append(gather_second(copies, view_all, x, y, c, halves))
        third.append(pass_own(copies, view_all, x, y, c, halves))
    wait_all(got)
    sum_c[...] = sum_y[y] + in_y[0] + in_y[1] + in_y[2]
    copies.send(sum_c.at[1 - c], in_c, chip(x, y, 1 - c), in_c).wait_recv()
    code_ref[...] = sum_c[c] + in_c[...] - 1.0
    page_columns(code_ref, ks_ref, vs_ref, rows_ref, wide_ref, pick_ref, pickt_ref)
    third[0] += pass_on(copies, second[0], view_all, x, y, c, chunks[0])
    third[1] += pass_on(copies, second[1], view_all, x, y, c, chunks[1])
    wait_all(third[0])
    page_queries(0, every_ref, pick_ref, qs_ref)
    wait_all(third[1])
    page_queries(1, every_ref, pick_ref, qs_ref)
    for load in loads:
        load.wait()
    page_sums(k_ref, v_ref, wide_ref, qs_ref, s_ref, p_ref, po_ref, pm_ref, ps_ref)
    log_ref[...] = request_weights(pick_ref, pickt_ref, pm_ref, ps_ref).reshape(
        2, 4, 4, rows, 128
    )
    twin = chip(x, y, 1 - c)
    log_wait = copies.send(log_ref.at[1 - c], log_in, twin, log_in)

    def sums(*pairs):
        for n in pairs:
            part_ref[:, :, :, :, n * 512 : n * 512 + 512] = request_sums(
                n, pickt_ref, po_ref, ps_ref
            ).reshape(2, 4, 4, rows, 512)

    def to_twin(halves):
        return [
            copies.send(
                part_ref.at[1 - c, :, :, :, cols], twin_in.at[:, :, :, cols], twin,
                twin_in.at[:, :, :, cols],
            )
            for cols in halves
        ]

    def first_shares(j, carry):
        for i in range(4):
            shares, log = shares_of([unpack_log(log_ref[c, i, j]), unpack_log(log_in[i, j])])
            now_log[i, j] = log
            for k in range(2):
                share0[k, i, j] = shares[k]
        return carry

    def across(k, waits):
        wait_all(waits)

        def body(i, carry):
            for j in range(4):
                shares = [share0[0, i, j], share0[1, i, j]]
                for h in range(4):
                    for side in range(2):
                        at = side * 1024 + k * 512 + h * 128
                        cols = slice(at, at + 128)
                        now[i, j, :, cols] = blended(
                            [part_ref[c, i, j, :, cols], twin_in[i, j, :, cols]],
                            shares, side * 8 + k * 4 + h,
                        )
            return carry

        lax.fori_loop(0, 4, body, 0)
        left, right = chunks[k]
        near = chunks[k][0]
        waits, logs = [], []
        for d in (2, 1, 3):
            to_x, to_y = chip(off(x, d), y, c), chip(x, off(y, d), c)
            if k == 0:
                logs.append(
                    copies.send(
                        now_log.at[off(x, d)], log_left.at[d - 1], to_x, log_left.at[d - 1]
                    )
                )
                logs.append(
                    copies.send(
                        now_log.at[:, off(y, d)], log_right.at[d - 1], to_y, log_right.at[d - 1]
                    )
                )
            here = in_left.at[d - 1, :, :, near]
            waits.append(copies.send(now.at[off(x, d), :, :, left], here, to_x, here))
            here = in_right.at[d - 1, :, :, near]
            waits.append(copies.send(now.at[:, off(y, d), :, right], here, to_y, here))
        return waits, logs

    def second_shares(j, carry):
        logs = [now_log[x, j]] + [log_left[d, j] for d in range(3)]
        shares, log = shares_of([unpack_log(g) for g in logs])
        left_log[j] = log
        for k in range(4):
            share_left[k, j] = shares[k]
        logs = [now_log[j, y]] + [log_right[d, j] for d in range(3)]
        shares, log = shares_of([unpack_log(g) for g in logs])
        right_log[j] = log
        for k in range(4):
            share_right[k, j] = shares[k]
        return carry

    def along(k, waits):
        wait_all(waits)

        def body(j, carry):
            shares = [share_left[i, j] for i in range(4)]
            for h in range(4):
                at = k * 512 + h * 128
                cols = slice(at, at + 128)
                blocks = [now[x, j, :, cols]] + [in_left[d, j, :, cols] for d in range(3)]
                left_now[j, :, cols] = blended(blocks, shares, k * 4 + h)
            shares = [share_right[i, j] for i in range(4)]
            for h in range(4):
                at = k * 512 + h * 128
                cols = slice(at, at + 128)
                blocks = [now[j, y, :, 1024 + at : 1152 + at]]
                blocks += [in_right[d, j, :, cols] for d in range(3)]
                right_now[j, :, cols] = blended(blocks, shares, 8 + k * 4 + h)
            return carry

        lax.fori_loop(0, 4, body, 0)
        near = chunks[k][0]
        waits, logs = [], []
        for d in (2, 1, 3):
            to_x, to_y = chip(off(x, d), y, c), chip(x, off(y, d), c)
            if k == 0:
                logs.append(
                    copies.send(
                        left_log.at[off(y, d)], log_left2.at[d - 1], to_y, log_left2.at[d - 1]
                    )
                )
                logs.append(
                    copies.send(
                        right_log.at[off(x, d)], log_right2.at[d - 1], to_x, log_right2.at[d - 1]
                    )
                )
            here = in_left2.at[d - 1, :, near]
            waits.append(copies.send(left_now.at[off(y, d), :, near], here, to_y, here))
            here = in_right2.at[d - 1, :, near]
            waits.append(copies.send(right_now.at[off(x, d), :, near], here, to_x, here))
        return waits, logs

    def third_shares():
        logs = [left_log[y]] + [log_left2[d] for d in range(3)]
        shares, _ = shares_of([unpack_log(g) for g in logs])
        for k in range(4):
            share_left2[k] = shares[k]
        logs = [right_log[x]] + [log_right2[d] for d in range(3)]
        shares, _ = shares_of([unpack_log(g) for g in logs])
        for k in range(4):
            share_right2[k] = shares[k]

    def view(i, j, k, cols):
        return all_ref.at[i, j, k, :, cols]

    def finish(k, waits):
        wait_all(waits)
        for h in range(4):
            at = k * 512 + h * 128
            cols = slice(at, at + 128)
            blocks = [left_now[y, :, cols]] + [in_left2[d, :, cols] for d in range(3)]
            shares = [share_left2[i] for i in range(4)]
            own[:, cols] = blended(blocks, shares, k * 4 + h)
            blocks = [right_now[x, :, cols]] + [in_right2[d, :, cols] for d in range(3)]
            shares = [share_right2[i] for i in range(4)]
            own[:, 1024 + at : 1152 + at] = blended(blocks, shares, 8 + k * 4 + h)
        return gather_first(copies, own, view, x, y, c, chunks[k])

    sums(0, 2)
    twin0 = to_twin(chunks[0])
    sums(1)
    log_wait.wait_recv()
    lax.fori_loop(0, 4, first_shares, 0)
    across0, logs = across(0, twin0)
    sums(3)
    twin1 = to_twin(chunks[1])
    across1, _ = across(1, twin1)
    load_weight.wait()
    for k in range(16):
        turned[:, k * 128 : (k + 1) * 128] = weight_ref[k * 128 : (k + 1) * 128, :].T
    wait_all(logs)
    lax.fori_loop(0, 4, second_shares, 0)
    along0, logs = along(0, across0)
    along1, _ = along(1, across1)
    wait_all(logs)
    third_shares()
    first = [finish(0, along0), finish(1, along1)]
    all_ref[x, y, c] = own[...]
    second, third = [], []
    for halves, waits in zip(chunks, first):
        wait_all(waits)
        second.append(gather_second(copies, view, x, y, c, halves))
        third.append(pass_own(copies, view, x, y, c, halves))

    def product(k, i):
        total = jnp.zeros((256, 256), f32)
        for cols in chunks[k]:
            total = total + lax.dot_general(
                turned[:, cols], all_ref[2 * i : 2 * i + 2, :, :, :, cols].reshape(256, 512),
                (((1,), (1,)), ((), ())), preferred_element_type=f32,
            )
        return total

    third[0] += pass_on(copies, second[0], view, x, y, c, chunks[0])
    third[1] += pass_on(copies, second[1], view, x, y, c, chunks[1])
    wait_all(third[0])
    for i in range(2):
        half_terms[:, i * 256 : i * 256 + 256] = product(0, i)
    wait_all(third[1])
    waits = []
    for i in range(2):
        cols = slice(i * 256, i * 256 + 256)
        terms[:, :, cols] = (
            (half_terms[:, cols] + product(1, i)).astype(bf16).reshape(4, 64, 256)
        )
        for d in (2, 1, 3):
            here = terms_in.at[d - 1, :, cols]
            waits.append(
                copies.send(terms.at[off(z, d), :, cols], here, {"head": off(z, d)}, here)
            )
    wait_all(waits)
    total = terms[z].astype(f32)
    for d in range(3):
        total = total + terms_in[d].astype(f32)
    out_ref[...] = total.astype(bf16)
    copies.drain()


def whole(lengths, queries, page_table, ks, vs, keys, values, weight):
    f32, bf16 = jnp.float32, jnp.bfloat16
    rows = queries.shape[0]
    width = queries.shape[1] * queries.shape[2]
    pages = keys.shape[0] // 32
    requests = 32 * rows
    vmem = pl.BlockSpec(memory_space=pltpu.VMEM)
    hbm = pl.BlockSpec(memory_space=pl.ANY)
    return pl.pallas_call(
        whole_kernel,
        out_shape=jax.ShapeDtypeStruct((64, 512), bf16),
        in_specs=[pl.BlockSpec(memory_space=pltpu.SMEM), vmem, vmem, vmem, vmem, hbm, hbm, hbm],
        out_specs=vmem,
        scratch_shapes=[
            pltpu.VMEM(keys.shape, bf16),
            pltpu.VMEM(keys.shape, bf16),
            pltpu.VMEM(weight.shape, bf16),
            pltpu.VMEM((rows * 16, 128), f32),
            pltpu.VMEM((rows, width), bf16),
            pltpu.VMEM((2, 4, 4, rows, width), bf16),
            pltpu.VMEM((8, 128), f32),
            pltpu.VMEM((4, 4, 2, 8, 128), f32),
            pltpu.VMEM((4, 2, 8, 128), f32),
            pltpu.VMEM((2, 8, 128), f32),
            pltpu.VMEM((3, 4, 2, 8, 128), f32),
            pltpu.VMEM((3, 2, 8, 128), f32),
            pltpu.VMEM((8, 128), f32),
            pltpu.VMEM((8, 128), f32),
            pltpu.VMEM((5, pages, 128), f32),
            pltpu.VMEM((pages, requests), bf16),
            pltpu.VMEM((requests, pages), bf16),
            pltpu.VMEM((pages // 8, 128, 128), bf16),
            pltpu.VMEM((UNROLL, 128, 256), f32),
            pltpu.VMEM((UNROLL, 128, 256), bf16),
            pltpu.VMEM((pages, width), f32),
            pltpu.VMEM((pages, 128), f32),
            pltpu.VMEM((pages, 128), f32),
            pltpu.VMEM((2, 4, 4, 16, 2048), bf16),
            pltpu.VMEM((2, 4, 4, 16, 128), bf16),
            pltpu.VMEM((4, 4, 16, 2048), bf16),
            pltpu.VMEM((4, 4, 16, 128), bf16),
            pltpu.VMEM((4, 4, 16, 2048), bf16),
            pltpu.VMEM((4, 4, 16, 128), bf16),
            pltpu.VMEM((2, 4, 4, 16, 128), f32),
            pltpu.VMEM((3, 4, 16, 1024), bf16),
            pltpu.VMEM((3, 4, 16, 1024), bf16),
            pltpu.VMEM((3, 4, 16, 128), bf16),
            pltpu.VMEM((3, 4, 16, 128), bf16),
            pltpu.VMEM((4, 4, 16, 128), f32),
            pltpu.VMEM((4, 4, 16, 128), f32),
            pltpu.VMEM((4, 16, 1024), bf16),
            pltpu.VMEM((4, 16, 1024), bf16),
            pltpu.VMEM((4, 16, 128), bf16),
            pltpu.VMEM((4, 16, 128), bf16),
            pltpu.VMEM((3, 16, 1024), bf16),
            pltpu.VMEM((3, 16, 1024), bf16),
            pltpu.VMEM((3, 16, 128), bf16),
            pltpu.VMEM((3, 16, 128), bf16),
            pltpu.VMEM((4, 16, 128), f32),
            pltpu.VMEM((4, 16, 128), f32),
            pltpu.VMEM((16, 2048), bf16),
            pltpu.VMEM((4, 4, 2, 16, 2048), bf16),
            pltpu.VMEM((256, 512), f32),
            pltpu.VMEM((4, 64, 512), bf16),
            pltpu.VMEM((3, 64, 512), bf16),
            pltpu.VMEM((256, 2048), bf16),
            pltpu.SemaphoreType.DMA((3,)),
            pltpu.SemaphoreType.DMA((134,)),
            pltpu.SemaphoreType.DMA((134,)),
        ],
        compiler_params=pltpu.CompilerParams(
            collective_id=1, has_side_effects=True, vmem_limit_bytes=60 * 1024 * 1024
        ),
        name="whole",
    )(lengths, queries, page_table, ks, vs, keys, values, weight)


def on_device(
    queries,
    k_codes,
    value_quantized_codes,
    key_page_scale,
    value_page_scale,
    lengths,
    page_table,
    out_weight,
):
    head_size = k_codes.shape[-1]
    return whole(
        lengths,
        queries,
        page_table,
        key_page_scale.T,
        value_page_scale.T,
        k_codes.reshape(-1, head_size),
        value_quantized_codes.reshape(-1, head_size),
        out_weight,
    ).T


def solution(mesh):
    in_specs = (
        P("req", "head", None),
        P("req", None, "head", None),
        P("req", None, "head", None),
        P("req", "head"),
        P("req", "head"),
        P("req"),
        P("req", None),
        P("head", "req"),
    )
    out_specs = P(None, ("req", "head"))
    return jax.shard_map(
        on_device, mesh=mesh, in_specs=in_specs, out_specs=out_specs, check_vma=False
    )
```
